32 devices in a mesh: depth: 2 (over core), rows: 4 (over y, x), cols: 4 (over z).
Axes of the slice: x: 2, y: 2, z: 4, core: 2. Of those that a mesh axis runs over, the one named last changes fastest.
Arguments:
- section_states: float32 [2, 128, 64, 256], P('depth', 'rows', 'cols'), may hold values from -6 to 6
- weights: bfloat16 [4, 3, 3, 256, 256], P('depth'), may hold values from -0.125 to 0.125
Outputs:
- fine_states: float32 [4, 128, 64, 256], P('depth', 'rows', 'cols')
- coarse_states: float32 [2, 128, 64, 256], P('depth', 'rows', 'cols')
The draws below stay inside these ranges and needn't reach their ends.
All inputs are finite; a program needn't handle non-finite values.
Results may differ from the reference program's by a relative error of at most 0.002.
Values may be sent and summed in bfloat16 or wider, within the bound.
A program may use at most 64 MiB of HBM per device.

```python
import jax
import jax.numpy as jnp
from jax import lax

C = 256
SECTIONS = 2
LAYERS = 4
HEIGHT = 128
WIDTH = 64


def level_of(rng, extent, cuts, least, high):
    loudness, own = 1.0, jax.random.fold_in(rng, 6)
    for dim, blocks in cuts:
        steps = jnp.exp(jax.random.uniform(jax.random.fold_in(own, dim), (blocks,), jnp.float32, least / len(cuts), high / len(cuts)))
        loudness = loudness * jnp.repeat(steps, extent[dim] // blocks).reshape([-1 if axis == dim else 1 for axis in range(len(extent))])
    return loudness


def gaussian(rng, extent, scale, reach, shards=(), held_as=jnp.bfloat16):
    drawn = jax.random.normal(rng, extent, jnp.float32) * scale
    if len(shards) > 0:
        drawn = level_of(rng, extent, shards, -0.22, 0.18) * drawn
    return jnp.clip(drawn, min=-reach, max=reach).astype(held_as)


def setup_inputs(seed: int = 0) -> dict:
    splits = jax.random.split(jax.random.key(seed), 3)
    section_states = gaussian(splits[0], (SECTIONS, HEIGHT, WIDTH, C), 1.0, 6.0, ((0, 2), (1, 4), (2, 4)), jnp.float32)
    weights = gaussian(splits[1], (LAYERS, 3, 3, C, C), (9 * C) ** -0.5, 0.125, ((0, 2),))
    return dict(section_states=section_states, weights=weights)


def velocity(field, kernel):
    rows_here, cols_here, channels = field.shape
    rounded = lax.optimization_barrier(jax.nn.silu(field).astype(jnp.bfloat16)).astype(jnp.float32)
    padded = jnp.pad(rounded, ((1, 1), (1, 1), (0, 0)))
    summed = jnp.zeros((rows_here * cols_here, channels), jnp.float32)
    for shift_row in range(3):
        for shift_col in range(3):
            window = padded[shift_row:shift_row + rows_here, shift_col:shift_col + cols_here].reshape(-1, channels)
            summed = summed + jnp.dot(window, kernel[shift_row, shift_col].astype(jnp.float32), preferred_element_type=jnp.float32)
    return summed.reshape(rows_here, cols_here, channels)


def reference(section_states, weights):
    step_size = 2.0 / LAYERS
    sections = section_states.shape[0]
    jump_list = []
    for section in range(sections):
        anchor = section_states[section]
        first_slope = velocity(anchor, weights[2 * section])
        middle = anchor + step_size * first_slope
        ending = middle + step_size * velocity(middle, weights[2 * section + 1])
        jump_list.append(ending - (anchor + 2.0 * step_size * first_slope))
    coarse = [section_states[0]]
    for section in range(sections - 1):
        current = coarse[-1]
        coarse.append(current + 2.0 * step_size * velocity(current, weights[2 * section]) + jump_list[section])
    fine_list = []
    for section in range(sections):
        middle = coarse[section] + step_size * velocity(coarse[section], weights[2 * section])
        ending = middle + step_size * velocity(middle, weights[2 * section + 1])
        fine_list.append(middle)
        fine_list.append(ending)
    return jnp.stack(fine_list), jnp.stack(coarse)
```

```python
import functools

import jax
import jax.numpy as jnp
from jax import lax
from jax.experimental import pallas as pl
from jax.experimental.pallas import tpu as pltpu
from jax.sharding import PartitionSpec as P

MESH = pl.DeviceIdType.MESH
HALO = 4
LANES = 128
LIMIT = 32 * 1024 * 1024


def padded_2(shard, sides, width):
    for axis, dim in sides:
        size, length = (lax.axis_size(axis), shard.shape[dim])
        up = [(i, (i + 1) % size) for i in range(size - 1)]
        down = [(j, i) for i, j in up]
        last = lax.slice_in_dim(shard, length - width, length, axis=dim)
        initial = lax.slice_in_dim(shard, 0, width, axis=dim)
        before = lax.ppermute(last, axis, up)
        after = lax.ppermute(initial, axis, down)
        shard = jnp.concatenate([before, shard, after], axis=dim)
    return shard


def shifted_2(block, axis, distance):
    devices = range(lax.axis_size(axis))
    route = [(i - distance, i) for i in devices if i - distance in devices]
    return lax.ppermute(block, axis, route)


def activate(field):
    return jax.nn.silu(field).astype(jnp.bfloat16)


def apply_stencil(padded, flat_weight, out_rows, out_cols):
    channels = padded.shape[2]
    patches = jnp.concatenate(
        [
            padded[shift_row : shift_row + out_rows, shift_col : shift_col + out_cols]
            for shift_row in range(3)
            for shift_col in range(3)
        ],
        axis=2,
    )
    summed = jnp.dot(
        patches.reshape(out_rows * out_cols, 9 * channels),
        flat_weight,
        preferred_element_type=jnp.float32,
    )
    return summed.reshape(out_rows, out_cols, channels)


def section_pass(anchor, first_weight, second_weight, step_size):
    rows_here, cols_here, channels = anchor.shape
    widened = padded_2(anchor, (("rows", 0), ("cols", 1)), 2)
    slope_wide = apply_stencil(activate(widened), first_weight, rows_here + 2, cols_here + 2)
    middle_wide = widened[1:-1, 1:-1] + step_size * slope_wide
    row_global = lax.axis_index("rows") * rows_here - 1 + jnp.arange(rows_here + 2)
    col_global = lax.axis_index("cols") * cols_here - 1 + jnp.arange(cols_here + 2)
    inside_rows = (row_global >= 0) & (row_global < rows_here * lax.axis_size("rows"))
    inside_cols = (col_global >= 0) & (col_global < cols_here * lax.axis_size("cols"))
    inside = inside_rows[:, None] & inside_cols[None, :]
    second_act = jnp.where(inside[:, :, None], activate(middle_wide), jnp.zeros((), jnp.bfloat16))
    first_slope = slope_wide[1:-1, 1:-1]
    middle = middle_wide[1:-1, 1:-1]
    second_slope = apply_stencil(second_act, second_weight, rows_here, cols_here)
    ending = middle + step_size * second_slope
    return (first_slope, middle, ending)


def chain_on_device(section_states, weights):
    rows_here, cols_here, channels = section_states.shape[1:]
    ndepth = lax.axis_size("depth")
    position = lax.axis_index("depth")
    step_size = 2.0 / (2 * ndepth)
    first_weight = weights[0].reshape(9 * channels, channels)
    second_weight = weights[1].reshape(9 * channels, channels)
    anchor = section_states[0]
    first_slope, middle, ending = section_pass(anchor, first_weight, second_weight, step_size)
    jump = ending - (anchor + 2.0 * step_size * first_slope)

    def chain_turn(step_index, current):
        padded = padded_2(activate(current), (("rows", 0), ("cols", 1)), 1)
        advanced = (
            current
            + 2.0 * step_size * apply_stencil(padded, first_weight, rows_here, cols_here)
            + jump
        )
        shifted = shifted_2(advanced, "depth", 1)
        return jnp.where(position == 0, anchor, shifted)

    corrected = lax.fori_loop(0, ndepth - 1, chain_turn, anchor)
    final_slope, final_middle, final_ending = section_pass(
        corrected, first_weight, second_weight, step_size
    )
    fine_states = jnp.stack([final_middle, final_ending])
    return (fine_states, corrected[None])


DIRECTIONS = ((-1, 0), (1, 0), (0, -1), (0, 1), (-1, -1), (-1, 1), (1, -1), (1, 1))
LEFT = 8


def silu(u):
    half = 0.5 * u
    return half + half * jnp.tanh(half)


def masked_silu(u, mask):
    kept = (0.5 * u) * mask
    return kept + kept * jnp.tanh(0.5 * u)


def as_rows(block):
    return block.reshape(-1, LANES).astype(jnp.bfloat16)


def tap_dot(windows, halves, weight):
    lhs = []
    for a in range(3):
        for b in range(3):
            for c in range(halves):
                parts = [as_rows(window(c, a, b)) for window in windows]
                lhs.append(parts[0] if len(parts) == 1 else jnp.concatenate(parts, axis=0))
    return jnp.dot(jnp.concatenate(lhs, axis=1), weight[...], preferred_element_type=jnp.float32)


def lanes_of(block, c, shape):
    return block[:, c * LANES : (c + 1) * LANES].reshape(shape)


def upper_sublanes(rows):
    return lax.broadcasted_iota(jnp.int32, (rows, 8, LANES), 1) < HALO


def packed(ref, c, first_row, rows, left, right):
    near = ref[c, first_row : first_row + rows, left : left + 8, :]
    far = ref[c, first_row : first_row + rows, right : right + 8, :]
    return jnp.where(upper_sublanes(rows), near, far)


def store_packed(ref, c, first_row, left, right, value):
    whole = slice(first_row, first_row + value.shape[0])
    ref[c, whole, left : left + HALO, :] = value[:, 0:HALO]
    ref[c, whole, right + HALO : right + 8, :] = value[:, HALO:8]


def interior(layer, act, weight, before, after, act_after, step_size, shape):
    halves, rows_here, cols_here = shape
    first, rows = HALO + 1 + layer, rows_here - 2 - 2 * layer
    narrow = layer == 3 and cols_here == 16
    left, wide = (LEFT + HALO, cols_here - 2 * HALO) if narrow else (LEFT, cols_here)

    def window(c, a, b):
        return act[c, first + a - 1 : first + a - 1 + rows, left + b - 1 : left + b - 1 + wide, :]

    acc = step_size * tap_dot([window], halves, weight)
    for c in range(halves):
        here = (c, slice(first, first + rows), slice(left, left + wide), slice(None))
        u = before[here] + lanes_of(acc, c, (rows, wide, LANES))
        after[here] = u
        if act_after is not None:
            act_after[here] = silu(u)


def ring(layer, act, weight, before, after, act_after, step_size, shape, place):
    halves, rows_here, cols_here = shape
    nrows, ncols, row, col = place
    high = rows_here + 2 * HALO
    first, rows = 1 + layer, high - 2 - 2 * layer
    tops = (first, high - HALO - first)
    narrow = layer == 3 and cols_here == 16
    left, wide = (LEFT + HALO, cols_here - 2 * HALO) if narrow else (LEFT, cols_here)
    near, far = HALO + layer, LEFT + cols_here - 6 - layer

    def strip(at):
        return lambda c, a, b: act[c, at + a - 1 : at + a - 1 + HALO, left + b - 1 : left + b - 1 + wide, :]

    def sides(c, a, b):
        return packed(act, c, first + a - 1, rows, near + b, far + b)

    acc = step_size * tap_dot([strip(tops[0]), strip(tops[1]), sides], halves, weight)
    above = jnp.where(row > 0, 1.0, 0.0)
    below = jnp.where(row < nrows - 1, 1.0, 0.0)
    sub = lax.broadcasted_iota(jnp.int32, (1, 8, LANES), 1)
    j = jnp.where(sub < HALO, sub + (layer - 3), sub + (cols_here - 5 - layer)) + col * cols_here
    held = jnp.where((j >= 0) & (j < ncols * cols_here), 1.0, 0.0)
    m = HALO * wide
    for c in range(halves):
        for k, at in enumerate(tops):
            rise = lanes_of(acc[k * m : (k + 1) * m], c, (HALO, wide, LANES))
            here = (c, slice(at, at + HALO), slice(left, left + wide), slice(None))
            u = before[here] + rise
            after[here] = u
            if act_after is None:
                continue
            for i in range(HALO):
                value = silu(u[i])
                if at + i < HALO:
                    value = value * above
                elif at + i >= high - HALO:
                    value = value * below
                act_after[c, at + i, left : left + wide, :] = value
        u = packed(before, c, first, rows, near + 1, far + 1) + lanes_of(acc[2 * m :], c, (rows, 8, LANES))
        store_packed(after, c, first, near + 1, far + 1, u)
        if act_after is None:
            continue
        edge = HALO - first
        for at, n, mask in (
            (0, edge, held * above), (edge, rows - 2 * edge, held), (rows - edge, edge, held * below),
        ):
            if n > 0:
                store_packed(act_after, c, first + at, near + 1, far + 1, masked_silu(u[at : at + n], mask))


def gather_kernel(
    sizes, x_hbm, w_hbm,
    keep, mid, end, mid2, fin, act2, act3, w2, w3,
    base, land_mid, land_end, act0, act1, w0, w1, flat, send_row, send_col, recv_row, recv_side,
    load_sem, part_send, part_recv, pass_send, pass_recv, send_sem, recv_sem, later,
):
    nrows, ncols, step_size = sizes
    halves, high = base.shape[:2]
    rows_here, cols_here = keep.shape[:2]
    depth, row, col = lax.axis_index("depth"), lax.axis_index("rows"), lax.axis_index("cols")
    shape, place = (halves, rows_here, cols_here), (nrows, ncols, row, col)
    partner = (1 - depth, row, col)
    corner = HALO * HALO
    barrier = pltpu.get_barrier_semaphore()

    def lanes(c):
        return pl.ds(c * LANES, LANES)

    def local(src, dst, k):
        return pltpu.make_async_copy(src, dst, load_sem.at[k])

    def to_partner(src, dst, k, sems=(part_send, part_recv)):
        return pltpu.make_async_remote_copy(
            src_ref=src, dst_ref=dst, send_sem=sems[0].at[k], recv_sem=sems[1].at[k],
            device_id=partner, device_id_type=MESH,
        )

    def exists_at(step):
        there_row, there_col = row + step[0], col + step[1]
        exists = (there_row >= 0) & (there_row < nrows) & (there_col >= 0) & (there_col < ncols)
        return exists, there_row, there_col

    odd, even = lax.rem(row, 2) == 1, lax.rem(row, 2) == 0

    def pick(step, always, sometimes, first, second):
        if step == always:
            return True, None
        if step in sometimes:
            return first, second
        return None, True

    def early(step):
        return pick(step, (0, -1), ((-1, 0), (-1, -1)), odd, even)

    def early_seen_by(step):
        return pick(step, (0, 1), ((1, 0), (1, 1)), even, odd)

    def run_if(exists, also, action):
        if also is True:
            pl.when(exists)(action)
        elif also is not None:
            pl.when(exists)(lambda: pl.when(also)(action))

    def count_of(part):
        count = jnp.int32(1)
        for step in DIRECTIONS:
            also = early(step)[part]
            if also is not None:
                there = exists_at(step)[0]
                there = there if also is True else there & also
                count = count + jnp.where(there, 1, 0)
        return count

    def own(c):
        return base.at[c, pl.ds(HALO, rows_here), pl.ds(LEFT, cols_here), :]

    x_loads = [local(x_hbm.at[0, :, :, lanes(c)], own(c), c) for c in range(halves)]
    x_parts = [to_partner(x_hbm.at[0, :, :, lanes(c)], own(c), c) for c in range(halves)]
    keep_load = local(x_hbm.at[0], keep, halves + 2)
    w_loads = [local(w_hbm.at[0], w0, halves), local(w_hbm.at[1], w1, halves + 1)]
    late_loads = [local(w_hbm.at[0], w2, 0), local(w_hbm.at[1], w3, 1)]
    w_parts = [to_partner(w_hbm.at[0], w0, halves), to_partner(w_hbm.at[1], w1, halves + 1)]

    def inner(ref, k):
        return ref.at[:, pl.ds(HALO + k, rows_here - 2 * k), pl.ds(LEFT, cols_here), :]

    mid_part = to_partner(inner(mid, 1), inner(land_mid, 1), halves + 2)
    end_part = to_partner(inner(end, 2), inner(land_end, 2), halves + 3)
    passes = [
        to_partner(ref, ref, k, (pass_send, pass_recv)) for k, ref in enumerate((recv_row, recv_side))
    ]

    def activate_rows(source, target, first, rows, copied=None):
        def body(i, _):
            for c in range(halves):
                u = source[c, i, LEFT : LEFT + cols_here, :]
                target[c, i, LEFT : LEFT + cols_here, :] = silu(u)
                if copied is not None:
                    copied[c, i, LEFT : LEFT + cols_here, :] = u
            return 0

        lax.fori_loop(first, first + rows, body, 0, unroll=2)

    copies = []
    for k, (dr, dc) in enumerate(DIRECTIONS):
        exists, there_row, there_col = exists_at((dr, dc))
        side = (dc + 1) // 2
        mine = {-1: (0, corner), 1: ((rows_here - HALO) * HALO, corner), 0: (0, rows_here * HALO)}[dr]
        theirs = {1: (0, corner), -1: (high * HALO - corner, corner), 0: (corner, rows_here * HALO)}[dr]
        if dc == 0:
            src, dst, here = send_row.at[(dr + 1) // 2], recv_row.at[(1 - dr) // 2], recv_row.at[(dr + 1) // 2]
            empty = (recv_row, (dr + 1) // 2, slice(None))
        else:
            back = {-1: (0, corner), 1: (high * HALO - corner, corner), 0: (corner, rows_here * HALO)}[dr]
            src = send_col.at[side, pl.ds(*mine)]
            dst = recv_side.at[1 - side, pl.ds(*theirs)]
            here = recv_side.at[side, pl.ds(*back)]
            empty = (recv_side, side, slice(back[0], back[0] + back[1]))

        def remote(src, dst, slot):
            return pltpu.make_async_remote_copy(
                src_ref=src, dst_ref=dst, send_sem=send_sem.at[k], recv_sem=recv_sem.at[slot],
                device_id=(1 - depth, there_row, there_col), device_id_type=MESH,
            )

        opposite = DIRECTIONS.index((-dr, -dc))
        copies.append((exists, remote(src, dst, opposite), remote(src, here, k), empty))
    order = (4, 5, 6, 7, 2, 3, 0, 1)

    def signal(target):
        pl.semaphore_signal(barrier, inc=1, device_id=target, device_id_type=MESH)

    def send_halos(part):
        for k in order:
            exists, copy, _, _ = copies[k]
            run_if(exists, early(DIRECTIONS[k])[part], copy.start)

    @pl.when(depth == 0)
    def _():
        for copy in x_loads + w_loads:
            copy.start()
        signal(partner)
        pl.semaphore_wait(barrier, count_of(0))
        for copy in x_parts + w_parts[:1]:
            copy.start()
        for copy in x_loads:
            copy.wait()
        for side in range(2):
            top = HALO if side == 0 else rows_here
            left = LEFT if side == 0 else LEFT + cols_here - HALO
            for c in range(halves):
                send_row[side, :, lanes(c)] = as_rows(base[c, top : top + HALO, LEFT : LEFT + cols_here, :])
                for i in range(rows_here):
                    flat[side, c, i * HALO : (i + 1) * HALO, :] = base[c, HALO + i, left : left + HALO, :]
            for c in range(halves):
                send_col[side, :, lanes(c)] = flat[side, c, 0 : rows_here * HALO, :].astype(jnp.bfloat16)
        send_halos(0)
        activate_rows(base, act0, HALO, rows_here)
        w_loads[0].wait()
        interior(0, act0, w0, base, mid, act1, step_size, shape)
        mid_part.start()
        first = (row == 0) & (col == 0)

        def send_rest():
            pl.semaphore_wait(later.at[0], 1)
            send_halos(1)

        pl.when(row + col > 0)(send_rest)
        keep_load.start()
        w_loads[1].wait()
        interior(1, act1, w1, mid, end, act2, step_size, shape)
        end_part.start()
        pl.when(first)(send_rest)
        mid_part.wait_send()
        end_part.wait_send()
        w_parts[1].start()
        for copy in passes:
            copy.wait_recv()

    @pl.when(depth == 1)
    def _():
        for copy in late_loads:
            copy.start()
        signal(partner)
        for step in DIRECTIONS:
            exists, there_row, there_col = exists_at(step)
            for side, also in enumerate(early_seen_by(step)):
                core = 1 - depth if side == 0 else depth
                run_if(exists, also, functools.partial(signal, (core, there_row, there_col)))
        for step, (_, _, _, (ref, at, rows)) in zip(DIRECTIONS, copies):
            _, there_row, there_col = exists_at(step)
            outside = (there_row < 0) | (there_row >= nrows) | (there_col < 0) | (there_col >= ncols)

            @pl.when(outside)
            def _(ref=ref, at=at, rows=rows):
                ref[at, rows, :] = jnp.zeros_like(ref[at, rows, :])

        pl.semaphore_wait(barrier, count_of(1))
        pl.semaphore_signal(later.at[0], inc=1, device_id=partner, device_id_type=MESH)
        for copy in x_parts:
            copy.wait_recv()
        activate_rows(base, act0, HALO, rows_here)
        mid_part.wait_recv()
        activate_rows(land_mid, act1, HALO + 1, rows_here - 2, mid)
        end_part.wait_recv()
        activate_rows(land_end, act2, HALO + 2, rows_here - 4, end)
        late_loads[0].wait()
        interior(2, act2, w2, end, mid2, act3, step_size, shape)
        late_loads[1].wait()
        interior(3, act3, w3, mid2, fin, None, step_size, shape)
        for k in (0, 1, 2, 3, 4, 5, 6, 7):
            exists, _, arrival, _ = copies[k]
            pl.when(exists)(arrival.wait_recv)
        for copy in passes:
            copy.start()
        w_parts[0].wait_recv()

    for side in range(2):
        for c in range(halves):
            flat[side, c, 8 : 8 + high * HALO, :] = recv_side[side, :, lanes(c)].astype(jnp.float32)
            u = recv_row[side, :, lanes(c)].astype(jnp.float32).reshape(HALO, cols_here, LANES)
            rows = slice(0, HALO) if side == 0 else slice(high - HALO, high)
            base[c, rows, LEFT : LEFT + cols_here, :] = u
            act0[c, rows, LEFT : LEFT + cols_here, :] = silu(u)
    for i in range(high):
        for c in range(halves):
            at = 8 + i * HALO
            u = jnp.where(upper_sublanes(1)[0], flat[0, c, at : at + 8, :], flat[1, c, at - HALO : at + HALO, :])
            value = silu(u)
            for ref, v in ((base, u), (act0, value)):
                ref[c, i, LEFT - HALO : LEFT, :] = v[0:HALO]
                ref[c, i, LEFT + cols_here : LEFT + cols_here + HALO, :] = v[HALO:8]
    ring(0, act0, w0, base, mid, act1, step_size, shape, place)

    @pl.when(depth == 1)
    def _():
        w_parts[1].wait_recv()

    ring(1, act1, w1, mid, end, act2, step_size, shape, place)

    @pl.when(depth == 0)
    def _():
        keep_load.wait()
        for copy in x_parts + w_parts:
            copy.wait_send()
        for exists, copy, _, _ in copies:
            pl.when(exists)(copy.wait_send)

    @pl.when(depth == 1)
    def _():
        for copy in passes:
            copy.wait_send()


def ring_kernel(
    sizes, keep, mid, end, act2, w2, w3, mid2_in, fin_in, act3_in,
    fine_hbm, coarse_hbm, mid2, fin, act3, store_sem, keep_sem,
):
    nrows, ncols, step_size = sizes
    halves = end.shape[0]
    rows_here, cols_here = fine_hbm.shape[1:3]
    depth, row, col = lax.axis_index("depth"), lax.axis_index("rows"), lax.axis_index("cols")
    shape, place = (halves, rows_here, cols_here), (nrows, ncols, row, col)

    def stores(ref, target, slot):
        return [
            pltpu.make_async_copy(
                ref.at[c, pl.ds(HALO, rows_here), pl.ds(LEFT, cols_here), :],
                target.at[:, :, pl.ds(c * LANES, LANES)],
                store_sem.at[slot, c],
            )
            for c in range(halves)
        ]

    def start(copies):
        for copy in copies:
            copy.start()

    @pl.when(depth == 0)
    def _():
        kept = pltpu.make_async_copy(keep, coarse_hbm.at[0], keep_sem.at[0])
        both = stores(mid, fine_hbm.at[0], 0) + stores(end, fine_hbm.at[1], 1)
        start([kept] + both)
        for copy in [kept] + both:
            copy.wait()

    @pl.when(depth == 1)
    def _():
        early = stores(end, coarse_hbm.at[0], 0)
        start(early)
        ring(2, act2, w2, end, mid2, act3, step_size, shape, place)
        middle = stores(mid2, fine_hbm.at[0], 1)
        start(middle)
        ring(3, act3, w3, mid2, fin, None, step_size, shape, place)
        late = stores(fin, fine_hbm.at[1], 2)
        start(late)
        for copy in early + middle + late:
            copy.wait()


def two_sections(section_states, weights):
    _, rows_here, cols_here, channels = section_states.shape
    halves = channels // LANES
    high, wide = rows_here + 2 * HALO, cols_here + 2 * LEFT
    sizes = (lax.axis_size("rows"), lax.axis_size("cols"), 2.0 / (2 * lax.axis_size("depth")))
    f32, bf16, vmem = jnp.float32, jnp.bfloat16, pltpu.VMEM
    state = vmem((halves, high, wide, LANES), f32)
    weight = vmem((9 * channels, channels), bf16)
    flat_weights = weights.reshape(2, 9 * channels, channels)
    any_space, in_vmem = pl.BlockSpec(memory_space=pl.ANY), pl.BlockSpec(memory_space=vmem)
    dma = pltpu.SemaphoreType.DMA
    kept = vmem((rows_here, cols_here, channels), f32)
    keep, mid, end, mid2, fin, act2, act3, w2, w3 = pl.pallas_call(
        functools.partial(gather_kernel, sizes),
        out_shape=(kept,) + (state,) * 6 + (weight,) * 2,
        in_specs=[pl.BlockSpec(memory_space=pltpu.HBM)] * 2,
        out_specs=[in_vmem] * 9,
        scratch_shapes=[
            state, state, state, state, state, weight, weight,
            vmem((2, halves, high * HALO + 16, LANES), f32),
            vmem((2, HALO * cols_here, channels), bf16),
            vmem((2, rows_here * HALO, channels), bf16),
            vmem((2, HALO * cols_here, channels), bf16),
            vmem((2, high * HALO, channels), bf16),
            dma((halves + 3,)), dma((halves + 4,)), dma((halves + 4,)),
            dma((2,)), dma((2,)), dma((8,)), dma((8,)),
            pltpu.SemaphoreType.REGULAR((1,)),
        ],
        compiler_params=pltpu.CompilerParams(
            collective_id=0, has_side_effects=True, vmem_limit_bytes=LIMIT
        ),
    )(
        pltpu.with_memory_space_constraint(section_states, pltpu.HBM),
        pltpu.with_memory_space_constraint(flat_weights, pltpu.HBM),
    )
    outs = pl.pallas_call(
        functools.partial(ring_kernel, sizes),
        out_shape=(
            jax.ShapeDtypeStruct((2, rows_here, cols_here, channels), f32),
            jax.ShapeDtypeStruct((1, rows_here, cols_here, channels), f32),
        ) + (state,) * 3,
        in_specs=[in_vmem] * 9,
        out_specs=[any_space] * 2 + [in_vmem] * 3,
        input_output_aliases={6: 2, 7: 3, 8: 4},
        scratch_shapes=[dma((3, halves)), dma((1,))],
        compiler_params=pltpu.CompilerParams(vmem_limit_bytes=LIMIT),
    )(keep, mid, end, act2, w2, w3, mid2, fin, act3)
    return outs[0], outs[1]


def on_device(section_states, weights):
    _, rows_here, cols_here, channels = section_states.shape
    tiles = rows_here % 8 == 0 and cols_here % 8 == 0 and channels % LANES == 0
    if lax.axis_size("depth") == 2 and tiles and min(rows_here, cols_here) >= 16:
        return two_sections(section_states, weights)
    return chain_on_device(section_states, weights)


def solution(mesh):
    in_specs = (P("depth", "rows", "cols", None), P("depth", None, None, None, None))
    out_specs = (P("depth", "rows", "cols", None), P("depth", "rows", "cols", None))
    return jax.shard_map(
        on_device, mesh=mesh, in_specs=in_specs, out_specs=out_specs, check_vma=False
    )
```

```python
import functools

import jax
import jax.numpy as jnp
from jax import lax
from jax.experimental import pallas as pl
from jax.experimental.pallas import tpu as pltpu
from jax.sharding import PartitionSpec as P

MESH = pl.DeviceIdType.MESH
HALO = 4
LANES = 128
LIMIT = 32 * 1024 * 1024


def padded_2(shard, sides, width):
    for axis, dim in sides:
        size, length = (lax.axis_size(axis), shard.shape[dim])
        up = [(i, (i + 1) % size) for i in range(size - 1)]
        down = [(j, i) for i, j in up]
        last = lax.slice_in_dim(shard, length - width, length, axis=dim)
        initial = lax.slice_in_dim(shard, 0, width, axis=dim)
        before = lax.ppermute(last, axis, up)
        after = lax.ppermute(initial, axis, down)
        shard = jnp.concatenate([before, shard, after], axis=dim)
    return shard


def shifted_2(block, axis, distance):
    devices = range(lax.axis_size(axis))
    route = [(i - distance, i) for i in devices if i - distance in devices]
    return lax.ppermute(block, axis, route)


def activate(field):
    return jax.nn.silu(field).astype(jnp.bfloat16)


def apply_stencil(padded, flat_weight, out_rows, out_cols):
    channels = padded.shape[2]
    patches = jnp.concatenate(
        [
            padded[shift_row : shift_row + out_rows, shift_col : shift_col + out_cols]
            for shift_row in range(3)
            for shift_col in range(3)
        ],
        axis=2,
    )
    summed = jnp.dot(
        patches.reshape(out_rows * out_cols, 9 * channels),
        flat_weight,
        preferred_element_type=jnp.float32,
    )
    return summed.reshape(out_rows, out_cols, channels)


def section_pass(anchor, first_weight, second_weight, step_size):
    rows_here, cols_here, channels = anchor.shape
    widened = padded_2(anchor, (("rows", 0), ("cols", 1)), 2)
    slope_wide = apply_stencil(activate(widened), first_weight, rows_here + 2, cols_here + 2)
    middle_wide = widened[1:-1, 1:-1] + step_size * slope_wide
    row_global = lax.axis_index("rows") * rows_here - 1 + jnp.arange(rows_here + 2)
    col_global = lax.axis_index("cols") * cols_here - 1 + jnp.arange(cols_here + 2)
    inside_rows = (row_global >= 0) & (row_global < rows_here * lax.axis_size("rows"))
    inside_cols = (col_global >= 0) & (col_global < cols_here * lax.axis_size("cols"))
    inside = inside_rows[:, None] & inside_cols[None, :]
    second_act = jnp.where(inside[:, :, None], activate(middle_wide), jnp.zeros((), jnp.bfloat16))
    first_slope = slope_wide[1:-1, 1:-1]
    middle = middle_wide[1:-1, 1:-1]
    second_slope = apply_stencil(second_act, second_weight, rows_here, cols_here)
    ending = middle + step_size * second_slope
    return (first_slope, middle, ending)


def chain_on_device(section_states, weights):
    rows_here, cols_here, channels = section_states.shape[1:]
    ndepth = lax.axis_size("depth")
    position = lax.axis_index("depth")
    step_size = 2.0 / (2 * ndepth)
    first_weight = weights[0].reshape(9 * channels, channels)
    second_weight = weights[1].reshape(9 * channels, channels)
    anchor = section_states[0]
    first_slope, middle, ending = section_pass(anchor, first_weight, second_weight, step_size)
    jump = ending - (anchor + 2.0 * step_size * first_slope)

    def chain_turn(step_index, current):
        padded = padded_2(activate(current), (("rows", 0), ("cols", 1)), 1)
        advanced = (
            current
            + 2.0 * step_size * apply_stencil(padded, first_weight, rows_here, cols_here)
            + jump
        )
        shifted = shifted_2(advanced, "depth", 1)
        return jnp.where(position == 0, anchor, shifted)

    corrected = lax.fori_loop(0, ndepth - 1, chain_turn, anchor)
    final_slope, final_middle, final_ending = section_pass(
        corrected, first_weight, second_weight, step_size
    )
    fine_states = jnp.stack([final_middle, final_ending])
    return (fine_states, corrected[None])


DIRECTIONS = ((-1, 0), (1, 0), (0, -1), (0, 1), (-1, -1), (-1, 1), (1, -1), (1, 1))
LEFT = 8


def silu(u):
    half = 0.5 * u
    return half + half * jnp.tanh(half)


def as_rows(block):
    return block.reshape(-1, LANES).astype(jnp.bfloat16)


def tap_dot(windows, halves, weight):
    lhs = []
    for a in range(3):
        for b in range(3):
            for c in range(halves):
                parts = [as_rows(window(c, a, b)) for window in windows]
                lhs.append(parts[0] if len(parts) == 1 else jnp.concatenate(parts, axis=0))
    return jnp.dot(jnp.concatenate(lhs, axis=1), weight[...], preferred_element_type=jnp.float32)


def lanes_of(block, c, shape):
    return block[:, c * LANES : (c + 1) * LANES].reshape(shape)


def upper_sublanes(rows):
    return lax.broadcasted_iota(jnp.int32, (rows, 8, LANES), 1) < HALO


def packed(ref, c, first_row, rows, left, right):
    near = ref[c, pl.ds(first_row, rows), left : left + 8, :]
    far = ref[c, pl.ds(first_row, rows), right : right + 8, :]
    return jnp.where(upper_sublanes(rows), near, far)


def store_packed(ref, c, first_row, left, right, value):
    whole = pl.ds(first_row, value.shape[0])
    ref[c, whole, left : left + HALO, :] = value[:, 0:HALO]
    ref[c, whole, right + HALO : right + 8, :] = value[:, HALO:8]


def largest_divisor(total, limit):
    return max(n for n in range(1, limit + 1) if total % n == 0)


def interior(layer, act, weight, before, after, act_after, step_size, shape):
    halves, rows_here, cols_here = shape
    narrow = layer == 3 and cols_here == 16
    left, wide = (LEFT + HALO, cols_here - 2 * HALO) if narrow else (LEFT, cols_here)
    exact = layer >= 2
    first, rows = (HALO + 1 + layer, rows_here - 2 - 2 * layer) if exact else (HALO + 1, rows_here - 2)
    n = rows if exact else largest_divisor(rows, 10)

    def chunk(k, _):
        at = first + k * n

        def window(c, a, b):
            return act[c, pl.ds(at + a - 1, n), left + b - 1 : left + b - 1 + wide, :]

        acc = step_size * tap_dot([window], halves, weight)
        for c in range(halves):
            here = (c, pl.ds(at, n), slice(left, left + wide), slice(None))
            u = before[here] + lanes_of(acc, c, (n, wide, LANES))
            after[here] = u
            if act_after is not None:
                act_after[here] = silu(u)
        return 0

    lax.fori_loop(0, rows // n, chunk, 0)


def ring(layer, act, weight, before, after, act_after, step_size, shape, place, done=None):
    halves, rows_here, cols_here = shape
    nrows, ncols, row, col = place
    high = rows_here + 2 * HALO
    first, rows = 1 + layer, high - 2 - 2 * layer
    n = (rows + 3) // 4 * 2
    narrow = layer == 3 and cols_here == 16
    left, wide = (LEFT + HALO, cols_here - 2 * HALO) if narrow else (LEFT, cols_here)
    near, far = HALO + layer, LEFT + cols_here - 6 - layer
    above = jnp.where(row > 0, 1.0, 0.0)
    below = jnp.where(row < nrows - 1, 1.0, 0.0)
    sub = lax.broadcasted_iota(jnp.int32, (1, 8, LANES), 1)
    j = jnp.where(sub < HALO, sub + (layer - 3), sub + (cols_here - 5 - layer)) + col * cols_here
    held = jnp.where((j >= 0) & (j < ncols * cols_here), 1.0, 0.0)
    m = HALO * wide

    def rows_held(at, block):
        i = lax.broadcasted_iota(jnp.int32, block, 0) + at
        return jnp.where(i < HALO, above, jnp.where(i >= high - HALO, below, 1.0))

    def chunk(k, _):
        top = first + k * (high - HALO - 2 * first)
        at = first + k * (rows - n)

        def strip(c, a, b):
            return act[c, pl.ds(top + a - 1, HALO), left + b - 1 : left + b - 1 + wide, :]

        def sides(c, a, b):
            return packed(act, c, at + a - 1, n, near + b, far + b)

        acc = step_size * tap_dot([strip, sides], halves, weight)
        for c in range(halves):
            here = (c, pl.ds(top, HALO), slice(left, left + wide), slice(None))
            u = before[here] + lanes_of(acc[:m], c, (HALO, wide, LANES))
            after[here] = u
            if act_after is not None:
                act_after[here] = silu(u) * rows_held(top, u.shape)
            u = packed(before, c, at, n, near + 1, far + 1) + lanes_of(acc[m:], c, (n, 8, LANES))
            store_packed(after, c, at, near + 1, far + 1, u)
            if act_after is not None:
                value = silu(u) * (held * rows_held(at, u.shape))
                store_packed(act_after, c, at, near + 1, far + 1, value)
        if done is not None:
            done(k)
        return 0

    lax.fori_loop(0, 2, chunk, 0)


def gather_kernel(
    sizes, x_hbm, w_hbm,
    keep, mid, end, mid2, fin, act2, act3, w2, w3,
    base, land_mid, land_end, act0, act1, w0, w1, flat, send_row, send_col, recv_row, recv_side,
    load_sem, part_send, part_recv, pass_send, pass_recv, send_sem, recv_sem, later,
):
    nrows, ncols, step_size = sizes
    halves, high = base.shape[:2]
    rows_here, cols_here = keep.shape[:2]
    depth, row, col = lax.axis_index("depth"), lax.axis_index("rows"), lax.axis_index("cols")
    shape, place = (halves, rows_here, cols_here), (nrows, ncols, row, col)
    partner = (1 - depth, row, col)
    corner = HALO * HALO
    barrier = pltpu.get_barrier_semaphore()

    def lanes(c):
        return pl.ds(c * LANES, LANES)

    def local(src, dst, k):
        return pltpu.make_async_copy(src, dst, load_sem.at[k])

    def to_partner(src, dst, k, sems=(part_send, part_recv)):
        return pltpu.make_async_remote_copy(
            src_ref=src, dst_ref=dst, send_sem=sems[0].at[k], recv_sem=sems[1].at[k],
            device_id=partner, device_id_type=MESH,
        )

    def exists_at(step):
        there_row, there_col = row + step[0], col + step[1]
        exists = (there_row >= 0) & (there_row < nrows) & (there_col >= 0) & (there_col < ncols)
        return exists, there_row, there_col

    odd, even = lax.rem(row, 2) == 1, lax.rem(row, 2) == 0

    def pick(step, always, sometimes, first, second):
        if step == always:
            return True, None
        if step in sometimes:
            return first, second
        return None, True

    def early(step):
        return pick(step, (0, -1), ((-1, 0), (-1, -1)), odd, even)

    def early_seen_by(step):
        return pick(step, (0, 1), ((1, 0), (1, 1)), even, odd)

    def run_if(exists, also, action):
        if also is True:
            pl.when(exists)(action)
        elif also is not None:
            pl.when(exists)(lambda: pl.when(also)(action))

    def count_of(part):
        count = jnp.int32(1)
        for step in DIRECTIONS:
            also = early(step)[part]
            if also is not None:
                there = exists_at(step)[0]
                there = there if also is True else there & also
                count = count + jnp.where(there, 1, 0)
        return count

    def own(c):
        return base.at[c, pl.ds(HALO, rows_here), pl.ds(LEFT, cols_here), :]

    x_loads = [local(x_hbm.at[0, :, :, lanes(c)], own(c), c) for c in range(halves)]
    x_parts = [to_partner(x_hbm.at[0, :, :, lanes(c)], own(c), c) for c in range(halves)]
    keep_load = local(x_hbm.at[0], keep, halves + 2)
    w_loads = [local(w_hbm.at[0], w0, halves), local(w_hbm.at[1], w1, halves + 1)]
    late_loads = [local(w_hbm.at[0], w2, 0), local(w_hbm.at[1], w3, 1)]
    w_parts = [to_partner(w_hbm.at[0], w0, halves), to_partner(w_hbm.at[1], w1, halves + 1)]

    def inner(ref, k):
        return ref.at[:, pl.ds(HALO + k, rows_here - 2 * k), pl.ds(LEFT, cols_here), :]

    mid_part = to_partner(inner(mid, 1), inner(land_mid, 1), halves + 2)
    end_part = to_partner(inner(end, 2), inner(land_end, 2), halves + 3)
    passes = [
        to_partner(ref, ref, k, (pass_send, pass_recv)) for k, ref in enumerate((recv_row, recv_side))
    ]

    def activate_rows(source, target, first, rows, copied=None):
        def body(i, _):
            for c in range(halves):
                u = source[c, i, LEFT : LEFT + cols_here, :]
                target[c, i, LEFT : LEFT + cols_here, :] = silu(u)
                if copied is not None:
                    copied[c, i, LEFT : LEFT + cols_here, :] = u
            return 0

        lax.fori_loop(first, first + rows, body, 0, unroll=2)

    copies = []
    for k, (dr, dc) in enumerate(DIRECTIONS):
        exists, there_row, there_col = exists_at((dr, dc))
        side = (dc + 1) // 2
        mine = {-1: (0, corner), 1: ((rows_here - HALO) * HALO, corner), 0: (0, rows_here * HALO)}[dr]
        theirs = {1: (0, corner), -1: (high * HALO - corner, corner), 0: (corner, rows_here * HALO)}[dr]
        if dc == 0:
            src, dst, here = send_row.at[(dr + 1) // 2], recv_row.at[(1 - dr) // 2], recv_row.at[(dr + 1) // 2]
            empty = (recv_row, (dr + 1) // 2, slice(None))
        else:
            back = {-1: (0, corner), 1: (high * HALO - corner, corner), 0: (corner, rows_here * HALO)}[dr]
            src = send_col.at[side, pl.ds(*mine)]
            dst = recv_side.at[1 - side, pl.ds(*theirs)]
            here = recv_side.at[side, pl.ds(*back)]
            empty = (recv_side, side, slice(back[0], back[0] + back[1]))

        def remote(src, dst, slot):
            return pltpu.make_async_remote_copy(
                src_ref=src, dst_ref=dst, send_sem=send_sem.at[k], recv_sem=recv_sem.at[slot],
                device_id=(1 - depth, there_row, there_col), device_id_type=MESH,
            )

        opposite = DIRECTIONS.index((-dr, -dc))
        copies.append((exists, remote(src, dst, opposite), remote(src, here, k), empty))
    order = (4, 5, 6, 7, 2, 3, 0, 1)

    def signal(target):
        pl.semaphore_signal(barrier, inc=1, device_id=target, device_id_type=MESH)

    def send_halos(part):
        for k in order:
            exists, copy, _, _ = copies[k]
            run_if(exists, early(DIRECTIONS[k])[part], copy.start)

    @pl.when(depth == 0)
    def _():
        for copy in x_loads + w_loads[:1]:
            copy.start()
        signal(partner)
        pl.semaphore_wait(barrier, count_of(0))
        for copy in x_parts + w_parts[:1]:
            copy.start()
        for copy in x_loads:
            copy.wait()
        w_loads[1].start()
        for side in range(2):
            top = HALO if side == 0 else rows_here
            left = LEFT if side == 0 else LEFT + cols_here - HALO
            for c in range(halves):
                send_row[side, :, lanes(c)] = as_rows(base[c, top : top + HALO, LEFT : LEFT + cols_here, :])
                for i in range(rows_here):
                    flat[side, c, i * HALO : (i + 1) * HALO, :] = base[c, HALO + i, left : left + HALO, :]
            for c in range(halves):
                send_col[side, :, lanes(c)] = flat[side, c, 0 : rows_here * HALO, :].astype(jnp.bfloat16)
        send_halos(0)
        activate_rows(base, act0, HALO, rows_here)
        w_loads[0].wait()
        interior(0, act0, w0, base, mid, act1, step_size, shape)
        mid_part.start()
        first = (row == 0) & (col == 0)

        def send_rest():
            pl.semaphore_wait(later.at[0], 1)
            send_halos(1)

        pl.when(row + col > 0)(send_rest)
        keep_load.start()
        w_loads[1].wait()
        interior(1, act1, w1, mid, end, act2, step_size, shape)
        end_part.start()
        pl.when(first)(send_rest)
        mid_part.wait_send()
        end_part.wait_send()
        w_parts[1].start()
        keep_load.wait()
        for exists, copy, _, _ in copies:
            pl.when(exists)(copy.wait_send)
        for copy in x_parts + w_parts:
            copy.wait_send()
        for copy in passes:
            copy.wait_recv()

    @pl.when(depth == 1)
    def _():
        for copy in late_loads:
            copy.start()
        signal(partner)
        for step in DIRECTIONS:
            exists, there_row, there_col = exists_at(step)
            for side, also in enumerate(early_seen_by(step)):
                core = 1 - depth if side == 0 else depth
                run_if(exists, also, functools.partial(signal, (core, there_row, there_col)))
        for step, (_, _, _, (ref, at, rows)) in zip(DIRECTIONS, copies):
            _, there_row, there_col = exists_at(step)
            outside = (there_row < 0) | (there_row >= nrows) | (there_col < 0) | (there_col >= ncols)

            @pl.when(outside)
            def _(ref=ref, at=at, rows=rows):
                ref[at, rows, :] = jnp.zeros_like(ref[at, rows, :])

        pl.semaphore_wait(barrier, count_of(1))
        pl.semaphore_signal(later.at[0], inc=1, device_id=partner, device_id_type=MESH)
        for copy in x_parts:
            copy.wait_recv()
        activate_rows(base, act0, HALO, rows_here)
        mid_part.wait_recv()
        activate_rows(land_mid, act1, HALO + 1, rows_here - 2, mid)
        end_part.wait_recv()
        activate_rows(land_end, act2, HALO + 2, rows_here - 4, end)
        late_loads[0].wait()
        interior(2, act2, w2, end, mid2, act3, step_size, shape)
        late_loads[1].wait()
        interior(3, act3, w3, mid2, fin, None, step_size, shape)
        for k in (0, 1, 2, 3, 4, 5, 6, 7):
            exists, _, arrival, _ = copies[k]
            pl.when(exists)(arrival.wait_recv)
        for copy in passes:
            copy.start()
        w_parts[0].wait_recv()

    for side in range(2):
        for c in range(halves):
            flat[side, c, 8 : 8 + high * HALO, :] = recv_side[side, :, lanes(c)].astype(jnp.float32)
            u = recv_row[side, :, lanes(c)].astype(jnp.float32).reshape(HALO, cols_here, LANES)
            rows = slice(0, HALO) if side == 0 else slice(high - HALO, high)
            base[c, rows, LEFT : LEFT + cols_here, :] = u
            act0[c, rows, LEFT : LEFT + cols_here, :] = silu(u)
    for i in range(high):
        for c in range(halves):
            at = 8 + i * HALO
            u = jnp.where(upper_sublanes(1)[0], flat[0, c, at : at + 8, :], flat[1, c, at - HALO : at + HALO, :])
            value = silu(u)
            for ref, v in ((base, u), (act0, value)):
                ref[c, i, LEFT - HALO : LEFT, :] = v[0:HALO]
                ref[c, i, LEFT + cols_here : LEFT + cols_here + HALO, :] = v[HALO:8]
    ring(0, act0, w0, base, mid, act1, step_size, shape, place)

    @pl.when(depth == 1)
    def _():
        w_parts[1].wait_recv()
        for copy in passes:
            copy.wait_send()

    ring(1, act1, w1, mid, end, act2, step_size, shape, place)


def ring_kernel(
    sizes, keep, mid, end, act2, w2, w3, mid2_in, fin_in, act3_in,
    fine_hbm, coarse_hbm, mid2, fin, act3, store_sem, keep_sem, late_sem,
):
    nrows, ncols, step_size = sizes
    halves = end.shape[0]
    rows_here, cols_here = fine_hbm.shape[1:3]
    depth, row, col = lax.axis_index("depth"), lax.axis_index("rows"), lax.axis_index("cols")
    shape, place = (halves, rows_here, cols_here), (nrows, ncols, row, col)

    def stores(ref, target, slot):
        return [
            pltpu.make_async_copy(
                ref.at[c, pl.ds(HALO, rows_here), pl.ds(LEFT, cols_here), :],
                target.at[:, :, pl.ds(c * LANES, LANES)],
                store_sem.at[slot, c],
            )
            for c in range(halves)
        ]

    def start(copies):
        for copy in copies:
            copy.start()

    @pl.when(depth == 0)
    def _():
        kept = pltpu.make_async_copy(keep, coarse_hbm.at[0], keep_sem.at[0])
        both = stores(mid, fine_hbm.at[0], 0) + stores(end, fine_hbm.at[1], 1)
        start([kept] + both)
        for copy in [kept] + both:
            copy.wait()

    @pl.when(depth == 1)
    def _():
        early = stores(end, coarse_hbm.at[0], 0)
        start(early)
        ring(2, act2, w2, end, mid2, act3, step_size, shape, place)
        middle = stores(mid2, fine_hbm.at[0], 1)
        start(middle)

        def late(k, c):
            rows = rows_here // 2
            return pltpu.make_async_copy(
                fin.at[c, pl.ds(HALO + k * rows, rows), pl.ds(LEFT, cols_here), :],
                fine_hbm.at[1, pl.ds(k * rows, rows), :, pl.ds(c * LANES, LANES)],
                late_sem.at[k, c],
            )

        def send(k):
            for c in range(halves):
                late(k, c).start()

        ring(3, act3, w3, mid2, fin, None, step_size, shape, place, send)
        for copy in early + middle + [late(k, c) for k in range(2) for c in range(halves)]:
            copy.wait()


def two_sections(section_states, weights):
    _, rows_here, cols_here, channels = section_states.shape
    halves = channels // LANES
    high, wide = rows_here + 2 * HALO, cols_here + 2 * LEFT
    sizes = (lax.axis_size("rows"), lax.axis_size("cols"), 2.0 / (2 * lax.axis_size("depth")))
    f32, bf16, vmem = jnp.float32, jnp.bfloat16, pltpu.VMEM
    state = vmem((halves, high, wide, LANES), f32)
    weight = vmem((9 * channels, channels), bf16)
    flat_weights = weights.reshape(2, 9 * channels, channels)
    any_space, in_vmem = pl.BlockSpec(memory_space=pl.ANY), pl.BlockSpec(memory_space=vmem)
    dma = pltpu.SemaphoreType.DMA
    kept = vmem((rows_here, cols_here, channels), f32)
    keep, mid, end, mid2, fin, act2, act3, w2, w3 = pl.pallas_call(
        functools.partial(gather_kernel, sizes),
        out_shape=(kept,) + (state,) * 6 + (weight,) * 2,
        in_specs=[pl.BlockSpec(memory_space=pltpu.HBM)] * 2,
        out_specs=[in_vmem] * 9,
        scratch_shapes=[
            state, state, state, state, state, weight, weight,
            vmem((2, halves, high * HALO + 16, LANES), f32),
            vmem((2, HALO * cols_here, channels), bf16),
            vmem((2, rows_here * HALO, channels), bf16),
            vmem((2, HALO * cols_here, channels), bf16),
            vmem((2, high * HALO, channels), bf16),
            dma((halves + 3,)), dma((halves + 4,)), dma((halves + 4,)),
            dma((2,)), dma((2,)), dma((8,)), dma((8,)),
            pltpu.SemaphoreType.REGULAR((1,)),
        ],
        compiler_params=pltpu.CompilerParams(
            collective_id=0, has_side_effects=True, vmem_limit_bytes=LIMIT
        ),
    )(
        pltpu.with_memory_space_constraint(section_states, pltpu.HBM),
        pltpu.with_memory_space_constraint(flat_weights, pltpu.HBM),
    )
    outs = pl.pallas_call(
        functools.partial(ring_kernel, sizes),
        out_shape=(
            jax.ShapeDtypeStruct((2, rows_here, cols_here, channels), f32),
            jax.ShapeDtypeStruct((1, rows_here, cols_here, channels), f32),
        ) + (state,) * 3,
        in_specs=[in_vmem] * 9,
        out_specs=[any_space] * 2 + [in_vmem] * 3,
        input_output_aliases={6: 2, 7: 3, 8: 4},
        scratch_shapes=[dma((2, halves)), dma((1,)), dma((2, halves))],
        compiler_params=pltpu.CompilerParams(vmem_limit_bytes=LIMIT),
    )(keep, mid, end, act2, w2, w3, mid2, fin, act3)
    return outs[0], outs[1]


def on_device(section_states, weights):
    _, rows_here, cols_here, channels = section_states.shape
    tiles = rows_here % 8 == 0 and cols_here % 8 == 0 and channels % LANES == 0
    if lax.axis_size("depth") == 2 and tiles and min(rows_here, cols_here) >= 16:
        return two_sections(section_states, weights)
    return chain_on_device(section_states, weights)


def solution(mesh):
    in_specs = (P("depth", "rows", "cols", None), P("depth", None, None, None, None))
    out_specs = (P("depth", "rows", "cols", None), P("depth", "rows", "cols", None))
    return jax.shard_map(
        on_device, mesh=mesh, in_specs=in_specs, out_specs=out_specs, check_vma=False
    )
```

```python
import functools

import jax
import jax.numpy as jnp
from jax import lax
from jax.experimental import pallas as pl
from jax.experimental.pallas import tpu as pltpu
from jax.sharding import PartitionSpec as P

MESH = pl.DeviceIdType.MESH
HALO = 4
LANES = 128
LIMIT = 32 * 1024 * 1024


def padded_2(shard, sides, width):
    for axis, dim in sides:
        size, length = (lax.axis_size(axis), shard.shape[dim])
        up = [(i, (i + 1) % size) for i in range(size - 1)]
        down = [(j, i) for i, j in up]
        last = lax.slice_in_dim(shard, length - width, length, axis=dim)
        initial = lax.slice_in_dim(shard, 0, width, axis=dim)
        before = lax.ppermute(last, axis, up)
        after = lax.ppermute(initial, axis, down)
        shard = jnp.concatenate([before, shard, after], axis=dim)
    return shard


def shifted_2(block, axis, distance):
    devices = range(lax.axis_size(axis))
    route = [(i - distance, i) for i in devices if i - distance in devices]
    return lax.ppermute(block, axis, route)


def activate(field):
    return jax.nn.silu(field).astype(jnp.bfloat16)


def apply_stencil(padded, flat_weight, out_rows, out_cols):
    channels = padded.shape[2]
    patches = jnp.concatenate(
        [
            padded[shift_row : shift_row + out_rows, shift_col : shift_col + out_cols]
            for shift_row in range(3)
            for shift_col in range(3)
        ],
        axis=2,
    )
    summed = jnp.dot(
        patches.reshape(out_rows * out_cols, 9 * channels),
        flat_weight,
        preferred_element_type=jnp.float32,
    )
    return summed.reshape(out_rows, out_cols, channels)


def section_pass(anchor, first_weight, second_weight, step_size):
    rows_here, cols_here, channels = anchor.shape
    widened = padded_2(anchor, (("rows", 0), ("cols", 1)), 2)
    slope_wide = apply_stencil(activate(widened), first_weight, rows_here + 2, cols_here + 2)
    middle_wide = widened[1:-1, 1:-1] + step_size * slope_wide
    row_global = lax.axis_index("rows") * rows_here - 1 + jnp.arange(rows_here + 2)
    col_global = lax.axis_index("cols") * cols_here - 1 + jnp.arange(cols_here + 2)
    inside_rows = (row_global >= 0) & (row_global < rows_here * lax.axis_size("rows"))
    inside_cols = (col_global >= 0) & (col_global < cols_here * lax.axis_size("cols"))
    inside = inside_rows[:, None] & inside_cols[None, :]
    second_act = jnp.where(inside[:, :, None], activate(middle_wide), jnp.zeros((), jnp.bfloat16))
    first_slope = slope_wide[1:-1, 1:-1]
    middle = middle_wide[1:-1, 1:-1]
    second_slope = apply_stencil(second_act, second_weight, rows_here, cols_here)
    ending = middle + step_size * second_slope
    return (first_slope, middle, ending)


def chain_on_device(section_states, weights):
    rows_here, cols_here, channels = section_states.shape[1:]
    ndepth = lax.axis_size("depth")
    position = lax.axis_index("depth")
    step_size = 2.0 / (2 * ndepth)
    first_weight = weights[0].reshape(9 * channels, channels)
    second_weight = weights[1].reshape(9 * channels, channels)
    anchor = section_states[0]
    first_slope, middle, ending = section_pass(anchor, first_weight, second_weight, step_size)
    jump = ending - (anchor + 2.0 * step_size * first_slope)

    def chain_turn(step_index, current):
        padded = padded_2(activate(current), (("rows", 0), ("cols", 1)), 1)
        advanced = (
            current
            + 2.0 * step_size * apply_stencil(padded, first_weight, rows_here, cols_here)
            + jump
        )
        shifted = shifted_2(advanced, "depth", 1)
        return jnp.where(position == 0, anchor, shifted)

    corrected = lax.fori_loop(0, ndepth - 1, chain_turn, anchor)
    final_slope, final_middle, final_ending = section_pass(
        corrected, first_weight, second_weight, step_size
    )
    fine_states = jnp.stack([final_middle, final_ending])
    return (fine_states, corrected[None])


DIRECTIONS = ((-1, 0), (1, 0), (0, -1), (0, 1), (-1, -1), (-1, 1), (1, -1), (1, 1))
LEFT = 8


def silu(u):
    half = 0.5 * u
    return half + half * jnp.tanh(half)


def as_rows(block):
    return block.reshape(-1, LANES).astype(jnp.bfloat16)


def tap_dot(windows, halves, weight):
    lhs = []
    for a in range(3):
        for b in range(3):
            for c in range(halves):
                parts = [as_rows(window(c, a, b)) for window in windows]
                lhs.append(parts[0] if len(parts) == 1 else jnp.concatenate(parts, axis=0))
    return jnp.dot(jnp.concatenate(lhs, axis=1), weight[...], preferred_element_type=jnp.float32)


def lanes_of(block, c, shape):
    return block[:, c * LANES : (c + 1) * LANES].reshape(shape)


def upper_sublanes(rows):
    return lax.broadcasted_iota(jnp.int32, (rows, 8, LANES), 1) < HALO


def packed(ref, c, first_row, rows, left, right):
    near = ref[c, pl.ds(first_row, rows), left : left + 8, :]
    far = ref[c, pl.ds(first_row, rows), right : right + 8, :]
    return jnp.where(upper_sublanes(rows), near, far)


def store_packed(ref, c, first_row, left, right, value):
    whole = pl.ds(first_row, value.shape[0])
    ref[c, whole, left : left + HALO, :] = value[:, 0:HALO]
    ref[c, whole, right + HALO : right + 8, :] = value[:, HALO:8]


def largest_divisor(total, limit):
    return max(n for n in range(1, limit + 1) if total % n == 0)


def once():
    return jnp.minimum(lax.axis_index("rows"), 0) + 1


def interior(layer, act, weight, before, after, act_after, step_size, shape):
    halves, rows_here, cols_here = shape
    narrow = layer == 3 and cols_here == 16
    left, wide = (LEFT + HALO, cols_here - 2 * HALO) if narrow else (LEFT, cols_here)
    exact = layer >= 2
    first, rows = (HALO + 1 + layer, rows_here - 2 - 2 * layer) if exact else (HALO + 1, rows_here - 2)
    n = rows if exact else largest_divisor(rows, 30)

    def chunk(k, _):
        at = first + k * n

        def window(c, a, b):
            return act[c, pl.ds(at + a - 1, n), left + b - 1 : left + b - 1 + wide, :]

        acc = step_size * tap_dot([window], halves, weight)
        for c in range(halves):
            here = (c, pl.ds(at, n), slice(left, left + wide), slice(None))
            u = before[here] + lanes_of(acc, c, (n, wide, LANES))
            after[here] = u
            if act_after is not None:
                act_after[here] = silu(u)
        return 0

    lax.fori_loop(0, once() if rows == n else rows // n, chunk, 0)


def ring(layer, act, weight, before, after, act_after, step_size, shape, place):
    halves, rows_here, cols_here = shape
    nrows, ncols, row, col = place
    high = rows_here + 2 * HALO
    first, rows = 1 + layer, high - 2 - 2 * layer
    tops = (first, high - HALO - first)
    narrow = layer == 3 and cols_here == 16
    left, wide = (LEFT + HALO, cols_here - 2 * HALO) if narrow else (LEFT, cols_here)
    near, far = HALO + layer, LEFT + cols_here - 6 - layer
    above = jnp.where(row > 0, 1.0, 0.0)
    below = jnp.where(row < nrows - 1, 1.0, 0.0)
    sub = lax.broadcasted_iota(jnp.int32, (1, 8, LANES), 1)
    j = jnp.where(sub < HALO, sub + (layer - 3), sub + (cols_here - 5 - layer)) + col * cols_here
    held = jnp.where((j >= 0) & (j < ncols * cols_here), 1.0, 0.0)
    m = HALO * wide

    def rows_held(at, block):
        i = lax.broadcasted_iota(jnp.int32, block, 0) + at
        return jnp.where(i < HALO, above, jnp.where(i >= high - HALO, below, 1.0))

    def whole(_, carry):
        def strip(at):
            return lambda c, a, b: act[c, pl.ds(at + a - 1, HALO), left + b - 1 : left + b - 1 + wide, :]

        def sides(c, a, b):
            return packed(act, c, first + a - 1, rows, near + b, far + b)

        acc = step_size * tap_dot([strip(at) for at in tops] + [sides], halves, weight)
        for c in range(halves):
            for k, at in enumerate(tops):
                here = (c, pl.ds(at, HALO), slice(left, left + wide), slice(None))
                u = before[here] + lanes_of(acc[k * m : (k + 1) * m], c, (HALO, wide, LANES))
                after[here] = u
                if act_after is not None:
                    act_after[here] = silu(u) * rows_held(at, u.shape)
            u = packed(before, c, first, rows, near + 1, far + 1) + lanes_of(acc[2 * m :], c, (rows, 8, LANES))
            store_packed(after, c, first, near + 1, far + 1, u)
            if act_after is not None:
                value = silu(u) * (held * rows_held(first, u.shape))
                store_packed(act_after, c, first, near + 1, far + 1, value)
        return carry

    lax.fori_loop(0, once(), whole, 0)


def gather_kernel(
    sizes, x_hbm, w_hbm,
    keep, states, mid2, fin, acts, act3, w2, w3,
    land_mid, land_end, w01, flat, send_row, send_col, recv_row, recv_side,
    load_sem, part_sem, pass_sem, halo_sem, later,
):
    nrows, ncols, step_size = sizes
    base, mid, end = [states.at[k] for k in range(3)]
    act0, act1, act2 = [acts.at[k] for k in range(3)]
    w0, w1 = w01.at[0], w01.at[1]
    halves, high = land_mid.shape[:2]
    rows_here, cols_here = keep.shape[:2]
    depth, row, col = lax.axis_index("depth"), lax.axis_index("rows"), lax.axis_index("cols")
    shape, place = (halves, rows_here, cols_here), (nrows, ncols, row, col)
    partner = (1 - depth, row, col)
    corner = HALO * HALO
    barrier = pltpu.get_barrier_semaphore()

    def lanes(c):
        return pl.ds(c * LANES, LANES)

    def local(src, dst, k):
        return pltpu.make_async_copy(src, dst, load_sem.at[k])

    def to_partner(src, dst, k, sem=part_sem):
        return pltpu.make_async_remote_copy(
            src_ref=src, dst_ref=dst, send_sem=sem.at[k], recv_sem=sem.at[k],
            device_id=partner, device_id_type=MESH,
        )

    def exists_at(step):
        there_row, there_col = row + step[0], col + step[1]
        exists = (there_row >= 0) & (there_row < nrows) & (there_col >= 0) & (there_col < ncols)
        return exists, there_row, there_col

    odd, even = lax.rem(row, 2) == 1, lax.rem(row, 2) == 0

    def pick(step, always, sometimes, first, second):
        if step == always:
            return True, None
        if step in sometimes:
            return first, second
        return None, True

    def early(step):
        return pick(step, (0, -1), ((-1, 0), (-1, -1)), odd, even)

    def early_seen_by(step):
        return pick(step, (0, 1), ((1, 0), (1, 1)), even, odd)

    def run_if(exists, also, action):
        if also is True:
            pl.when(exists)(action)
        elif also is not None:
            pl.when(exists)(lambda: pl.when(also)(action))

    def count_of(part):
        count = jnp.int32(1)
        for step in DIRECTIONS:
            also = early(step)[part]
            if also is not None:
                there = exists_at(step)[0]
                there = there if also is True else there & also
                count = count + jnp.where(there, 1, 0)
        return count

    def own(c):
        return base.at[c, pl.ds(HALO, rows_here), pl.ds(LEFT, cols_here), :]

    x_loads = [local(x_hbm.at[0, :, :, lanes(c)], own(c), c) for c in range(halves)]
    x_parts = [to_partner(x_hbm.at[0, :, :, lanes(c)], own(c), c) for c in range(halves)]
    keep_load = local(x_hbm.at[0], keep, 1)
    w_loads = [local(w_hbm.at[0], w0, halves), local(w_hbm.at[1], w1, 0)]
    late_loads = [local(w_hbm.at[0], w2, 0), local(w_hbm.at[1], w3, 1)]
    w_parts = [to_partner(w_hbm.at[0], w0, halves), to_partner(w_hbm.at[1], w1, halves + 1)]

    def inner(ref, k):
        return ref.at[:, pl.ds(HALO + k, rows_here - 2 * k), pl.ds(LEFT, cols_here), :]

    mid_part = to_partner(inner(mid, 1), inner(land_mid, 1), halves + 2)
    end_part = to_partner(inner(end, 2), inner(land_end, 2), halves + 3)
    passes = [
        to_partner(ref, ref, k, pass_sem) for k, ref in enumerate((recv_row, recv_side))
    ]

    def activate_rows(source, target, first, rows, copied=None):
        def body(i, _):
            for c in range(halves):
                u = source[c, i, LEFT : LEFT + cols_here, :]
                target[c, i, LEFT : LEFT + cols_here, :] = silu(u)
                if copied is not None:
                    copied[c, i, LEFT : LEFT + cols_here, :] = u
            return 0

        lax.fori_loop(first, first + rows, body, 0, unroll=2)

    copies = []
    for k, (dr, dc) in enumerate(DIRECTIONS):
        exists, there_row, there_col = exists_at((dr, dc))
        side = (dc + 1) // 2
        mine = {-1: (0, corner), 1: ((rows_here - HALO) * HALO, corner), 0: (0, rows_here * HALO)}[dr]
        theirs = {1: (0, corner), -1: (high * HALO - corner, corner), 0: (corner, rows_here * HALO)}[dr]
        if dc == 0:
            src, dst, here = send_row.at[(dr + 1) // 2], recv_row.at[(1 - dr) // 2], recv_row.at[(dr + 1) // 2]
            empty = (recv_row, (dr + 1) // 2, slice(None))
        else:
            back = {-1: (0, corner), 1: (high * HALO - corner, corner), 0: (corner, rows_here * HALO)}[dr]
            src = send_col.at[side, pl.ds(*mine)]
            dst = recv_side.at[1 - side, pl.ds(*theirs)]
            here = recv_side.at[side, pl.ds(*back)]
            empty = (recv_side, side, slice(back[0], back[0] + back[1]))

        def remote(src, dst, slot):
            return pltpu.make_async_remote_copy(
                src_ref=src, dst_ref=dst, send_sem=halo_sem.at[k], recv_sem=halo_sem.at[slot],
                device_id=(1 - depth, there_row, there_col), device_id_type=MESH,
            )

        opposite = DIRECTIONS.index((-dr, -dc))
        copies.append((exists, remote(src, dst, opposite), remote(src, here, k), empty))
    order = (4, 5, 6, 7, 2, 3, 0, 1)

    def signal(target):
        pl.semaphore_signal(barrier, inc=1, device_id=target, device_id_type=MESH)

    def send_halos(part):
        for k in order:
            exists, copy, _, _ = copies[k]
            run_if(exists, early(DIRECTIONS[k])[part], copy.start)

    @pl.when(depth == 0)
    def _():
        for copy in x_loads + w_loads[:1]:
            copy.start()
        signal(partner)
        pl.semaphore_wait(barrier, count_of(0))
        for copy in x_parts + w_parts[:1]:
            copy.start()
        for copy in x_loads:
            copy.wait()
        w_loads[1].start()
        for side in range(2):
            top = HALO if side == 0 else rows_here
            left = LEFT if side == 0 else LEFT + cols_here - HALO
            for c in range(halves):
                send_row[side, :, lanes(c)] = as_rows(base[c, top : top + HALO, LEFT : LEFT + cols_here, :])
                for i in range(rows_here):
                    flat[side, c, i * HALO : (i + 1) * HALO, :] = base[c, HALO + i, left : left + HALO, :]
            for c in range(halves):
                send_col[side, :, lanes(c)] = flat[side, c, 0 : rows_here * HALO, :].astype(jnp.bfloat16)
        send_halos(0)
        activate_rows(base, act0, HALO, rows_here)
        w_loads[0].wait()
        first = (row == 0) & (col == 0)

        def send_rest():
            pl.semaphore_wait(later.at[0], 1)
            send_halos(1)

        def both(layer, _):
            @pl.when(layer == 1)
            def _():
                mid_part.start()
                pl.when(row + col > 0)(send_rest)
                w_loads[1].wait()

            interior(
                0, acts.at[layer], w01.at[layer], states.at[layer], states.at[layer + 1],
                acts.at[layer + 1], step_size, shape,
            )
            return 0

        lax.fori_loop(0, 2, both, 0)
        keep_load.start()
        end_part.start()
        pl.when(first)(send_rest)
        mid_part.wait_send()
        end_part.wait_send()
        w_parts[1].start()
        keep_load.wait()
        for exists, copy, _, _ in copies:
            pl.when(exists)(copy.wait_send)
        for copy in x_parts + w_parts:
            copy.wait_send()
        for copy in passes:
            copy.wait_recv()

    @pl.when(depth == 1)
    def _():
        for copy in late_loads:
            copy.start()
        signal(partner)
        for step in DIRECTIONS:
            exists, there_row, there_col = exists_at(step)
            for side, also in enumerate(early_seen_by(step)):
                core = 1 - depth if side == 0 else depth
                run_if(exists, also, functools.partial(signal, (core, there_row, there_col)))
        for step, (_, _, _, (ref, at, rows)) in zip(DIRECTIONS, copies):
            _, there_row, there_col = exists_at(step)
            outside = (there_row < 0) | (there_row >= nrows) | (there_col < 0) | (there_col >= ncols)

            @pl.when(outside)
            def _(ref=ref, at=at, rows=rows):
                ref[at, rows, :] = jnp.zeros_like(ref[at, rows, :])

        pl.semaphore_wait(barrier, count_of(1))
        pl.semaphore_signal(later.at[0], inc=1, device_id=partner, device_id_type=MESH)
        for copy in x_parts:
            copy.wait_recv()
        activate_rows(base, act0, HALO, rows_here)
        mid_part.wait_recv()
        activate_rows(land_mid, act1, HALO + 1, rows_here - 2, mid)
        end_part.wait_recv()
        activate_rows(land_end, act2, HALO + 2, rows_here - 4, end)
        late_loads[0].wait()
        interior(2, act2, w2, end, mid2, act3, step_size, shape)
        late_loads[1].wait()
        interior(3, act3, w3, mid2, fin, None, step_size, shape)
        for k in (0, 1, 2, 3, 4, 5, 6, 7):
            exists, _, arrival, _ = copies[k]
            pl.when(exists)(arrival.wait_recv)
        for copy in passes:
            copy.start()
        w_parts[0].wait_recv()

    for side in range(2):
        for c in range(halves):
            flat[side, c, 8 : 8 + high * HALO, :] = recv_side[side, :, lanes(c)].astype(jnp.float32)
            u = recv_row[side, :, lanes(c)].astype(jnp.float32).reshape(HALO, cols_here, LANES)
            rows = slice(0, HALO) if side == 0 else slice(high - HALO, high)
            base[c, rows, LEFT : LEFT + cols_here, :] = u
            act0[c, rows, LEFT : LEFT + cols_here, :] = silu(u)
    for i in range(high):
        for c in range(halves):
            at = 8 + i * HALO
            u = jnp.where(upper_sublanes(1)[0], flat[0, c, at : at + 8, :], flat[1, c, at - HALO : at + HALO, :])
            value = silu(u)
            for ref, v in ((base, u), (act0, value)):
                ref[c, i, LEFT - HALO : LEFT, :] = v[0:HALO]
                ref[c, i, LEFT + cols_here : LEFT + cols_here + HALO, :] = v[HALO:8]
    ring(0, act0, w0, base, mid, act1, step_size, shape, place)

    @pl.when(depth == 1)
    def _():
        w_parts[1].wait_recv()
        for copy in passes:
            copy.wait_send()

    ring(1, act1, w1, mid, end, act2, step_size, shape, place)


def ring_kernel(
    sizes, keep, states, acts, w2, w3, mid2_in, fin_in, act3_in,
    fine_hbm, coarse_hbm, mid2, fin, act3, store_sem,
):
    nrows, ncols, step_size = sizes
    mid, end, act2 = states.at[1], states.at[2], acts.at[2]
    halves = fin.shape[0]
    rows_here, cols_here = fine_hbm.shape[1:3]
    depth, row, col = lax.axis_index("depth"), lax.axis_index("rows"), lax.axis_index("cols")
    shape, place = (halves, rows_here, cols_here), (nrows, ncols, row, col)

    def stores(ref, target, slot):
        return [
            pltpu.make_async_copy(
                ref.at[c, pl.ds(HALO, rows_here), pl.ds(LEFT, cols_here), :],
                target.at[:, :, pl.ds(c * LANES, LANES)],
                store_sem.at[slot, c],
            )
            for c in range(halves)
        ]

    def start(copies):
        for copy in copies:
            copy.start()

    @pl.when(depth == 0)
    def _():
        kept = pltpu.make_async_copy(keep, coarse_hbm.at[0], store_sem.at[2, 0])
        both = stores(mid, fine_hbm.at[0], 0) + stores(end, fine_hbm.at[1], 1)
        start([kept] + both)
        for copy in [kept] + both:
            copy.wait()

    @pl.when(depth == 1)
    def _():
        early = stores(end, coarse_hbm.at[0], 0)
        start(early)
        ring(2, act2, w2, end, mid2, act3, step_size, shape, place)
        middle = stores(mid2, fine_hbm.at[0], 1)
        start(middle)

        def late(k, c):
            rows = rows_here // 2
            return pltpu.make_async_copy(
                fin.at[c, pl.ds(HALO + k * rows, rows), pl.ds(LEFT, cols_here), :],
                fine_hbm.at[1, pl.ds(k * rows, rows), :, pl.ds(c * LANES, LANES)],
                store_sem.at[2 * k, c],
            )

        def send(k):
            for c in range(halves):
                late(k, c).start()

        for copy in early:
            copy.wait()
        ring(3, act3, w3, mid2, fin, None, step_size, shape, place)
        send(0)
        send(1)
        for copy in middle + [late(k, c) for k in range(2) for c in range(halves)]:
            copy.wait()


def two_sections(section_states, weights):
    _, rows_here, cols_here, channels = section_states.shape
    halves = channels // LANES
    high, wide = rows_here + 2 * HALO, cols_here + 2 * LEFT
    sizes = (lax.axis_size("rows"), lax.axis_size("cols"), 2.0 / (2 * lax.axis_size("depth")))
    f32, bf16, vmem = jnp.float32, jnp.bfloat16, pltpu.VMEM
    state = vmem((halves, high, wide, LANES), f32)
    weight = vmem((9 * channels, channels), bf16)
    flat_weights = weights.reshape(2, 9 * channels, channels)
    any_space, in_vmem = pl.BlockSpec(memory_space=pl.ANY), pl.BlockSpec(memory_space=vmem)
    dma = pltpu.SemaphoreType.DMA
    kept = vmem((rows_here, cols_here, channels), f32)
    three = vmem((3, halves, high, wide, LANES), f32)
    keep, states, mid2, fin, acts, act3, w2, w3 = pl.pallas_call(
        functools.partial(gather_kernel, sizes),
        out_shape=(kept, three, state, state, three, state, weight, weight),
        in_specs=[pl.BlockSpec(memory_space=pltpu.HBM)] * 2,
        out_specs=[in_vmem] * 8,
        scratch_shapes=[
            state, state, vmem((2, 9 * channels, channels), bf16),
            vmem((2, halves, high * HALO + 16, LANES), f32),
            vmem((2, HALO * cols_here, channels), bf16),
            vmem((2, rows_here * HALO, channels), bf16),
            vmem((2, HALO * cols_here, channels), bf16),
            vmem((2, high * HALO, channels), bf16),
            dma((halves + 1,)), dma((halves + 4,)), dma((2,)), dma((8,)),
            pltpu.SemaphoreType.REGULAR((1,)),
        ],
        compiler_params=pltpu.CompilerParams(
            collective_id=0, has_side_effects=True, vmem_limit_bytes=LIMIT
        ),
    )(
        pltpu.with_memory_space_constraint(section_states, pltpu.HBM),
        pltpu.with_memory_space_constraint(flat_weights, pltpu.HBM),
    )
    outs = pl.pallas_call(
        functools.partial(ring_kernel, sizes),
        out_shape=(
            jax.ShapeDtypeStruct((2, rows_here, cols_here, channels), f32),
            jax.ShapeDtypeStruct((1, rows_here, cols_here, channels), f32),
        ) + (state,) * 3,
        in_specs=[in_vmem] * 8,
        out_specs=[any_space] * 2 + [in_vmem] * 3,
        input_output_aliases={5: 2, 6: 3, 7: 4},
        scratch_shapes=[dma((3, halves))],
        compiler_params=pltpu.CompilerParams(vmem_limit_bytes=LIMIT),
    )(keep, states, acts, w2, w3, mid2, fin, act3)
    return outs[0], outs[1]


def on_device(section_states, weights):
    _, rows_here, cols_here, channels = section_states.shape
    tiles = rows_here % 8 == 0 and cols_here % 8 == 0 and channels % LANES == 0
    if lax.axis_size("depth") == 2 and tiles and min(rows_here, cols_here) >= 16:
        return two_sections(section_states, weights)
    return chain_on_device(section_states, weights)


def solution(mesh):
    in_specs = (P("depth", "rows", "cols", None), P("depth", None, None, None, None))
    out_specs = (P("depth", "rows", "cols", None), P("depth", "rows", "cols", None))
    return jax.shard_map(
        on_device, mesh=mesh, in_specs=in_specs, out_specs=out_specs, check_vma=False
    )
```

```python
import functools

import jax
import jax.numpy as jnp
from jax import lax
from jax.experimental import pallas as pl
from jax.experimental.pallas import tpu as pltpu
from jax.sharding import PartitionSpec as P

MESH = pl.DeviceIdType.MESH
HALO = 4
LANES = 128
LIMIT = 32 * 1024 * 1024


def padded_2(shard, sides, width):
    for axis, dim in sides:
        size, length = (lax.axis_size(axis), shard.shape[dim])
        up = [(i, (i + 1) % size) for i in range(size - 1)]
        down = [(j, i) for i, j in up]
        last = lax.slice_in_dim(shard, length - width, length, axis=dim)
        initial = lax.slice_in_dim(shard, 0, width, axis=dim)
        before = lax.ppermute(last, axis, up)
        after = lax.ppermute(initial, axis, down)
        shard = jnp.concatenate([before, shard, after], axis=dim)
    return shard


def shifted_2(block, axis, distance):
    devices = range(lax.axis_size(axis))
    route = [(i - distance, i) for i in devices if i - distance in devices]
    return lax.ppermute(block, axis, route)


def activate(field):
    return jax.nn.silu(field).astype(jnp.bfloat16)


def apply_stencil(padded, flat_weight, out_rows, out_cols):
    channels = padded.shape[2]
    patches = jnp.concatenate(
        [
            padded[shift_row : shift_row + out_rows, shift_col : shift_col + out_cols]
            for shift_row in range(3)
            for shift_col in range(3)
        ],
        axis=2,
    )
    summed = jnp.dot(
        patches.reshape(out_rows * out_cols, 9 * channels),
        flat_weight,
        preferred_element_type=jnp.float32,
    )
    return summed.reshape(out_rows, out_cols, channels)


def section_pass(anchor, first_weight, second_weight, step_size):
    rows_here, cols_here, channels = anchor.shape
    widened = padded_2(anchor, (("rows", 0), ("cols", 1)), 2)
    slope_wide = apply_stencil(activate(widened), first_weight, rows_here + 2, cols_here + 2)
    middle_wide = widened[1:-1, 1:-1] + step_size * slope_wide
    row_global = lax.axis_index("rows") * rows_here - 1 + jnp.arange(rows_here + 2)
    col_global = lax.axis_index("cols") * cols_here - 1 + jnp.arange(cols_here + 2)
    inside_rows = (row_global >= 0) & (row_global < rows_here * lax.axis_size("rows"))
    inside_cols = (col_global >= 0) & (col_global < cols_here * lax.axis_size("cols"))
    inside = inside_rows[:, None] & inside_cols[None, :]
    second_act = jnp.where(inside[:, :, None], activate(middle_wide), jnp.zeros((), jnp.bfloat16))
    first_slope = slope_wide[1:-1, 1:-1]
    middle = middle_wide[1:-1, 1:-1]
    second_slope = apply_stencil(second_act, second_weight, rows_here, cols_here)
    ending = middle + step_size * second_slope
    return (first_slope, middle, ending)


def chain_on_device(section_states, weights):
    rows_here, cols_here, channels = section_states.shape[1:]
    ndepth = lax.axis_size("depth")
    position = lax.axis_index("depth")
    step_size = 2.0 / (2 * ndepth)
    first_weight = weights[0].reshape(9 * channels, channels)
    second_weight = weights[1].reshape(9 * channels, channels)
    anchor = section_states[0]
    first_slope, middle, ending = section_pass(anchor, first_weight, second_weight, step_size)
    jump = ending - (anchor + 2.0 * step_size * first_slope)

    def chain_turn(step_index, current):
        padded = padded_2(activate(current), (("rows", 0), ("cols", 1)), 1)
        advanced = (
            current
            + 2.0 * step_size * apply_stencil(padded, first_weight, rows_here, cols_here)
            + jump
        )
        shifted = shifted_2(advanced, "depth", 1)
        return jnp.where(position == 0, anchor, shifted)

    corrected = lax.fori_loop(0, ndepth - 1, chain_turn, anchor)
    final_slope, final_middle, final_ending = section_pass(
        corrected, first_weight, second_weight, step_size
    )
    fine_states = jnp.stack([final_middle, final_ending])
    return (fine_states, corrected[None])


DIRECTIONS = ((-1, 0), (1, 0), (0, -1), (0, 1), (-1, -1), (-1, 1), (1, -1), (1, 1))
LEFT = 8


def silu(u):
    half = 0.5 * u
    return half + half * jnp.tanh(half)


def as_rows(block):
    return block.reshape(-1, LANES).astype(jnp.bfloat16)


def tap_dot(windows, halves, weight):
    lhs = []
    for a in range(3):
        for b in range(3):
            for c in range(halves):
                parts = [as_rows(window(c, a, b)) for window in windows]
                lhs.append(parts[0] if len(parts) == 1 else jnp.concatenate(parts, axis=0))
    return jnp.dot(jnp.concatenate(lhs, axis=1), weight[...], preferred_element_type=jnp.float32)


def lanes_of(block, c, shape):
    return block[:, c * LANES : (c + 1) * LANES].reshape(shape)


def upper_sublanes(rows):
    return lax.broadcasted_iota(jnp.int32, (rows, 8, LANES), 1) < HALO


def packed(ref, c, first_row, rows, left, right):
    near = ref[c, pl.ds(first_row, rows), left : left + 8, :]
    far = ref[c, pl.ds(first_row, rows), right : right + 8, :]
    return jnp.where(upper_sublanes(rows), near, far)


def store_packed(ref, c, first_row, left, right, value):
    whole = pl.ds(first_row, value.shape[0])
    ref[c, whole, left : left + HALO, :] = value[:, 0:HALO]
    ref[c, whole, right + HALO : right + 8, :] = value[:, HALO:8]


def largest_divisor(total, limit):
    return max(n for n in range(1, limit + 1) if total % n == 0)


def once():
    return jnp.minimum(lax.axis_index("rows"), 0) + 1


def interior(layer, act, weight, before, after, act_after, step_size, shape):
    halves, rows_here, cols_here = shape
    narrow = layer == 3 and cols_here == 16
    left, wide = (LEFT + HALO, cols_here - 2 * HALO) if narrow else (LEFT, cols_here)
    exact = layer >= 2
    first, rows = (HALO + 1 + layer, rows_here - 2 - 2 * layer) if exact else (HALO + 1, rows_here - 2)
    n = rows if exact else largest_divisor(rows, 30)

    def chunk(k, _):
        at = first + k * n

        def window(c, a, b):
            return act[c, pl.ds(at + a - 1, n), left + b - 1 : left + b - 1 + wide, :]

        acc = step_size * tap_dot([window], halves, weight)
        for c in range(halves):
            here = (c, pl.ds(at, n), slice(left, left + wide), slice(None))
            u = before[here] + lanes_of(acc, c, (n, wide, LANES))
            after[here] = u
            if act_after is not None:
                act_after[here] = silu(u)
        return 0

    lax.fori_loop(0, once() if rows == n else rows // n, chunk, 0)


def ring(layer, act, weight, before, after, act_after, step_size, shape, place):
    halves, rows_here, cols_here = shape
    nrows, ncols, row, col = place
    high = rows_here + 2 * HALO
    first, rows = 1 + layer, high - 2 - 2 * layer
    tops = (first, high - HALO - first)
    narrow = layer == 3 and cols_here == 16
    left, wide = (LEFT + HALO, cols_here - 2 * HALO) if narrow else (LEFT, cols_here)
    near, far = HALO + layer, LEFT + cols_here - 6 - layer
    above = jnp.where(row > 0, 1.0, 0.0)
    below = jnp.where(row < nrows - 1, 1.0, 0.0)
    sub = lax.broadcasted_iota(jnp.int32, (1, 8, LANES), 1)
    j = jnp.where(sub < HALO, sub + (layer - 3), sub + (cols_here - 5 - layer)) + col * cols_here
    held = jnp.where((j >= 0) & (j < ncols * cols_here), 1.0, 0.0)
    m = HALO * wide

    def rows_held(at, block):
        i = lax.broadcasted_iota(jnp.int32, block, 0) + at
        return jnp.where(i < HALO, above, jnp.where(i >= high - HALO, below, 1.0))

    def whole(_, carry):
        def strip(at):
            return lambda c, a, b: act[c, pl.ds(at + a - 1, HALO), left + b - 1 : left + b - 1 + wide, :]

        def sides(c, a, b):
            return packed(act, c, first + a - 1, rows, near + b, far + b)

        acc = step_size * tap_dot([strip(at) for at in tops] + [sides], halves, weight)
        for c in range(halves):
            for k, at in enumerate(tops):
                here = (c, pl.ds(at, HALO), slice(left, left + wide), slice(None))
                u = before[here] + lanes_of(acc[k * m : (k + 1) * m], c, (HALO, wide, LANES))
                after[here] = u
                if act_after is not None:
                    act_after[here] = silu(u) * rows_held(at, u.shape)
            u = packed(before, c, first, rows, near + 1, far + 1) + lanes_of(acc[2 * m :], c, (rows, 8, LANES))
            store_packed(after, c, first, near + 1, far + 1, u)
            if act_after is not None:
                value = silu(u) * (held * rows_held(first, u.shape))
                store_packed(act_after, c, first, near + 1, far + 1, value)
        return carry

    lax.fori_loop(0, once(), whole, 0)


def gather_kernel(
    sizes, x_hbm, w_hbm,
    keep, states, mid2, fin, acts, act3, w2, w3,
    land_mid, land_end, w01, flat, send_row, send_col, recv_row, recv_side,
    load_sem, part_sem, pass_sem, halo_sem, later,
):
    nrows, ncols, step_size = sizes
    base, mid, end = [states.at[k] for k in range(3)]
    act0, act1, act2 = [acts.at[k] for k in range(3)]
    w0, w1 = w01.at[0], w01.at[1]
    halves, high = land_mid.shape[:2]
    rows_here, cols_here = keep.shape[:2]
    depth, row, col = lax.axis_index("depth"), lax.axis_index("rows"), lax.axis_index("cols")
    shape, place = (halves, rows_here, cols_here), (nrows, ncols, row, col)
    partner = (1 - depth, row, col)
    corner = HALO * HALO
    barrier = pltpu.get_barrier_semaphore()

    def lanes(c):
        return pl.ds(c * LANES, LANES)

    def local(src, dst, k):
        return pltpu.make_async_copy(src, dst, load_sem.at[k])

    def to_partner(src, dst, k, sem=part_sem):
        return pltpu.make_async_remote_copy(
            src_ref=src, dst_ref=dst, send_sem=sem.at[k], recv_sem=sem.at[k],
            device_id=partner, device_id_type=MESH,
        )

    def exists_at(step):
        there_row, there_col = row + step[0], col + step[1]
        exists = (there_row >= 0) & (there_row < nrows) & (there_col >= 0) & (there_col < ncols)
        return exists, there_row, there_col

    odd, even = lax.rem(row, 2) == 1, lax.rem(row, 2) == 0

    def pick(step, always, sometimes, first, second):
        if step == always:
            return True, None
        if step in sometimes:
            return first, second
        return None, True

    def early(step):
        return pick(step, (0, -1), ((-1, 0), (-1, -1)), odd, even)

    def early_seen_by(step):
        return pick(step, (0, 1), ((1, 0), (1, 1)), even, odd)

    def run_if(exists, also, action):
        if also is True:
            pl.when(exists)(action)
        elif also is not None:
            pl.when(exists)(lambda: pl.when(also)(action))

    def count_of(part):
        count = jnp.int32(1)
        for step in DIRECTIONS:
            also = early(step)[part]
            if also is not None:
                there = exists_at(step)[0]
                there = there if also is True else there & also
                count = count + jnp.where(there, 1, 0)
        return count

    def own(c):
        return base.at[c, pl.ds(HALO, rows_here), pl.ds(LEFT, cols_here), :]

    x_loads = [local(x_hbm.at[0, :, :, lanes(c)], own(c), c) for c in range(halves)]
    x_parts = [to_partner(x_hbm.at[0, :, :, lanes(c)], own(c), c) for c in range(halves)]
    keep_load = local(x_hbm.at[0], keep, 1)
    w_loads = [local(w_hbm.at[0], w0, halves), local(w_hbm.at[1], w1, 0)]
    late_loads = [local(w_hbm.at[0], w2, 0), local(w_hbm.at[1], w3, 1)]
    w_parts = [to_partner(w_hbm.at[0], w0, halves), to_partner(w_hbm.at[1], w1, halves + 1)]

    def inner(ref, k):
        return ref.at[:, pl.ds(HALO + k, rows_here - 2 * k), pl.ds(LEFT, cols_here), :]

    mid_part = to_partner(inner(mid, 1), inner(land_mid, 1), halves + 2)
    end_part = to_partner(inner(end, 2), inner(land_end, 2), halves + 3)
    passes = [
        to_partner(ref, ref, k, pass_sem) for k, ref in enumerate((recv_row, recv_side))
    ]

    def activate_rows(source, target, first, rows, copied=None):
        for c in range(halves):
            here = (c, pl.ds(first, rows), slice(LEFT, LEFT + cols_here), slice(None))
            u = source[here]
            target[here] = silu(u)
            if copied is not None:
                copied[here] = u

    copies = []
    for k, (dr, dc) in enumerate(DIRECTIONS):
        exists, there_row, there_col = exists_at((dr, dc))
        side = (dc + 1) // 2
        mine = {-1: (0, corner), 1: ((rows_here - HALO) * HALO, corner), 0: (0, rows_here * HALO)}[dr]
        theirs = {1: (0, corner), -1: (high * HALO - corner, corner), 0: (corner, rows_here * HALO)}[dr]
        if dc == 0:
            src, dst, here = send_row.at[(dr + 1) // 2], recv_row.at[(1 - dr) // 2], recv_row.at[(dr + 1) // 2]
            empty = (recv_row, (dr + 1) // 2, slice(None))
        else:
            back = {-1: (0, corner), 1: (high * HALO - corner, corner), 0: (corner, rows_here * HALO)}[dr]
            src = send_col.at[side, pl.ds(*mine)]
            dst = recv_side.at[1 - side, pl.ds(*theirs)]
            here = recv_side.at[side, pl.ds(*back)]
            empty = (recv_side, side, slice(back[0], back[0] + back[1]))

        def remote(src, dst, slot):
            return pltpu.make_async_remote_copy(
                src_ref=src, dst_ref=dst, send_sem=halo_sem.at[k], recv_sem=halo_sem.at[slot],
                device_id=(1 - depth, there_row, there_col), device_id_type=MESH,
            )

        opposite = DIRECTIONS.index((-dr, -dc))
        copies.append((exists, remote(src, dst, opposite), remote(src, here, k), empty))
    order = (4, 5, 6, 7, 2, 3, 0, 1)

    def signal(target):
        pl.semaphore_signal(barrier, inc=1, device_id=target, device_id_type=MESH)

    def send_halos(part):
        for k in order:
            exists, copy, _, _ = copies[k]
            run_if(exists, early(DIRECTIONS[k])[part], copy.start)

    @pl.when(depth == 0)
    def _():
        for copy in x_loads + w_loads[:1]:
            copy.start()
        signal(partner)
        pl.semaphore_wait(barrier, count_of(0))
        for copy in x_parts + w_parts[:1]:
            copy.start()
        for copy in x_loads:
            copy.wait()
        w_loads[1].start()
        for side in range(2):
            top = HALO if side == 0 else rows_here
            left = LEFT if side == 0 else LEFT + cols_here - HALO
            for c in range(halves):
                send_row[side, :, lanes(c)] = as_rows(base[c, top : top + HALO, LEFT : LEFT + cols_here, :])
                for i in range(rows_here):
                    flat[side, c, i * HALO : (i + 1) * HALO, :] = base[c, HALO + i, left : left + HALO, :]
            for c in range(halves):
                send_col[side, :, lanes(c)] = flat[side, c, 0 : rows_here * HALO, :].astype(jnp.bfloat16)
        send_halos(0)
        activate_rows(base, act0, HALO, rows_here)
        w_loads[0].wait()
        first = (row == 0) & (col == 0)

        def send_rest():
            pl.semaphore_wait(later.at[0], 1)
            send_halos(1)

        def both(layer, _):
            @pl.when(layer == 1)
            def _():
                mid_part.start()
                pl.when(row + col > 0)(send_rest)
                w_loads[1].wait()

            interior(
                0, acts.at[layer], w01.at[layer], states.at[layer], states.at[layer + 1],
                acts.at[layer + 1], step_size, shape,
            )
            return 0

        lax.fori_loop(0, 2, both, 0)
        keep_load.start()
        end_part.start()
        w_parts[1].start()
        pl.when(first)(send_rest)
        mid_part.wait_send()
        end_part.wait_send()
        keep_load.wait()
        for exists, copy, _, _ in copies:
            pl.when(exists)(copy.wait_send)
        for copy in x_parts + w_parts:
            copy.wait_send()
        for copy in passes:
            copy.wait_recv()

    @pl.when(depth == 1)
    def _():
        for copy in late_loads:
            copy.start()
        signal(partner)
        for step in DIRECTIONS:
            exists, there_row, there_col = exists_at(step)
            for side, also in enumerate(early_seen_by(step)):
                core = 1 - depth if side == 0 else depth
                run_if(exists, also, functools.partial(signal, (core, there_row, there_col)))
        for step, (_, _, _, (ref, at, rows)) in zip(DIRECTIONS, copies):
            _, there_row, there_col = exists_at(step)
            outside = (there_row < 0) | (there_row >= nrows) | (there_col < 0) | (there_col >= ncols)

            @pl.when(outside)
            def _(ref=ref, at=at, rows=rows):
                ref[at, rows, :] = jnp.zeros_like(ref[at, rows, :])

        pl.semaphore_wait(barrier, count_of(1))
        pl.semaphore_signal(later.at[0], inc=1, device_id=partner, device_id_type=MESH)
        for copy in x_parts:
            copy.wait_recv()
        activate_rows(base, act0, HALO, rows_here)
        mid_part.wait_recv()
        activate_rows(land_mid, act1, HALO + 1, rows_here - 2, mid)
        end_part.wait_recv()
        activate_rows(land_end, act2, HALO + 2, rows_here - 4, end)
        def forward():
            for exists, _, arrival, _ in copies:
                pl.when(exists)(arrival.wait_recv)
            for copy in passes:
                copy.start()

        late_loads[0].wait()
        interior(2, act2, w2, end, mid2, act3, step_size, shape)
        pl.when((row == 0) & (col == 0))(forward)
        late_loads[1].wait()
        interior(3, act3, w3, mid2, fin, None, step_size, shape)
        pl.when(row + col > 0)(forward)
        w_parts[0].wait_recv()

    for side in range(2):
        for c in range(halves):
            flat[side, c, 8 : 8 + high * HALO, :] = recv_side[side, :, lanes(c)].astype(jnp.float32)
            u = recv_row[side, :, lanes(c)].astype(jnp.float32).reshape(HALO, cols_here, LANES)
            rows = slice(0, HALO) if side == 0 else slice(high - HALO, high)
            base[c, rows, LEFT : LEFT + cols_here, :] = u
            act0[c, rows, LEFT : LEFT + cols_here, :] = silu(u)
    for i in range(high):
        for c in range(halves):
            at = 8 + i * HALO
            u = jnp.where(upper_sublanes(1)[0], flat[0, c, at : at + 8, :], flat[1, c, at - HALO : at + HALO, :])
            value = silu(u)
            for ref, v in ((base, u), (act0, value)):
                ref[c, i, LEFT - HALO : LEFT, :] = v[0:HALO]
                ref[c, i, LEFT + cols_here : LEFT + cols_here + HALO, :] = v[HALO:8]
    ring(0, act0, w0, base, mid, act1, step_size, shape, place)

    @pl.when(depth == 1)
    def _():
        w_parts[1].wait_recv()

    ring(1, act1, w1, mid, end, act2, step_size, shape, place)

    @pl.when(depth == 1)
    def _():
        for copy in passes:
            copy.wait_send()


def ring_kernel(
    sizes, keep, states, acts, w2, w3, mid2_in, fin_in, act3_in,
    fine_hbm, coarse_hbm, mid2, fin, act3, store_sem,
):
    nrows, ncols, step_size = sizes
    mid, end, act2 = states.at[1], states.at[2], acts.at[2]
    halves = fin.shape[0]
    rows_here, cols_here = fine_hbm.shape[1:3]
    depth, row, col = lax.axis_index("depth"), lax.axis_index("rows"), lax.axis_index("cols")
    shape, place = (halves, rows_here, cols_here), (nrows, ncols, row, col)

    def stores(ref, target, slot):
        return [
            pltpu.make_async_copy(
                ref.at[c, pl.ds(HALO, rows_here), pl.ds(LEFT, cols_here), :],
                target.at[:, :, pl.ds(c * LANES, LANES)],
                store_sem.at[slot, c],
            )
            for c in range(halves)
        ]

    def start(copies):
        for copy in copies:
            copy.start()

    @pl.when(depth == 0)
    def _():
        kept = pltpu.make_async_copy(keep, coarse_hbm.at[0], store_sem.at[2, 0])
        both = stores(mid, fine_hbm.at[0], 0) + stores(end, fine_hbm.at[1], 1)
        start([kept] + both)
        for copy in [kept] + both:
            copy.wait()

    @pl.when(depth == 1)
    def _():
        early = stores(end, coarse_hbm.at[0], 0)
        start(early)
        ring(2, act2, w2, end, mid2, act3, step_size, shape, place)
        middle = stores(mid2, fine_hbm.at[0], 1)
        start(middle)

        def late(k, c):
            rows = rows_here // 2
            return pltpu.make_async_copy(
                fin.at[c, pl.ds(HALO + k * rows, rows), pl.ds(LEFT, cols_here), :],
                fine_hbm.at[1, pl.ds(k * rows, rows), :, pl.ds(c * LANES, LANES)],
                store_sem.at[2 * k, c],
            )

        def send(k):
            for c in range(halves):
                late(k, c).start()

        for copy in early:
            copy.wait()
        ring(3, act3, w3, mid2, fin, None, step_size, shape, place)
        send(0)
        send(1)
        for copy in middle + [late(k, c) for k in range(2) for c in range(halves)]:
            copy.wait()


def two_sections(section_states, weights):
    _, rows_here, cols_here, channels = section_states.shape
    halves = channels // LANES
    high, wide = rows_here + 2 * HALO, cols_here + 2 * LEFT
    sizes = (lax.axis_size("rows"), lax.axis_size("cols"), 2.0 / (2 * lax.axis_size("depth")))
    f32, bf16, vmem = jnp.float32, jnp.bfloat16, pltpu.VMEM
    state = vmem((halves, high, wide, LANES), f32)
    weight = vmem((9 * channels, channels), bf16)
    flat_weights = weights.reshape(2, 9 * channels, channels)
    any_space, in_vmem = pl.BlockSpec(memory_space=pl.ANY), pl.BlockSpec(memory_space=vmem)
    dma = pltpu.SemaphoreType.DMA
    kept = vmem((rows_here, cols_here, channels), f32)
    three = vmem((3, halves, high, wide, LANES), f32)
    keep, states, mid2, fin, acts, act3, w2, w3 = pl.pallas_call(
        functools.partial(gather_kernel, sizes),
        out_shape=(kept, three, state, state, three, state, weight, weight),
        in_specs=[pl.BlockSpec(memory_space=pltpu.HBM)] * 2,
        out_specs=[in_vmem] * 8,
        scratch_shapes=[
            state, state, vmem((2, 9 * channels, channels), bf16),
            vmem((2, halves, high * HALO + 16, LANES), f32),
            vmem((2, HALO * cols_here, channels), bf16),
            vmem((2, rows_here * HALO, channels), bf16),
            vmem((2, HALO * cols_here, channels), bf16),
            vmem((2, high * HALO, channels), bf16),
            dma((halves + 1,)), dma((halves + 4,)), dma((2,)), dma((8,)),
            pltpu.SemaphoreType.REGULAR((1,)),
        ],
        compiler_params=pltpu.CompilerParams(
            collective_id=0, has_side_effects=True, vmem_limit_bytes=LIMIT
        ),
    )(
        pltpu.with_memory_space_constraint(section_states, pltpu.HBM),
        pltpu.with_memory_space_constraint(flat_weights, pltpu.HBM),
    )
    outs = pl.pallas_call(
        functools.partial(ring_kernel, sizes),
        out_shape=(
            jax.ShapeDtypeStruct((2, rows_here, cols_here, channels), f32),
            jax.ShapeDtypeStruct((1, rows_here, cols_here, channels), f32),
        ) + (state,) * 3,
        in_specs=[in_vmem] * 8,
        out_specs=[any_space] * 2 + [in_vmem] * 3,
        input_output_aliases={5: 2, 6: 3, 7: 4},
        scratch_shapes=[dma((3, halves))],
        compiler_params=pltpu.CompilerParams(vmem_limit_bytes=LIMIT),
    )(keep, states, acts, w2, w3, mid2, fin, act3)
    return outs[0], outs[1]


def on_device(section_states, weights):
    _, rows_here, cols_here, channels = section_states.shape
    tiles = rows_here % 8 == 0 and cols_here % 8 == 0 and channels % LANES == 0
    if lax.axis_size("depth") == 2 and tiles and min(rows_here, cols_here) >= 16:
        return two_sections(section_states, weights)
    return chain_on_device(section_states, weights)


def solution(mesh):
    in_specs = (P("depth", "rows", "cols", None), P("depth", None, None, None, None))
    out_specs = (P("depth", "rows", "cols", None), P("depth", "rows", "cols", None))
    return jax.shard_map(
        on_device, mesh=mesh, in_specs=in_specs, out_specs=out_specs, check_vma=False
    )
```

```python
import functools

import jax
import jax.numpy as jnp
from jax import lax
from jax.experimental import pallas as pl
from jax.experimental.pallas import tpu as pltpu
from jax.sharding import PartitionSpec as P

MESH = pl.DeviceIdType.MESH
HALO = 4
LANES = 128
LIMIT = 32 * 1024 * 1024


def padded_2(shard, sides, width):
    for axis, dim in sides:
        size, length = (lax.axis_size(axis), shard.shape[dim])
        up = [(i, (i + 1) % size) for i in range(size - 1)]
        down = [(j, i) for i, j in up]
        last = lax.slice_in_dim(shard, length - width, length, axis=dim)
        initial = lax.slice_in_dim(shard, 0, width, axis=dim)
        before = lax.ppermute(last, axis, up)
        after = lax.ppermute(initial, axis, down)
        shard = jnp.concatenate([before, shard, after], axis=dim)
    return shard


def shifted_2(block, axis, distance):
    devices = range(lax.axis_size(axis))
    route = [(i - distance, i) for i in devices if i - distance in devices]
    return lax.ppermute(block, axis, route)


def activate(field):
    return jax.nn.silu(field).astype(jnp.bfloat16)


def apply_stencil(padded, flat_weight, out_rows, out_cols):
    channels = padded.shape[2]
    patches = jnp.concatenate(
        [
            padded[shift_row : shift_row + out_rows, shift_col : shift_col + out_cols]
            for shift_row in range(3)
            for shift_col in range(3)
        ],
        axis=2,
    )
    summed = jnp.dot(
        patches.reshape(out_rows * out_cols, 9 * channels),
        flat_weight,
        preferred_element_type=jnp.float32,
    )
    return summed.reshape(out_rows, out_cols, channels)


def section_pass(anchor, first_weight, second_weight, step_size):
    rows_here, cols_here, channels = anchor.shape
    widened = padded_2(anchor, (("rows", 0), ("cols", 1)), 2)
    slope_wide = apply_stencil(activate(widened), first_weight, rows_here + 2, cols_here + 2)
    middle_wide = widened[1:-1, 1:-1] + step_size * slope_wide
    row_global = lax.axis_index("rows") * rows_here - 1 + jnp.arange(rows_here + 2)
    col_global = lax.axis_index("cols") * cols_here - 1 + jnp.arange(cols_here + 2)
    inside_rows = (row_global >= 0) & (row_global < rows_here * lax.axis_size("rows"))
    inside_cols = (col_global >= 0) & (col_global < cols_here * lax.axis_size("cols"))
    inside = inside_rows[:, None] & inside_cols[None, :]
    second_act = jnp.where(inside[:, :, None], activate(middle_wide), jnp.zeros((), jnp.bfloat16))
    first_slope = slope_wide[1:-1, 1:-1]
    middle = middle_wide[1:-1, 1:-1]
    second_slope = apply_stencil(second_act, second_weight, rows_here, cols_here)
    ending = middle + step_size * second_slope
    return (first_slope, middle, ending)


def chain_on_device(section_states, weights):
    rows_here, cols_here, channels = section_states.shape[1:]
    ndepth = lax.axis_size("depth")
    position = lax.axis_index("depth")
    step_size = 2.0 / (2 * ndepth)
    first_weight = weights[0].reshape(9 * channels, channels)
    second_weight = weights[1].reshape(9 * channels, channels)
    anchor = section_states[0]
    first_slope, middle, ending = section_pass(anchor, first_weight, second_weight, step_size)
    jump = ending - (anchor + 2.0 * step_size * first_slope)

    def chain_turn(step_index, current):
        padded = padded_2(activate(current), (("rows", 0), ("cols", 1)), 1)
        advanced = (
            current
            + 2.0 * step_size * apply_stencil(padded, first_weight, rows_here, cols_here)
            + jump
        )
        shifted = shifted_2(advanced, "depth", 1)
        return jnp.where(position == 0, anchor, shifted)

    corrected = lax.fori_loop(0, ndepth - 1, chain_turn, anchor)
    final_slope, final_middle, final_ending = section_pass(
        corrected, first_weight, second_weight, step_size
    )
    fine_states = jnp.stack([final_middle, final_ending])
    return (fine_states, corrected[None])


DIRECTIONS = ((-1, 0), (1, 0), (0, -1), (0, 1), (-1, -1), (-1, 1), (1, -1), (1, 1))
LEFT = 8


def silu(u):
    half = 0.5 * u
    return half + half * jnp.tanh(half)


def as_rows(block):
    return block.reshape(-1, LANES).astype(jnp.bfloat16)


def tap_dot(windows, halves, weight):
    lhs = []
    for a in range(3):
        for b in range(3):
            for c in range(halves):
                parts = [as_rows(window(c, a, b)) for window in windows]
                lhs.append(parts[0] if len(parts) == 1 else jnp.concatenate(parts, axis=0))
    return jnp.dot(jnp.concatenate(lhs, axis=1), weight[...], preferred_element_type=jnp.float32)


def lanes_of(block, c, shape):
    return block[:, c * LANES : (c + 1) * LANES].reshape(shape)


def upper_sublanes(rows):
    return lax.broadcasted_iota(jnp.int32, (rows, 8, LANES), 1) < HALO


def packed(ref, c, first_row, rows, left, right):
    near = ref[c, pl.ds(first_row, rows), left : left + 8, :]
    far = ref[c, pl.ds(first_row, rows), right : right + 8, :]
    return jnp.where(upper_sublanes(rows), near, far)


def store_packed(ref, c, first_row, left, right, value):
    whole = pl.ds(first_row, value.shape[0])
    ref[c, whole, left : left + HALO, :] = value[:, 0:HALO]
    ref[c, whole, right + HALO : right + 8, :] = value[:, HALO:8]


def largest_divisor(total, limit):
    return max(n for n in range(1, limit + 1) if total % n == 0)


def once():
    return jnp.minimum(lax.axis_index("rows"), 0) + 1


def interior(layer, act, weight, before, after, act_after, step_size, shape):
    halves, rows_here, cols_here = shape
    narrow = layer == 3 and cols_here == 16
    left, wide = (LEFT + HALO, cols_here - 2 * HALO) if narrow else (LEFT, cols_here)
    exact = layer >= 2
    first, rows = (HALO + 1 + layer, rows_here - 2 - 2 * layer) if exact else (HALO + 1, rows_here - 2)
    n = rows if exact else largest_divisor(rows, 30)

    def chunk(k, _):
        at = first + k * n

        def window(c, a, b):
            return act[c, pl.ds(at + a - 1, n), left + b - 1 : left + b - 1 + wide, :]

        acc = step_size * tap_dot([window], halves, weight)
        for c in range(halves):
            here = (c, pl.ds(at, n), slice(left, left + wide), slice(None))
            u = before[here] + lanes_of(acc, c, (n, wide, LANES))
            after[here] = u
            if act_after is not None:
                act_after[here] = silu(u)
        return 0

    lax.fori_loop(0, once() if rows == n else rows // n, chunk, 0)


def ring(layer, act, weight, before, after, act_after, step_size, shape, place):
    halves, rows_here, cols_here = shape
    nrows, ncols, row, col = place
    high = rows_here + 2 * HALO
    first, rows = 1 + layer, high - 2 - 2 * layer
    tops = (first, high - HALO - first)
    narrow = layer == 3 and cols_here == 16
    left, wide = (LEFT + HALO, cols_here - 2 * HALO) if narrow else (LEFT, cols_here)
    near, far = HALO + layer, LEFT + cols_here - 6 - layer
    above = jnp.where(row > 0, 1.0, 0.0)
    below = jnp.where(row < nrows - 1, 1.0, 0.0)
    sub = lax.broadcasted_iota(jnp.int32, (1, 8, LANES), 1)
    j = jnp.where(sub < HALO, sub + (layer - 3), sub + (cols_here - 5 - layer)) + col * cols_here
    held = jnp.where((j >= 0) & (j < ncols * cols_here), 1.0, 0.0)
    m = HALO * wide

    def rows_held(at, block):
        i = lax.broadcasted_iota(jnp.int32, block, 0) + at
        return jnp.where(i < HALO, above, jnp.where(i >= high - HALO, below, 1.0))

    def whole(_, carry):
        def strip(at):
            return lambda c, a, b: act[c, pl.ds(at + a - 1, HALO), left + b - 1 : left + b - 1 + wide, :]

        def sides(c, a, b):
            return packed(act, c, first + a - 1, rows, near + b, far + b)

        acc = step_size * tap_dot([strip(at) for at in tops] + [sides], halves, weight)
        for c in range(halves):
            for k, at in enumerate(tops):
                here = (c, pl.ds(at, HALO), slice(left, left + wide), slice(None))
                u = before[here] + lanes_of(acc[k * m : (k + 1) * m], c, (HALO, wide, LANES))
                after[here] = u
                if act_after is not None:
                    act_after[here] = silu(u) * rows_held(at, u.shape)
            u = packed(before, c, first, rows, near + 1, far + 1) + lanes_of(acc[2 * m :], c, (rows, 8, LANES))
            store_packed(after, c, first, near + 1, far + 1, u)
            if act_after is not None:
                value = silu(u) * (held * rows_held(first, u.shape))
                store_packed(act_after, c, first, near + 1, far + 1, value)
        return carry

    lax.fori_loop(0, once(), whole, 0)


def gather_kernel(
    sizes, x_hbm, w_hbm,
    keep, states, mid2, fin, acts, act3, w2, w3,
    land_mid, land_end, w01, mid_side, land_side, flat, send_row, send_col, recv_row, recv_side,
    load_sem, part_sem, pass_sem, halo_sem, later,
):
    nrows, ncols, step_size = sizes
    base, mid, end = [states.at[k] for k in range(3)]
    act0, act1, act2 = [acts.at[k] for k in range(3)]
    w0, w1 = w01.at[0], w01.at[1]
    halves, high = land_mid.shape[:2]
    rows_here, cols_here = keep.shape[:2]
    depth, row, col = lax.axis_index("depth"), lax.axis_index("rows"), lax.axis_index("cols")
    shape, place = (halves, rows_here, cols_here), (nrows, ncols, row, col)
    partner = (1 - depth, row, col)
    corner = HALO * HALO
    barrier = pltpu.get_barrier_semaphore()

    def lanes(c):
        return pl.ds(c * LANES, LANES)

    def local(src, dst, k):
        return pltpu.make_async_copy(src, dst, load_sem.at[k])

    def to_partner(src, dst, k, sem=part_sem):
        return pltpu.make_async_remote_copy(
            src_ref=src, dst_ref=dst, send_sem=sem.at[k], recv_sem=sem.at[k],
            device_id=partner, device_id_type=MESH,
        )

    def exists_at(step):
        there_row, there_col = row + step[0], col + step[1]
        exists = (there_row >= 0) & (there_row < nrows) & (there_col >= 0) & (there_col < ncols)
        return exists, there_row, there_col

    odd, even = lax.rem(row, 2) == 1, lax.rem(row, 2) == 0

    def pick(step, always, sometimes, first, second):
        if step == always:
            return True, None
        if step in sometimes:
            return first, second
        return None, True

    def early(step):
        return pick(step, (0, -1), ((-1, 0), (-1, -1)), odd, even)

    def early_seen_by(step):
        return pick(step, (0, 1), ((1, 0), (1, 1)), even, odd)

    def run_if(exists, also, action):
        if also is True:
            pl.when(exists)(action)
        elif also is not None:
            pl.when(exists)(lambda: pl.when(also)(action))

    def count_of(part):
        count = jnp.int32(1)
        for step in DIRECTIONS:
            also = early(step)[part]
            if also is not None:
                there = exists_at(step)[0]
                there = there if also is True else there & also
                count = count + jnp.where(there, 1, 0)
        return count

    def own(c):
        return base.at[c, pl.ds(HALO, rows_here), pl.ds(LEFT, cols_here), :]

    x_loads = [local(x_hbm.at[0, :, :, lanes(c)], own(c), c) for c in range(halves)]
    x_parts = [to_partner(x_hbm.at[0, :, :, lanes(c)], own(c), c) for c in range(halves)]
    keep_load = local(x_hbm.at[0], keep, 1)
    w_loads = [local(w_hbm.at[0], w0, halves), local(w_hbm.at[1], w1, 0)]
    late_loads = [local(w_hbm.at[0], w2, 0), local(w_hbm.at[1], w3, 1)]
    w_parts = [to_partner(w_hbm.at[0], w0, halves), to_partner(w_hbm.at[1], w1, halves + 1)]

    def inner(ref, k):
        return ref.at[:, pl.ds(HALO + k, rows_here - 2 * k), pl.ds(LEFT, cols_here), :]

    def two_rows(ref, at):
        return ref.at[:, pl.ds(at, 2), pl.ds(LEFT, cols_here), :]

    edge_rows = (HALO + 1, HALO + rows_here - 3)
    far_side = LEFT + cols_here - 8
    mid_parts = [to_partner(mid_side, land_side, halves + 2)] + [
        to_partner(two_rows(mid, at), two_rows(land_mid, at), halves + 4 + k) for k, at in enumerate(edge_rows)
    ]
    end_part = to_partner(inner(end, 2), inner(land_end, 2), halves + 3)
    passes = [
        to_partner(ref, ref, k, pass_sem) for k, ref in enumerate((recv_row, recv_side))
    ]

    def activate_rows(source, target, first, rows, copied=None):
        for c in range(halves):
            here = (c, pl.ds(first, rows), slice(LEFT, LEFT + cols_here), slice(None))
            u = source[here]
            target[here] = silu(u)
            if copied is not None:
                copied[here] = u

    copies = []
    for k, (dr, dc) in enumerate(DIRECTIONS):
        exists, there_row, there_col = exists_at((dr, dc))
        side = (dc + 1) // 2
        mine = {-1: (0, corner), 1: ((rows_here - HALO) * HALO, corner), 0: (0, rows_here * HALO)}[dr]
        theirs = {1: (0, corner), -1: (high * HALO - corner, corner), 0: (corner, rows_here * HALO)}[dr]
        if dc == 0:
            src, dst, here = send_row.at[(dr + 1) // 2], recv_row.at[(1 - dr) // 2], recv_row.at[(dr + 1) // 2]
            empty = (recv_row, (dr + 1) // 2, slice(None))
        else:
            back = {-1: (0, corner), 1: (high * HALO - corner, corner), 0: (corner, rows_here * HALO)}[dr]
            src = send_col.at[side, pl.ds(*mine)]
            dst = recv_side.at[1 - side, pl.ds(*theirs)]
            here = recv_side.at[side, pl.ds(*back)]
            empty = (recv_side, side, slice(back[0], back[0] + back[1]))

        def remote(src, dst, slot):
            return pltpu.make_async_remote_copy(
                src_ref=src, dst_ref=dst, send_sem=halo_sem.at[k], recv_sem=halo_sem.at[slot],
                device_id=(1 - depth, there_row, there_col), device_id_type=MESH,
            )

        opposite = DIRECTIONS.index((-dr, -dc))
        copies.append((exists, remote(src, dst, opposite), remote(src, here, k), empty))
    order = (4, 5, 6, 7, 2, 3, 0, 1)

    def signal(target):
        pl.semaphore_signal(barrier, inc=1, device_id=target, device_id_type=MESH)

    def send_halos(part):
        for k in order:
            exists, copy, _, _ = copies[k]
            run_if(exists, early(DIRECTIONS[k])[part], copy.start)

    @pl.when(depth == 0)
    def _():
        for copy in x_loads + w_loads[:1]:
            copy.start()
        signal(partner)
        pl.semaphore_wait(barrier, count_of(0))
        for copy in x_parts + w_parts[:1]:
            copy.start()
        for copy in x_loads:
            copy.wait()
        w_loads[1].start()
        for side in range(2):
            top = HALO if side == 0 else rows_here
            left = LEFT if side == 0 else LEFT + cols_here - HALO
            for c in range(halves):
                send_row[side, :, lanes(c)] = as_rows(base[c, top : top + HALO, LEFT : LEFT + cols_here, :])
                for i in range(rows_here):
                    flat[side, c, i * HALO : (i + 1) * HALO, :] = base[c, HALO + i, left : left + HALO, :]
            for c in range(halves):
                send_col[side, :, lanes(c)] = flat[side, c, 0 : rows_here * HALO, :].astype(jnp.bfloat16)
        send_halos(0)
        activate_rows(base, act0, HALO, rows_here)
        w_loads[0].wait()
        first = (row == 0) & (col == 0)

        def send_rest():
            pl.semaphore_wait(later.at[0], 1)
            send_halos(1)

        def both(layer, _):
            @pl.when(layer == 1)
            def _():
                for c in range(halves):
                    mid_side[c] = packed(mid, c, HALO + 1, rows_here - 2, LEFT, far_side)
                for copy in mid_parts:
                    copy.start()
                pl.when(row + col > 0)(send_rest)
                w_loads[1].wait()

            interior(
                0, acts.at[layer], w01.at[layer], states.at[layer], states.at[layer + 1],
                acts.at[layer + 1], step_size, shape,
            )
            return 0

        lax.fori_loop(0, 2, both, 0)
        keep_load.start()
        end_part.start()
        w_parts[1].start()
        pl.when(first)(send_rest)
        for copy in mid_parts:
            copy.wait_send()
        end_part.wait_send()
        keep_load.wait()
        for exists, copy, _, _ in copies:
            pl.when(exists)(copy.wait_send)
        for copy in x_parts + w_parts:
            copy.wait_send()
        for copy in passes:
            copy.wait_recv()

    @pl.when(depth == 1)
    def _():
        for copy in late_loads:
            copy.start()
        signal(partner)
        for step in DIRECTIONS:
            exists, there_row, there_col = exists_at(step)
            for side, also in enumerate(early_seen_by(step)):
                core = 1 - depth if side == 0 else depth
                run_if(exists, also, functools.partial(signal, (core, there_row, there_col)))
        for step, (_, _, _, (ref, at, rows)) in zip(DIRECTIONS, copies):
            _, there_row, there_col = exists_at(step)
            outside = (there_row < 0) | (there_row >= nrows) | (there_col < 0) | (there_col >= ncols)

            @pl.when(outside)
            def _(ref=ref, at=at, rows=rows):
                ref[at, rows, :] = jnp.zeros_like(ref[at, rows, :])

        pl.semaphore_wait(barrier, count_of(1))
        pl.semaphore_signal(later.at[0], inc=1, device_id=partner, device_id_type=MESH)
        for copy in x_parts:
            copy.wait_recv()
        activate_rows(base, act0, HALO, rows_here)
        for copy in mid_parts:
            copy.wait_recv()
        for at in edge_rows:
            activate_rows(land_mid, act1, at, 2, mid)
        for c in range(halves):
            u = land_side[c]
            store_packed(mid, c, HALO + 1, LEFT, far_side, u)
            store_packed(act1, c, HALO + 1, LEFT, far_side, silu(u))
        end_part.wait_recv()
        activate_rows(land_end, act2, HALO + 2, rows_here - 4, end)
        def forward():
            for exists, _, arrival, _ in copies:
                pl.when(exists)(arrival.wait_recv)
            for copy in passes:
                copy.start()

        late_loads[0].wait()
        interior(2, act2, w2, end, mid2, act3, step_size, shape)
        pl.when((row == 0) & (col == 0))(forward)
        late_loads[1].wait()
        interior(3, act3, w3, mid2, fin, None, step_size, shape)
        pl.when(row + col > 0)(forward)
        w_parts[0].wait_recv()

    for side in range(2):
        for c in range(halves):
            flat[side, c, 8 : 8 + high * HALO, :] = recv_side[side, :, lanes(c)].astype(jnp.float32)
            u = recv_row[side, :, lanes(c)].astype(jnp.float32).reshape(HALO, cols_here, LANES)
            rows = slice(0, HALO) if side == 0 else slice(high - HALO, high)
            base[c, rows, LEFT : LEFT + cols_here, :] = u
            act0[c, rows, LEFT : LEFT + cols_here, :] = silu(u)
    for i in range(high):
        for c in range(halves):
            at = 8 + i * HALO
            u = jnp.where(upper_sublanes(1)[0], flat[0, c, at : at + 8, :], flat[1, c, at - HALO : at + HALO, :])
            value = silu(u)
            for ref, v in ((base, u), (act0, value)):
                ref[c, i, LEFT - HALO : LEFT, :] = v[0:HALO]
                ref[c, i, LEFT + cols_here : LEFT + cols_here + HALO, :] = v[HALO:8]
    ring(0, act0, w0, base, mid, act1, step_size, shape, place)

    @pl.when(depth == 1)
    def _():
        w_parts[1].wait_recv()

    ring(1, act1, w1, mid, end, act2, step_size, shape, place)

    @pl.when(depth == 1)
    def _():
        for copy in passes:
            copy.wait_send()


def ring_kernel(
    sizes, keep, states, acts, w2, w3, mid2_in, fin_in, act3_in,
    fine_hbm, coarse_hbm, mid2, fin, act3, store_sem,
):
    nrows, ncols, step_size = sizes
    mid, end, act2 = states.at[1], states.at[2], acts.at[2]
    halves = fin.shape[0]
    rows_here, cols_here = fine_hbm.shape[1:3]
    depth, row, col = lax.axis_index("depth"), lax.axis_index("rows"), lax.axis_index("cols")
    shape, place = (halves, rows_here, cols_here), (nrows, ncols, row, col)

    def stores(ref, target, slot):
        return [
            pltpu.make_async_copy(
                ref.at[c, pl.ds(HALO, rows_here), pl.ds(LEFT, cols_here), :],
                target.at[:, :, pl.ds(c * LANES, LANES)],
                store_sem.at[slot, c],
            )
            for c in range(halves)
        ]

    def start(copies):
        for copy in copies:
            copy.start()

    @pl.when(depth == 0)
    def _():
        kept = pltpu.make_async_copy(keep, coarse_hbm.at[0], store_sem.at[2, 0])
        both = stores(mid, fine_hbm.at[0], 0) + stores(end, fine_hbm.at[1], 1)
        start([kept] + both)
        for copy in [kept] + both:
            copy.wait()

    @pl.when(depth == 1)
    def _():
        early = stores(end, coarse_hbm.at[0], 0)
        start(early)
        ring(2, act2, w2, end, mid2, act3, step_size, shape, place)
        middle = stores(mid2, fine_hbm.at[0], 1)
        start(middle)

        def late(k, c):
            rows = rows_here // 2
            return pltpu.make_async_copy(
                fin.at[c, pl.ds(HALO + k * rows, rows), pl.ds(LEFT, cols_here), :],
                fine_hbm.at[1, pl.ds(k * rows, rows), :, pl.ds(c * LANES, LANES)],
                store_sem.at[2 * k, c],
            )

        def send(k):
            for c in range(halves):
                late(k, c).start()

        for copy in early:
            copy.wait()
        ring(3, act3, w3, mid2, fin, None, step_size, shape, place)
        send(0)
        send(1)
        for copy in middle + [late(k, c) for k in range(2) for c in range(halves)]:
            copy.wait()


def two_sections(section_states, weights):
    _, rows_here, cols_here, channels = section_states.shape
    halves = channels // LANES
    high, wide = rows_here + 2 * HALO, cols_here + 2 * LEFT
    sizes = (lax.axis_size("rows"), lax.axis_size("cols"), 2.0 / (2 * lax.axis_size("depth")))
    f32, bf16, vmem = jnp.float32, jnp.bfloat16, pltpu.VMEM
    state = vmem((halves, high, wide, LANES), f32)
    weight = vmem((9 * channels, channels), bf16)
    flat_weights = weights.reshape(2, 9 * channels, channels)
    any_space, in_vmem = pl.BlockSpec(memory_space=pl.ANY), pl.BlockSpec(memory_space=vmem)
    dma = pltpu.SemaphoreType.DMA
    kept = vmem((rows_here, cols_here, channels), f32)
    three = vmem((3, halves, high, wide, LANES), f32)
    keep, states, mid2, fin, acts, act3, w2, w3 = pl.pallas_call(
        functools.partial(gather_kernel, sizes),
        out_shape=(kept, three, state, state, three, state, weight, weight),
        in_specs=[pl.BlockSpec(memory_space=pltpu.HBM)] * 2,
        out_specs=[in_vmem] * 8,
        scratch_shapes=[
            state, state, vmem((2, 9 * channels, channels), bf16),
            vmem((halves, rows_here - 2, 8, LANES), f32), vmem((halves, rows_here - 2, 8, LANES), f32),
            vmem((2, halves, high * HALO + 16, LANES), f32),
            vmem((2, HALO * cols_here, channels), bf16),
            vmem((2, rows_here * HALO, channels), bf16),
            vmem((2, HALO * cols_here, channels), bf16),
            vmem((2, high * HALO, channels), bf16),
            dma((halves + 1,)), dma((halves + 6,)), dma((2,)), dma((8,)),
            pltpu.SemaphoreType.REGULAR((1,)),
        ],
        compiler_params=pltpu.CompilerParams(
            collective_id=0, has_side_effects=True, vmem_limit_bytes=LIMIT
        ),
    )(
        pltpu.with_memory_space_constraint(section_states, pltpu.HBM),
        pltpu.with_memory_space_constraint(flat_weights, pltpu.HBM),
    )
    outs = pl.pallas_call(
        functools.partial(ring_kernel, sizes),
        out_shape=(
            jax.ShapeDtypeStruct((2, rows_here, cols_here, channels), f32),
            jax.ShapeDtypeStruct((1, rows_here, cols_here, channels), f32),
        ) + (state,) * 3,
        in_specs=[in_vmem] * 8,
        out_specs=[any_space] * 2 + [in_vmem] * 3,
        input_output_aliases={5: 2, 6: 3, 7: 4},
        scratch_shapes=[dma((3, halves))],
        compiler_params=pltpu.CompilerParams(vmem_limit_bytes=LIMIT),
    )(keep, states, acts, w2, w3, mid2, fin, act3)
    return outs[0], outs[1]


def on_device(section_states, weights):
    _, rows_here, cols_here, channels = section_states.shape
    tiles = rows_here % 8 == 0 and cols_here % 8 == 0 and channels % LANES == 0
    if lax.axis_size("depth") == 2 and tiles and min(rows_here, cols_here) >= 16:
        return two_sections(section_states, weights)
    return chain_on_device(section_states, weights)


def solution(mesh):
    in_specs = (P("depth", "rows", "cols", None), P("depth", None, None, None, None))
    out_specs = (P("depth", "rows", "cols", None), P("depth", "rows", "cols", None))
    return jax.shard_map(
        on_device, mesh=mesh, in_specs=in_specs, out_specs=out_specs, check_vma=False
    )
```

```python
import functools

import jax
import jax.numpy as jnp
from jax import lax
from jax.experimental import pallas as pl
from jax.experimental.pallas import tpu as pltpu
from jax.sharding import PartitionSpec as P

MESH = pl.DeviceIdType.MESH
HALO = 4
LANES = 128
LIMIT = 32 * 1024 * 1024


def padded_2(shard, sides, width):
    for axis, dim in sides:
        size, length = (lax.axis_size(axis), shard.shape[dim])
        up = [(i, (i + 1) % size) for i in range(size - 1)]
        down = [(j, i) for i, j in up]
        last = lax.slice_in_dim(shard, length - width, length, axis=dim)
        initial = lax.slice_in_dim(shard, 0, width, axis=dim)
        before = lax.ppermute(last, axis, up)
        after = lax.ppermute(initial, axis, down)
        shard = jnp.concatenate([before, shard, after], axis=dim)
    return shard


def shifted_2(block, axis, distance):
    devices = range(lax.axis_size(axis))
    route = [(i - distance, i) for i in devices if i - distance in devices]
    return lax.ppermute(block, axis, route)


def activate(field):
    return jax.nn.silu(field).astype(jnp.bfloat16)


def apply_stencil(padded, flat_weight, out_rows, out_cols):
    channels = padded.shape[2]
    patches = jnp.concatenate(
        [
            padded[shift_row : shift_row + out_rows, shift_col : shift_col + out_cols]
            for shift_row in range(3)
            for shift_col in range(3)
        ],
        axis=2,
    )
    summed = jnp.dot(
        patches.reshape(out_rows * out_cols, 9 * channels),
        flat_weight,
        preferred_element_type=jnp.float32,
    )
    return summed.reshape(out_rows, out_cols, channels)


def section_pass(anchor, first_weight, second_weight, step_size):
    rows_here, cols_here, channels = anchor.shape
    widened = padded_2(anchor, (("rows", 0), ("cols", 1)), 2)
    slope_wide = apply_stencil(activate(widened), first_weight, rows_here + 2, cols_here + 2)
    middle_wide = widened[1:-1, 1:-1] + step_size * slope_wide
    row_global = lax.axis_index("rows") * rows_here - 1 + jnp.arange(rows_here + 2)
    col_global = lax.axis_index("cols") * cols_here - 1 + jnp.arange(cols_here + 2)
    inside_rows = (row_global >= 0) & (row_global < rows_here * lax.axis_size("rows"))
    inside_cols = (col_global >= 0) & (col_global < cols_here * lax.axis_size("cols"))
    inside = inside_rows[:, None] & inside_cols[None, :]
    second_act = jnp.where(inside[:, :, None], activate(middle_wide), jnp.zeros((), jnp.bfloat16))
    first_slope = slope_wide[1:-1, 1:-1]
    middle = middle_wide[1:-1, 1:-1]
    second_slope = apply_stencil(second_act, second_weight, rows_here, cols_here)
    ending = middle + step_size * second_slope
    return (first_slope, middle, ending)


def chain_on_device(section_states, weights):
    rows_here, cols_here, channels = section_states.shape[1:]
    ndepth = lax.axis_size("depth")
    position = lax.axis_index("depth")
    step_size = 2.0 / (2 * ndepth)
    first_weight = weights[0].reshape(9 * channels, channels)
    second_weight = weights[1].reshape(9 * channels, channels)
    anchor = section_states[0]
    first_slope, middle, ending = section_pass(anchor, first_weight, second_weight, step_size)
    jump = ending - (anchor + 2.0 * step_size * first_slope)

    def chain_turn(step_index, current):
        padded = padded_2(activate(current), (("rows", 0), ("cols", 1)), 1)
        advanced = (
            current
            + 2.0 * step_size * apply_stencil(padded, first_weight, rows_here, cols_here)
            + jump
        )
        shifted = shifted_2(advanced, "depth", 1)
        return jnp.where(position == 0, anchor, shifted)

    corrected = lax.fori_loop(0, ndepth - 1, chain_turn, anchor)
    final_slope, final_middle, final_ending = section_pass(
        corrected, first_weight, second_weight, step_size
    )
    fine_states = jnp.stack([final_middle, final_ending])
    return (fine_states, corrected[None])


DIRECTIONS = ((-1, 0), (1, 0), (0, -1), (0, 1), (-1, -1), (-1, 1), (1, -1), (1, 1))
LEFT = 8


def silu(u):
    half = 0.5 * u
    return half + half * jnp.tanh(half)


def as_rows(block):
    return block.reshape(-1, LANES).astype(jnp.bfloat16)


def tap_dot(windows, halves, weight):
    lhs = []
    for a in range(3):
        for b in range(3):
            for c in range(halves):
                parts = [as_rows(window(c, a, b)) for window in windows]
                lhs.append(parts[0] if len(parts) == 1 else jnp.concatenate(parts, axis=0))
    return jnp.dot(jnp.concatenate(lhs, axis=1), weight[...], preferred_element_type=jnp.float32)


def lanes_of(block, c, shape):
    return block[:, c * LANES : (c + 1) * LANES].reshape(shape)


def upper_sublanes(rows):
    return lax.broadcasted_iota(jnp.int32, (rows, 8, LANES), 1) < HALO


def packed(ref, c, first_row, rows, left, right):
    near = ref[c, pl.ds(first_row, rows), left : left + 8, :]
    far = ref[c, pl.ds(first_row, rows), right : right + 8, :]
    return jnp.where(upper_sublanes(rows), near, far)


def store_packed(ref, c, first_row, left, right, value):
    whole = pl.ds(first_row, value.shape[0])
    ref[c, whole, left : left + HALO, :] = value[:, 0:HALO]
    ref[c, whole, right + HALO : right + 8, :] = value[:, HALO:8]


def largest_divisor(total, limit):
    return max(n for n in range(1, limit + 1) if total % n == 0)


def once():
    return jnp.minimum(lax.axis_index("rows"), 0) + 1


def interior(layer, act, weight, before, after, act_after, step_size, shape):
    halves, rows_here, cols_here = shape
    narrow = layer == 3 and cols_here == 16
    left, wide = (LEFT + HALO, cols_here - 2 * HALO) if narrow else (LEFT, cols_here)
    exact = layer >= 2
    first, rows = (HALO + 1 + layer, rows_here - 2 - 2 * layer) if exact else (HALO + 1, rows_here - 2)
    n = rows if exact else largest_divisor(rows, 30)

    def chunk(k, _):
        at = first + k * n

        def window(c, a, b):
            return act[c, pl.ds(at + a - 1, n), left + b - 1 : left + b - 1 + wide, :]

        acc = step_size * tap_dot([window], halves, weight)
        for c in range(halves):
            here = (c, pl.ds(at, n), slice(left, left + wide), slice(None))
            u = before[here] + lanes_of(acc, c, (n, wide, LANES))
            after[here] = u
            if act_after is not None:
                act_after[here] = silu(u)
        return 0

    lax.fori_loop(0, once() if rows == n else rows // n, chunk, 0)


def ring(layer, act, weight, before, after, act_after, step_size, shape, place):
    halves, rows_here, cols_here = shape
    nrows, ncols, row, col = place
    high = rows_here + 2 * HALO
    first, rows = 1 + layer, high - 2 - 2 * layer
    tops = (first, high - HALO - first)
    narrow = layer == 3 and cols_here == 16
    left, wide = (LEFT + HALO, cols_here - 2 * HALO) if narrow else (LEFT, cols_here)
    near, far = HALO + layer, LEFT + cols_here - 6 - layer
    above = jnp.where(row > 0, 1.0, 0.0)
    below = jnp.where(row < nrows - 1, 1.0, 0.0)
    sub = lax.broadcasted_iota(jnp.int32, (1, 8, LANES), 1)
    j = jnp.where(sub < HALO, sub + (layer - 3), sub + (cols_here - 5 - layer)) + col * cols_here
    held = jnp.where((j >= 0) & (j < ncols * cols_here), 1.0, 0.0)
    m = HALO * wide

    def rows_held(at, block):
        i = lax.broadcasted_iota(jnp.int32, block, 0) + at
        return jnp.where(i < HALO, above, jnp.where(i >= high - HALO, below, 1.0))

    def whole(_, carry):
        def strip(at):
            return lambda c, a, b: act[c, pl.ds(at + a - 1, HALO), left + b - 1 : left + b - 1 + wide, :]

        def sides(c, a, b):
            return packed(act, c, first + a - 1, rows, near + b, far + b)

        acc = step_size * tap_dot([strip(at) for at in tops] + [sides], halves, weight)
        for c in range(halves):
            for k, at in enumerate(tops):
                here = (c, pl.ds(at, HALO), slice(left, left + wide), slice(None))
                u = before[here] + lanes_of(acc[k * m : (k + 1) * m], c, (HALO, wide, LANES))
                after[here] = u
                if act_after is not None:
                    act_after[here] = silu(u) * rows_held(at, u.shape)
            u = packed(before, c, first, rows, near + 1, far + 1) + lanes_of(acc[2 * m :], c, (rows, 8, LANES))
            store_packed(after, c, first, near + 1, far + 1, u)
            if act_after is not None:
                value = silu(u) * (held * rows_held(first, u.shape))
                store_packed(act_after, c, first, near + 1, far + 1, value)
        return carry

    lax.fori_loop(0, once(), whole, 0)


def gather_kernel(
    sizes, x_hbm, w_hbm,
    keep, states, mid2, fin, acts, act3, w2, w3,
    land_mid, land_end, w01, mid_side, land_side, flat, send_row, send_col, recv_row, recv_side,
    load_sem, part_sem, pass_sem, halo_sem, later,
):
    nrows, ncols, step_size = sizes
    base, mid, end = [states.at[k] for k in range(3)]
    act0, act1, act2 = [acts.at[k] for k in range(3)]
    w0, w1 = w01.at[0], w01.at[1]
    halves, high = land_mid.shape[:2]
    rows_here, cols_here = keep.shape[:2]
    depth, row, col = lax.axis_index("depth"), lax.axis_index("rows"), lax.axis_index("cols")
    shape, place = (halves, rows_here, cols_here), (nrows, ncols, row, col)
    partner = (1 - depth, row, col)
    corner = HALO * HALO
    barrier = pltpu.get_barrier_semaphore()

    def lanes(c):
        return pl.ds(c * LANES, LANES)

    def local(src, dst, k):
        return pltpu.make_async_copy(src, dst, load_sem.at[k])

    def to_partner(src, dst, k, sem=part_sem):
        return pltpu.make_async_remote_copy(
            src_ref=src, dst_ref=dst, send_sem=sem.at[k], recv_sem=sem.at[k],
            device_id=partner, device_id_type=MESH,
        )

    def exists_at(step):
        there_row, there_col = row + step[0], col + step[1]
        exists = (there_row >= 0) & (there_row < nrows) & (there_col >= 0) & (there_col < ncols)
        return exists, there_row, there_col

    odd, even = lax.rem(row, 2) == 1, lax.rem(row, 2) == 0

    def pick(step, always, sometimes, first, second):
        if step == always:
            return True, None
        if step in sometimes:
            return first, second
        return None, True

    def early(step):
        return pick(step, (0, -1), ((-1, 0), (-1, -1)), odd, even)

    def early_seen_by(step):
        return pick(step, (0, 1), ((1, 0), (1, 1)), even, odd)

    def run_if(exists, also, action):
        if also is True:
            pl.when(exists)(action)
        elif also is not None:
            pl.when(exists)(lambda: pl.when(also)(action))

    def count_of(part):
        count = jnp.int32(1)
        for step in DIRECTIONS:
            also = early(step)[part]
            if also is not None:
                there = exists_at(step)[0]
                there = there if also is True else there & also
                count = count + jnp.where(there, 1, 0)
        return count

    def own(c):
        return base.at[c, pl.ds(HALO, rows_here), pl.ds(LEFT, cols_here), :]

    x_loads = [local(x_hbm.at[0, :, :, lanes(c)], own(c), c) for c in range(halves)]
    x_parts = [to_partner(x_hbm.at[0, :, :, lanes(c)], own(c), c) for c in range(halves)]
    keep_load = local(x_hbm.at[0], keep, 1)
    w_loads = [local(w_hbm.at[0], w0, halves), local(w_hbm.at[1], w1, 0)]
    late_loads = [local(w_hbm.at[0], w2, 0), local(w_hbm.at[1], w3, 1)]
    w_parts = [to_partner(w_hbm.at[0], w0, halves), to_partner(w_hbm.at[1], w1, halves + 1)]

    def inner(ref, k):
        return ref.at[:, pl.ds(HALO + k, rows_here - 2 * k), pl.ds(LEFT, cols_here), :]

    def two_rows(ref, at):
        return ref.at[:, pl.ds(at, 2), pl.ds(LEFT, cols_here), :]

    edge_rows = (HALO + 1, HALO + rows_here - 3)
    far_side = LEFT + cols_here - 8
    mid_parts = [to_partner(mid_side, land_side, halves + 2)] + [
        to_partner(two_rows(mid, at), two_rows(land_mid, at), halves + 4 + k) for k, at in enumerate(edge_rows)
    ]
    end_part = to_partner(inner(end, 2), inner(land_end, 2), halves + 3)
    passes = [
        to_partner(ref, ref, k, pass_sem) for k, ref in enumerate((recv_row, recv_side))
    ]

    def activate_rows(source, target, first, rows, copied=None):
        for c in range(halves):
            here = (c, pl.ds(first, rows), slice(LEFT, LEFT + cols_here), slice(None))
            u = source[here]
            target[here] = silu(u)
            if copied is not None:
                copied[here] = u

    copies = []
    for k, (dr, dc) in enumerate(DIRECTIONS):
        exists, there_row, there_col = exists_at((dr, dc))
        side = (dc + 1) // 2
        mine = {-1: (0, corner), 1: ((rows_here - HALO) * HALO, corner), 0: (0, rows_here * HALO)}[dr]
        theirs = {1: (0, corner), -1: (high * HALO - corner, corner), 0: (corner, rows_here * HALO)}[dr]
        if dc == 0:
            src, dst, here = send_row.at[(dr + 1) // 2], recv_row.at[(1 - dr) // 2], recv_row.at[(dr + 1) // 2]
            empty = (recv_row, (dr + 1) // 2, slice(None))
        else:
            back = {-1: (0, corner), 1: (high * HALO - corner, corner), 0: (corner, rows_here * HALO)}[dr]
            src = send_col.at[side, pl.ds(*mine)]
            dst = recv_side.at[1 - side, pl.ds(*theirs)]
            here = recv_side.at[side, pl.ds(*back)]
            empty = (recv_side, side, slice(back[0], back[0] + back[1]))

        def remote(src, dst, slot):
            return pltpu.make_async_remote_copy(
                src_ref=src, dst_ref=dst, send_sem=halo_sem.at[k], recv_sem=halo_sem.at[slot],
                device_id=(1 - depth, there_row, there_col), device_id_type=MESH,
            )

        opposite = DIRECTIONS.index((-dr, -dc))
        copies.append((exists, remote(src, dst, opposite), remote(src, here, k), empty))
    order = (4, 5, 6, 7, 2, 3, 0, 1)

    def signal(target):
        pl.semaphore_signal(barrier, inc=1, device_id=target, device_id_type=MESH)

    def send_halos(part):
        for k in order:
            exists, copy, _, _ = copies[k]
            run_if(exists, early(DIRECTIONS[k])[part], copy.start)

    @pl.when(depth == 0)
    def _():
        for copy in x_loads + w_loads[:1]:
            copy.start()
        signal(partner)
        pl.semaphore_wait(barrier, count_of(0))
        for copy in x_parts + w_parts[:1]:
            copy.start()
        for copy in x_loads:
            copy.wait()
        w_loads[1].start()
        for side in range(2):
            top = HALO if side == 0 else rows_here
            left = LEFT if side == 0 else LEFT + cols_here - HALO
            for c in range(halves):
                send_row[side, :, lanes(c)] = as_rows(base[c, top : top + HALO, LEFT : LEFT + cols_here, :])
                for i in range(rows_here):
                    flat[side, c, i * HALO : (i + 1) * HALO, :] = base[c, HALO + i, left : left + HALO, :]
            for c in range(halves):
                send_col[side, :, lanes(c)] = flat[side, c, 0 : rows_here * HALO, :].astype(jnp.bfloat16)
        send_halos(0)
        activate_rows(base, act0, HALO, rows_here)
        w_loads[0].wait()
        first = (row == 0) & (col == 0)

        def send_rest():
            pl.semaphore_wait(later.at[0], 1)
            send_halos(1)

        def both(layer, _):
            @pl.when(layer == 1)
            def _():
                for c in range(halves):
                    mid_side[c] = packed(mid, c, HALO + 1, rows_here - 2, LEFT, far_side)
                for copy in mid_parts:
                    copy.start()
                pl.when(row + col > 0)(send_rest)
                w_loads[1].wait()

            interior(
                0, acts.at[layer], w01.at[layer], states.at[layer], states.at[layer + 1],
                acts.at[layer + 1], step_size, shape,
            )
            return 0

        lax.fori_loop(0, 2, both, 0)
        keep_load.start()
        end_part.start()
        w_parts[1].start()
        pl.when(first)(send_rest)
        for copy in mid_parts:
            copy.wait_send()
        end_part.wait_send()
        keep_load.wait()
        for exists, copy, _, _ in copies:
            pl.when(exists)(copy.wait_send)
        for copy in x_parts + w_parts:
            copy.wait_send()
        for copy in passes:
            copy.wait_recv()

    @pl.when(depth == 1)
    def _():
        for copy in late_loads:
            copy.start()
        signal(partner)
        for step in DIRECTIONS:
            exists, there_row, there_col = exists_at(step)
            for side, also in enumerate(early_seen_by(step)):
                core = 1 - depth if side == 0 else depth
                run_if(exists, also, functools.partial(signal, (core, there_row, there_col)))
        for step, (_, _, _, (ref, at, rows)) in zip(DIRECTIONS, copies):
            _, there_row, there_col = exists_at(step)
            outside = (there_row < 0) | (there_row >= nrows) | (there_col < 0) | (there_col >= ncols)

            @pl.when(outside)
            def _(ref=ref, at=at, rows=rows):
                ref[at, rows, :] = jnp.zeros_like(ref[at, rows, :])

        pl.semaphore_wait(barrier, count_of(1))
        pl.semaphore_signal(later.at[0], inc=1, device_id=partner, device_id_type=MESH)
        for copy in x_parts:
            copy.wait_recv()
        activate_rows(base, act0, HALO, rows_here)
        for copy in mid_parts:
            copy.wait_recv()
        for at in edge_rows:
            activate_rows(land_mid, act1, at, 2, mid)
        for c in range(halves):
            u = land_side[c]
            store_packed(mid, c, HALO + 1, LEFT, far_side, u)
            store_packed(act1, c, HALO + 1, LEFT, far_side, silu(u))
        end_part.wait_recv()
        activate_rows(land_end, act2, HALO + 2, rows_here - 4, end)
        def forward():
            for exists, _, arrival, _ in copies:
                pl.when(exists)(arrival.wait_recv)
            for copy in passes:
                copy.start()

        late_loads[0].wait()
        interior(2, act2, w2, end, mid2, act3, step_size, shape)
        pl.when((row == 0) & (col == 0))(forward)
        late_loads[1].wait()
        interior(3, act3, w3, mid2, fin, None, step_size, shape)
        pl.when(row + col > 0)(forward)
        w_parts[0].wait_recv()

    for side in range(2):
        for c in range(halves):
            flat[side, c, 8 : 8 + high * HALO, :] = recv_side[side, :, lanes(c)].astype(jnp.float32)
            u = recv_row[side, :, lanes(c)].astype(jnp.float32).reshape(HALO, cols_here, LANES)
            rows = slice(0, HALO) if side == 0 else slice(high - HALO, high)
            base[c, rows, LEFT : LEFT + cols_here, :] = u
            act0[c, rows, LEFT : LEFT + cols_here, :] = silu(u)
    for i in range(high):
        for c in range(halves):
            at = 8 + i * HALO
            u = jnp.where(upper_sublanes(1)[0], flat[0, c, at : at + 8, :], flat[1, c, at - HALO : at + HALO, :])
            value = silu(u)
            for ref, v in ((base, u), (act0, value)):
                ref[c, i, LEFT - HALO : LEFT, :] = v[0:HALO]
                ref[c, i, LEFT + cols_here : LEFT + cols_here + HALO, :] = v[HALO:8]
    ring(0, act0, w0, base, mid, act1, step_size, shape, place)

    @pl.when(depth == 1)
    def _():
        w_parts[1].wait_recv()

    ring(1, act1, w1, mid, end, act2, step_size, shape, place)

    @pl.when(depth == 1)
    def _():
        for copy in passes:
            copy.wait_send()


def ring_kernel(
    sizes, keep, states, acts, w2, w3, mid2_in, fin_in, act3_in,
    fine_hbm, coarse_hbm, mid2, fin, act3, store_sem,
):
    nrows, ncols, step_size = sizes
    mid, end, act2 = states.at[1], states.at[2], acts.at[2]
    halves = fin.shape[0]
    rows_here, cols_here = fine_hbm.shape[1:3]
    depth, row, col = lax.axis_index("depth"), lax.axis_index("rows"), lax.axis_index("cols")
    shape, place = (halves, rows_here, cols_here), (nrows, ncols, row, col)

    def stores(ref, target, slot):
        return [
            pltpu.make_async_copy(
                ref.at[c, pl.ds(HALO, rows_here), pl.ds(LEFT, cols_here), :],
                target.at[:, :, pl.ds(c * LANES, LANES)],
                store_sem.at[slot, c],
            )
            for c in range(halves)
        ]

    def start(copies):
        for copy in copies:
            copy.start()

    @pl.when(depth == 0)
    def _():
        kept = pltpu.make_async_copy(keep, coarse_hbm.at[0], store_sem.at[2, 0])
        both = stores(mid, fine_hbm.at[0], 0) + stores(end, fine_hbm.at[1], 1)
        start([kept] + both)
        for copy in [kept] + both:
            copy.wait()

    @pl.when(depth == 1)
    def _():
        early = stores(end, coarse_hbm.at[0], 0)
        start(early)
        ring(2, act2, w2, end, mid2, act3, step_size, shape, place)
        middle = stores(mid2, fine_hbm.at[0], 1)
        start(middle)

        ring(3, act3, w3, mid2, fin, None, step_size, shape, place)
        last = stores(fin, fine_hbm.at[1], 2)
        start(last)
        for copy in early + middle + last:
            copy.wait()


def two_sections(section_states, weights):
    _, rows_here, cols_here, channels = section_states.shape
    halves = channels // LANES
    high, wide = rows_here + 2 * HALO, cols_here + 2 * LEFT
    sizes = (lax.axis_size("rows"), lax.axis_size("cols"), 2.0 / (2 * lax.axis_size("depth")))
    f32, bf16, vmem = jnp.float32, jnp.bfloat16, pltpu.VMEM
    state = vmem((halves, high, wide, LANES), f32)
    weight = vmem((9 * channels, channels), bf16)
    flat_weights = weights.reshape(2, 9 * channels, channels)
    any_space, in_vmem = pl.BlockSpec(memory_space=pl.ANY), pl.BlockSpec(memory_space=vmem)
    dma = pltpu.SemaphoreType.DMA
    kept = vmem((rows_here, cols_here, channels), f32)
    three = vmem((3, halves, high, wide, LANES), f32)
    keep, states, mid2, fin, acts, act3, w2, w3 = pl.pallas_call(
        functools.partial(gather_kernel, sizes),
        out_shape=(kept, three, state, state, three, state, weight, weight),
        in_specs=[pl.BlockSpec(memory_space=pltpu.HBM)] * 2,
        out_specs=[in_vmem] * 8,
        scratch_shapes=[
            state, state, vmem((2, 9 * channels, channels), bf16),
            vmem((halves, rows_here - 2, 8, LANES), f32), vmem((halves, rows_here - 2, 8, LANES), f32),
            vmem((2, halves, high * HALO + 16, LANES), f32),
            vmem((2, HALO * cols_here, channels), bf16),
            vmem((2, rows_here * HALO, channels), bf16),
            vmem((2, HALO * cols_here, channels), bf16),
            vmem((2, high * HALO, channels), bf16),
            dma((halves + 1,)), dma((halves + 6,)), dma((2,)), dma((8,)),
            pltpu.SemaphoreType.REGULAR((1,)),
        ],
        compiler_params=pltpu.CompilerParams(
            collective_id=0, has_side_effects=True, vmem_limit_bytes=LIMIT
        ),
    )(
        pltpu.with_memory_space_constraint(section_states, pltpu.HBM),
        pltpu.with_memory_space_constraint(flat_weights, pltpu.HBM),
    )
    outs = pl.pallas_call(
        functools.partial(ring_kernel, sizes),
        out_shape=(
            jax.ShapeDtypeStruct((2, rows_here, cols_here, channels), f32),
            jax.ShapeDtypeStruct((1, rows_here, cols_here, channels), f32),
        ) + (state,) * 3,
        in_specs=[in_vmem] * 8,
        out_specs=[any_space] * 2 + [in_vmem] * 3,
        input_output_aliases={5: 2, 6: 3, 7: 4},
        scratch_shapes=[dma((3, halves))],
        compiler_params=pltpu.CompilerParams(vmem_limit_bytes=LIMIT),
    )(keep, states, acts, w2, w3, mid2, fin, act3)
    return outs[0], outs[1]


def on_device(section_states, weights):
    _, rows_here, cols_here, channels = section_states.shape
    tiles = rows_here % 8 == 0 and cols_here % 8 == 0 and channels % LANES == 0
    if lax.axis_size("depth") == 2 and tiles and min(rows_here, cols_here) >= 16:
        return two_sections(section_states, weights)
    return chain_on_device(section_states, weights)


def solution(mesh):
    in_specs = (P("depth", "rows", "cols", None), P("depth", None, None, None, None))
    out_specs = (P("depth", "rows", "cols", None), P("depth", "rows", "cols", None))
    return jax.shard_map(
        on_device, mesh=mesh, in_specs=in_specs, out_specs=out_specs, check_vma=False
    )
```

```python
import functools

import jax
import jax.numpy as jnp
from jax import lax
from jax.experimental import pallas as pl
from jax.experimental.pallas import tpu as pltpu
from jax.sharding import PartitionSpec as P

MESH = pl.DeviceIdType.MESH
HALO = 4
LANES = 128
LIMIT = 32 * 1024 * 1024


def padded_2(shard, sides, width):
    for axis, dim in sides:
        size, length = (lax.axis_size(axis), shard.shape[dim])
        up = [(i, (i + 1) % size) for i in range(size - 1)]
        down = [(j, i) for i, j in up]
        last = lax.slice_in_dim(shard, length - width, length, axis=dim)
        initial = lax.slice_in_dim(shard, 0, width, axis=dim)
        before = lax.ppermute(last, axis, up)
        after = lax.ppermute(initial, axis, down)
        shard = jnp.concatenate([before, shard, after], axis=dim)
    return shard


def shifted_2(block, axis, distance):
    devices = range(lax.axis_size(axis))
    route = [(i - distance, i) for i in devices if i - distance in devices]
    return lax.ppermute(block, axis, route)


def activate(field):
    return jax.nn.silu(field).astype(jnp.bfloat16)


def apply_stencil(padded, flat_weight, out_rows, out_cols):
    channels = padded.shape[2]
    patches = jnp.concatenate(
        [
            padded[shift_row : shift_row + out_rows, shift_col : shift_col + out_cols]
            for shift_row in range(3)
            for shift_col in range(3)
        ],
        axis=2,
    )
    summed = jnp.dot(
        patches.reshape(out_rows * out_cols, 9 * channels),
        flat_weight,
        preferred_element_type=jnp.float32,
    )
    return summed.reshape(out_rows, out_cols, channels)


def section_pass(anchor, first_weight, second_weight, step_size):
    rows_here, cols_here, channels = anchor.shape
    widened = padded_2(anchor, (("rows", 0), ("cols", 1)), 2)
    slope_wide = apply_stencil(activate(widened), first_weight, rows_here + 2, cols_here + 2)
    middle_wide = widened[1:-1, 1:-1] + step_size * slope_wide
    row_global = lax.axis_index("rows") * rows_here - 1 + jnp.arange(rows_here + 2)
    col_global = lax.axis_index("cols") * cols_here - 1 + jnp.arange(cols_here + 2)
    inside_rows = (row_global >= 0) & (row_global < rows_here * lax.axis_size("rows"))
    inside_cols = (col_global >= 0) & (col_global < cols_here * lax.axis_size("cols"))
    inside = inside_rows[:, None] & inside_cols[None, :]
    second_act = jnp.where(inside[:, :, None], activate(middle_wide), jnp.zeros((), jnp.bfloat16))
    first_slope = slope_wide[1:-1, 1:-1]
    middle = middle_wide[1:-1, 1:-1]
    second_slope = apply_stencil(second_act, second_weight, rows_here, cols_here)
    ending = middle + step_size * second_slope
    return (first_slope, middle, ending)


def chain_on_device(section_states, weights):
    rows_here, cols_here, channels = section_states.shape[1:]
    ndepth = lax.axis_size("depth")
    position = lax.axis_index("depth")
    step_size = 2.0 / (2 * ndepth)
    first_weight = weights[0].reshape(9 * channels, channels)
    second_weight = weights[1].reshape(9 * channels, channels)
    anchor = section_states[0]
    first_slope, middle, ending = section_pass(anchor, first_weight, second_weight, step_size)
    jump = ending - (anchor + 2.0 * step_size * first_slope)

    def chain_turn(step_index, current):
        padded = padded_2(activate(current), (("rows", 0), ("cols", 1)), 1)
        advanced = (
            current
            + 2.0 * step_size * apply_stencil(padded, first_weight, rows_here, cols_here)
            + jump
        )
        shifted = shifted_2(advanced, "depth", 1)
        return jnp.where(position == 0, anchor, shifted)

    corrected = lax.fori_loop(0, ndepth - 1, chain_turn, anchor)
    final_slope, final_middle, final_ending = section_pass(
        corrected, first_weight, second_weight, step_size
    )
    fine_states = jnp.stack([final_middle, final_ending])
    return (fine_states, corrected[None])


DIRECTIONS = ((-1, 0), (1, 0), (0, -1), (0, 1), (-1, -1), (-1, 1), (1, -1), (1, 1))
LEFT = 8


def silu(u):
    half = 0.5 * u
    return half + half * jnp.tanh(half)


def as_rows(block):
    return block.reshape(-1, LANES).astype(jnp.bfloat16)


def tap_dot(windows, halves, weight):
    lhs = []
    for a in range(3):
        for b in range(3):
            for c in range(halves):
                parts = [as_rows(window(c, a, b)) for window in windows]
                lhs.append(parts[0] if len(parts) == 1 else jnp.concatenate(parts, axis=0))
    return jnp.dot(jnp.concatenate(lhs, axis=1), weight[...], preferred_element_type=jnp.float32)


def lanes_of(block, c, shape):
    return block[:, c * LANES : (c + 1) * LANES].reshape(shape)


def upper_sublanes(rows):
    return lax.broadcasted_iota(jnp.int32, (rows, 8, LANES), 1) < HALO


def packed(ref, c, first_row, rows, left, right):
    near = ref[c, pl.ds(first_row, rows), left : left + 8, :]
    far = ref[c, pl.ds(first_row, rows), right : right + 8, :]
    return jnp.where(upper_sublanes(rows), near, far)


def store_packed(ref, c, first_row, left, right, value):
    whole = pl.ds(first_row, value.shape[0])
    ref[c, whole, left : left + HALO, :] = value[:, 0:HALO]
    ref[c, whole, right + HALO : right + 8, :] = value[:, HALO:8]


def largest_divisor(total, limit):
    return max(n for n in range(1, limit + 1) if total % n == 0)


def once():
    return jnp.minimum(lax.axis_index("rows"), 0) + 1


def interior(layer, act, weight, before, after, act_after, step_size, shape):
    halves, rows_here, cols_here = shape
    narrow = layer == 3 and cols_here == 16
    left, wide = (LEFT + HALO, cols_here - 2 * HALO) if narrow else (LEFT, cols_here)
    exact = layer >= 2
    first, rows = (HALO + 1 + layer, rows_here - 2 - 2 * layer) if exact else (HALO + 1, rows_here - 2)
    n = rows if exact else largest_divisor(rows, 30)

    def chunk(k, _):
        at = first + k * n

        def window(c, a, b):
            return act[c, pl.ds(at + a - 1, n), left + b - 1 : left + b - 1 + wide, :]

        acc = step_size * tap_dot([window], halves, weight)
        for c in range(halves):
            here = (c, pl.ds(at, n), slice(left, left + wide), slice(None))
            u = before[here] + lanes_of(acc, c, (n, wide, LANES))
            after[here] = u
            if act_after is not None:
                act_after[here] = silu(u)
        return 0

    lax.fori_loop(0, once() if rows == n else rows // n, chunk, 0)


def ring(layer, act, weight, before, after, act_after, step_size, shape, place):
    halves, rows_here, cols_here = shape
    nrows, ncols, row, col = place
    high = rows_here + 2 * HALO
    first, rows = 1 + layer, high - 2 - 2 * layer
    tops = (first, high - HALO - first)
    narrow = layer == 3 and cols_here == 16
    left, wide = (LEFT + HALO, cols_here - 2 * HALO) if narrow else (LEFT, cols_here)
    near, far = HALO + layer, LEFT + cols_here - 6 - layer
    above = jnp.where(row > 0, 1.0, 0.0)
    below = jnp.where(row < nrows - 1, 1.0, 0.0)
    sub = lax.broadcasted_iota(jnp.int32, (1, 8, LANES), 1)
    j = jnp.where(sub < HALO, sub + (layer - 3), sub + (cols_here - 5 - layer)) + col * cols_here
    held = jnp.where((j >= 0) & (j < ncols * cols_here), 1.0, 0.0)
    m = HALO * wide

    def rows_held(at, block):
        i = lax.broadcasted_iota(jnp.int32, block, 0) + at
        return jnp.where(i < HALO, above, jnp.where(i >= high - HALO, below, 1.0))

    def whole(_, carry):
        def strip(at):
            return lambda c, a, b: act[c, pl.ds(at + a - 1, HALO), left + b - 1 : left + b - 1 + wide, :]

        def sides(c, a, b):
            return packed(act, c, first + a - 1, rows, near + b, far + b)

        acc = step_size * tap_dot([strip(at) for at in tops] + [sides], halves, weight)
        for c in range(halves):
            for k, at in enumerate(tops):
                here = (c, pl.ds(at, HALO), slice(left, left + wide), slice(None))
                u = before[here] + lanes_of(acc[k * m : (k + 1) * m], c, (HALO, wide, LANES))
                after[here] = u
                if act_after is not None:
                    act_after[here] = silu(u) * rows_held(at, u.shape)
            u = packed(before, c, first, rows, near + 1, far + 1) + lanes_of(acc[2 * m :], c, (rows, 8, LANES))
            store_packed(after, c, first, near + 1, far + 1, u)
            if act_after is not None:
                edge = HALO - first
                for at, n, mask in (
                    (0, edge, held * above), (edge, rows - 2 * edge, held), (rows - edge, edge, held * below),
                ):
                    if n > 0:
                        value = silu(u[at : at + n]) * mask
                        store_packed(act_after, c, first + at, near + 1, far + 1, value)
        return carry

    lax.fori_loop(0, once(), whole, 0)


def gather_kernel(
    sizes, x_hbm, w_hbm,
    keep, states, mid2, fin, acts, act3, w2, w3,
    land_mid, land_end, w01, mid_side, land_side, flat, send_row, send_col, recv_row, recv_side,
    load_sem, part_sem, pass_sem, halo_sem, later,
):
    nrows, ncols, step_size = sizes
    base, mid, end = [states.at[k] for k in range(3)]
    act0, act1, act2 = [acts.at[k] for k in range(3)]
    w0, w1 = w01.at[0], w01.at[1]
    halves, high = land_mid.shape[:2]
    rows_here, cols_here = keep.shape[:2]
    depth, row, col = lax.axis_index("depth"), lax.axis_index("rows"), lax.axis_index("cols")
    shape, place = (halves, rows_here, cols_here), (nrows, ncols, row, col)
    partner = (1 - depth, row, col)
    corner = HALO * HALO
    barrier = pltpu.get_barrier_semaphore()

    def lanes(c):
        return pl.ds(c * LANES, LANES)

    def local(src, dst, k):
        return pltpu.make_async_copy(src, dst, load_sem.at[k])

    def to_partner(src, dst, k, sem=part_sem):
        return pltpu.make_async_remote_copy(
            src_ref=src, dst_ref=dst, send_sem=sem.at[k], recv_sem=sem.at[k],
            device_id=partner, device_id_type=MESH,
        )

    def exists_at(step):
        there_row, there_col = row + step[0], col + step[1]
        exists = (there_row >= 0) & (there_row < nrows) & (there_col >= 0) & (there_col < ncols)
        return exists, there_row, there_col

    odd, even = lax.rem(row, 2) == 1, lax.rem(row, 2) == 0

    def pick(step, always, sometimes, first, second):
        if step == always:
            return True, None
        if step in sometimes:
            return first, second
        return None, True

    def early(step):
        return pick(step, (0, -1), ((-1, 0), (-1, -1)), odd, even)

    def early_seen_by(step):
        return pick(step, (0, 1), ((1, 0), (1, 1)), even, odd)

    def run_if(exists, also, action):
        if also is True:
            pl.when(exists)(action)
        elif also is not None:
            pl.when(exists)(lambda: pl.when(also)(action))

    def count_of(part):
        count = jnp.int32(1)
        for step in DIRECTIONS:
            also = early(step)[part]
            if also is not None:
                there = exists_at(step)[0]
                there = there if also is True else there & also
                count = count + jnp.where(there, 1, 0)
        return count

    def own(c):
        return base.at[c, pl.ds(HALO, rows_here), pl.ds(LEFT, cols_here), :]

    x_loads = [local(x_hbm.at[0, :, :, lanes(c)], own(c), c) for c in range(halves)]
    x_parts = [to_partner(x_hbm.at[0, :, :, lanes(c)], own(c), c) for c in range(halves)]
    keep_load = local(x_hbm.at[0], keep, 1)
    w_loads = [local(w_hbm.at[0], w0, halves), local(w_hbm.at[1], w1, 0)]
    late_loads = [local(w_hbm.at[0], w2, 0), local(w_hbm.at[1], w3, 1)]
    w_parts = [to_partner(w_hbm.at[0], w0, halves), to_partner(w_hbm.at[1], w1, halves + 1)]

    def inner(ref, k):
        return ref.at[:, pl.ds(HALO + k, rows_here - 2 * k), pl.ds(LEFT, cols_here), :]

    def two_rows(ref, at):
        return ref.at[:, pl.ds(at, 2), pl.ds(LEFT, cols_here), :]

    edge_rows = (HALO + 1, HALO + rows_here - 3)
    far_side = LEFT + cols_here - 8
    mid_parts = [to_partner(mid_side, land_side, halves + 2)] + [
        to_partner(two_rows(mid, at), two_rows(land_mid, at), halves + 4 + k) for k, at in enumerate(edge_rows)
    ]
    end_part = to_partner(inner(end, 2), inner(land_end, 2), halves + 3)
    passes = [
        to_partner(ref, ref, k, pass_sem) for k, ref in enumerate((recv_row, recv_side))
    ]

    def activate_rows(source, target, first, rows, copied=None):
        for c in range(halves):
            here = (c, pl.ds(first, rows), slice(LEFT, LEFT + cols_here), slice(None))
            u = source[here]
            target[here] = silu(u)
            if copied is not None:
                copied[here] = u

    copies = []
    for k, (dr, dc) in enumerate(DIRECTIONS):
        exists, there_row, there_col = exists_at((dr, dc))
        side = (dc + 1) // 2
        mine = {-1: (0, corner), 1: ((rows_here - HALO) * HALO, corner), 0: (0, rows_here * HALO)}[dr]
        theirs = {1: (0, corner), -1: (high * HALO - corner, corner), 0: (corner, rows_here * HALO)}[dr]
        if dc == 0:
            src, dst, here = send_row.at[(dr + 1) // 2], recv_row.at[(1 - dr) // 2], recv_row.at[(dr + 1) // 2]
            empty = (recv_row, (dr + 1) // 2, slice(None))
        else:
            back = {-1: (0, corner), 1: (high * HALO - corner, corner), 0: (corner, rows_here * HALO)}[dr]
            src = send_col.at[side, pl.ds(*mine)]
            dst = recv_side.at[1 - side, pl.ds(*theirs)]
            here = recv_side.at[side, pl.ds(*back)]
            empty = (recv_side, side, slice(back[0], back[0] + back[1]))

        def remote(src, dst, slot):
            return pltpu.make_async_remote_copy(
                src_ref=src, dst_ref=dst, send_sem=halo_sem.at[k], recv_sem=halo_sem.at[slot],
                device_id=(1 - depth, there_row, there_col), device_id_type=MESH,
            )

        opposite = DIRECTIONS.index((-dr, -dc))
        copies.append((exists, remote(src, dst, opposite), remote(src, here, k), empty))
    order = (4, 5, 6, 7, 2, 3, 0, 1)

    def signal(target):
        pl.semaphore_signal(barrier, inc=1, device_id=target, device_id_type=MESH)

    def send_halos(part):
        for k in order:
            exists, copy, _, _ = copies[k]
            run_if(exists, early(DIRECTIONS[k])[part], copy.start)

    @pl.when(depth == 0)
    def _():
        for copy in x_loads + w_loads[:1]:
            copy.start()
        signal(partner)
        pl.semaphore_wait(barrier, count_of(0))
        for copy in x_parts + w_parts[:1]:
            copy.start()
        for copy in x_loads:
            copy.wait()
        w_loads[1].start()
        for side in range(2):
            top = HALO if side == 0 else rows_here
            left = LEFT if side == 0 else LEFT + cols_here - HALO
            for c in range(halves):
                send_row[side, :, lanes(c)] = as_rows(base[c, top : top + HALO, LEFT : LEFT + cols_here, :])
                for i in range(rows_here):
                    flat[side, c, i * HALO : (i + 1) * HALO, :] = base[c, HALO + i, left : left + HALO, :]
            for c in range(halves):
                send_col[side, :, lanes(c)] = flat[side, c, 0 : rows_here * HALO, :].astype(jnp.bfloat16)
        send_halos(0)
        activate_rows(base, act0, HALO, rows_here)
        w_loads[0].wait()
        first = (row == 0) & (col == 0)

        def send_rest():
            pl.semaphore_wait(later.at[0], 1)
            send_halos(1)

        def both(layer, _):
            @pl.when(layer == 1)
            def _():
                for c in range(halves):
                    mid_side[c] = packed(mid, c, HALO + 1, rows_here - 2, LEFT, far_side)
                for copy in mid_parts:
                    copy.start()
                pl.when(row + col > 0)(send_rest)
                w_loads[1].wait()

            interior(
                0, acts.at[layer], w01.at[layer], states.at[layer], states.at[layer + 1],
                acts.at[layer + 1], step_size, shape,
            )
            return 0

        lax.fori_loop(0, 2, both, 0)
        keep_load.start()
        end_part.start()
        w_parts[1].start()
        pl.when(first)(send_rest)
        for copy in mid_parts:
            copy.wait_send()
        end_part.wait_send()
        keep_load.wait()
        for exists, copy, _, _ in copies:
            pl.when(exists)(copy.wait_send)
        for copy in x_parts + w_parts:
            copy.wait_send()
        for copy in passes:
            copy.wait_recv()

    @pl.when(depth == 1)
    def _():
        for copy in late_loads:
            copy.start()
        signal(partner)
        for step in DIRECTIONS:
            exists, there_row, there_col = exists_at(step)
            for side, also in enumerate(early_seen_by(step)):
                core = 1 - depth if side == 0 else depth
                run_if(exists, also, functools.partial(signal, (core, there_row, there_col)))
        for step, (_, _, _, (ref, at, rows)) in zip(DIRECTIONS, copies):
            _, there_row, there_col = exists_at(step)
            outside = (there_row < 0) | (there_row >= nrows) | (there_col < 0) | (there_col >= ncols)

            @pl.when(outside)
            def _(ref=ref, at=at, rows=rows):
                ref[at, rows, :] = jnp.zeros_like(ref[at, rows, :])

        pl.semaphore_wait(barrier, count_of(1))
        pl.semaphore_signal(later.at[0], inc=1, device_id=partner, device_id_type=MESH)
        for copy in x_parts:
            copy.wait_recv()
        activate_rows(base, act0, HALO, rows_here)
        for copy in mid_parts:
            copy.wait_recv()
        for at in edge_rows:
            activate_rows(land_mid, act1, at, 2, mid)
        for c in range(halves):
            u = land_side[c]
            store_packed(mid, c, HALO + 1, LEFT, far_side, u)
            store_packed(act1, c, HALO + 1, LEFT, far_side, silu(u))
        end_part.wait_recv()
        activate_rows(land_end, act2, HALO + 2, rows_here - 4, end)
        def forward():
            for exists, _, arrival, _ in copies:
                pl.when(exists)(arrival.wait_recv)
            for copy in passes:
                copy.start()

        late_loads[0].wait()
        interior(2, act2, w2, end, mid2, act3, step_size, shape)
        pl.when((row == 0) & (col == 0))(forward)
        late_loads[1].wait()
        interior(3, act3, w3, mid2, fin, None, step_size, shape)
        pl.when(row + col > 0)(forward)
        w_parts[0].wait_recv()

    for side in range(2):
        for c in range(halves):
            flat[side, c, 8 : 8 + high * HALO, :] = recv_side[side, :, lanes(c)].astype(jnp.float32)
            u = recv_row[side, :, lanes(c)].astype(jnp.float32).reshape(HALO, cols_here, LANES)
            rows = slice(0, HALO) if side == 0 else slice(high - HALO, high)
            base[c, rows, LEFT : LEFT + cols_here, :] = u
            act0[c, rows, LEFT : LEFT + cols_here, :] = silu(u)
    for i in range(high):
        for c in range(halves):
            at = 8 + i * HALO
            u = jnp.where(upper_sublanes(1)[0], flat[0, c, at : at + 8, :], flat[1, c, at - HALO : at + HALO, :])
            value = silu(u)
            for ref, v in ((base, u), (act0, value)):
                ref[c, i, LEFT - HALO : LEFT, :] = v[0:HALO]
                ref[c, i, LEFT + cols_here : LEFT + cols_here + HALO, :] = v[HALO:8]
    ring(0, act0, w0, base, mid, act1, step_size, shape, place)

    @pl.when(depth == 1)
    def _():
        w_parts[1].wait_recv()

    ring(1, act1, w1, mid, end, act2, step_size, shape, place)

    @pl.when(depth == 1)
    def _():
        for copy in passes:
            copy.wait_send()


def ring_kernel(
    sizes, keep, states, acts, w2, w3, mid2_in, fin_in, act3_in,
    fine_hbm, coarse_hbm, mid2, fin, act3, store_sem,
):
    nrows, ncols, step_size = sizes
    mid, end, act2 = states.at[1], states.at[2], acts.at[2]
    halves = fin.shape[0]
    rows_here, cols_here = fine_hbm.shape[1:3]
    depth, row, col = lax.axis_index("depth"), lax.axis_index("rows"), lax.axis_index("cols")
    shape, place = (halves, rows_here, cols_here), (nrows, ncols, row, col)

    def stores(ref, target, slot):
        return [
            pltpu.make_async_copy(
                ref.at[c, pl.ds(HALO, rows_here), pl.ds(LEFT, cols_here), :],
                target.at[:, :, pl.ds(c * LANES, LANES)],
                store_sem.at[slot, c],
            )
            for c in range(halves)
        ]

    def start(copies):
        for copy in copies:
            copy.start()

    @pl.when(depth == 0)
    def _():
        kept = pltpu.make_async_copy(keep, coarse_hbm.at[0], store_sem.at[2, 0])
        both = stores(mid, fine_hbm.at[0], 0) + stores(end, fine_hbm.at[1], 1)
        start([kept] + both)
        for copy in [kept] + both:
            copy.wait()

    @pl.when(depth == 1)
    def _():
        early = stores(end, coarse_hbm.at[0], 0)
        start(early)
        ring(2, act2, w2, end, mid2, act3, step_size, shape, place)
        middle = stores(mid2, fine_hbm.at[0], 1)
        start(middle)

        ring(3, act3, w3, mid2, fin, None, step_size, shape, place)
        last = stores(fin, fine_hbm.at[1], 2)
        start(last)
        for copy in early + middle + last:
            copy.wait()


def two_sections(section_states, weights):
    _, rows_here, cols_here, channels = section_states.shape
    halves = channels // LANES
    high, wide = rows_here + 2 * HALO, cols_here + 2 * LEFT
    sizes = (lax.axis_size("rows"), lax.axis_size("cols"), 2.0 / (2 * lax.axis_size("depth")))
    f32, bf16, vmem = jnp.float32, jnp.bfloat16, pltpu.VMEM
    state = vmem((halves, high, wide, LANES), f32)
    weight = vmem((9 * channels, channels), bf16)
    flat_weights = weights.reshape(2, 9 * channels, channels)
    any_space, in_vmem = pl.BlockSpec(memory_space=pl.ANY), pl.BlockSpec(memory_space=vmem)
    dma = pltpu.SemaphoreType.DMA
    kept = vmem((rows_here, cols_here, channels), f32)
    three = vmem((3, halves, high, wide, LANES), f32)
    keep, states, mid2, fin, acts, act3, w2, w3 = pl.pallas_call(
        functools.partial(gather_kernel, sizes),
        out_shape=(kept, three, state, state, three, state, weight, weight),
        in_specs=[pl.BlockSpec(memory_space=pltpu.HBM)] * 2,
        out_specs=[in_vmem] * 8,
        scratch_shapes=[
            state, state, vmem((2, 9 * channels, channels), bf16),
            vmem((halves, rows_here - 2, 8, LANES), f32), vmem((halves, rows_here - 2, 8, LANES), f32),
            vmem((2, halves, high * HALO + 16, LANES), f32),
            vmem((2, HALO * cols_here, channels), bf16),
            vmem((2, rows_here * HALO, channels), bf16),
            vmem((2, HALO * cols_here, channels), bf16),
            vmem((2, high * HALO, channels), bf16),
            dma((halves + 1,)), dma((halves + 6,)), dma((2,)), dma((8,)),
            pltpu.SemaphoreType.REGULAR((1,)),
        ],
        compiler_params=pltpu.CompilerParams(
            collective_id=0, has_side_effects=True, vmem_limit_bytes=LIMIT
        ),
    )(
        pltpu.with_memory_space_constraint(section_states, pltpu.HBM),
        pltpu.with_memory_space_constraint(flat_weights, pltpu.HBM),
    )
    outs = pl.pallas_call(
        functools.partial(ring_kernel, sizes),
        out_shape=(
            jax.ShapeDtypeStruct((2, rows_here, cols_here, channels), f32),
            jax.ShapeDtypeStruct((1, rows_here, cols_here, channels), f32),
        ) + (state,) * 3,
        in_specs=[in_vmem] * 8,
        out_specs=[any_space] * 2 + [in_vmem] * 3,
        input_output_aliases={5: 2, 6: 3, 7: 4},
        scratch_shapes=[dma((3, halves))],
        compiler_params=pltpu.CompilerParams(vmem_limit_bytes=LIMIT),
    )(keep, states, acts, w2, w3, mid2, fin, act3)
    return outs[0], outs[1]


def on_device(section_states, weights):
    _, rows_here, cols_here, channels = section_states.shape
    tiles = rows_here % 8 == 0 and cols_here % 8 == 0 and channels % LANES == 0
    if lax.axis_size("depth") == 2 and tiles and min(rows_here, cols_here) >= 16:
        return two_sections(section_states, weights)
    return chain_on_device(section_states, weights)


def solution(mesh):
    in_specs = (P("depth", "rows", "cols", None), P("depth", None, None, None, None))
    out_specs = (P("depth", "rows", "cols", None), P("depth", "rows", "cols", None))
    return jax.shard_map(
        on_device, mesh=mesh, in_specs=in_specs, out_specs=out_specs, check_vma=False
    )
```

```python
import functools

import jax
import jax.numpy as jnp
from jax import lax
from jax.experimental import pallas as pl
from jax.experimental.pallas import tpu as pltpu
from jax.sharding import PartitionSpec as P

MESH = pl.DeviceIdType.MESH
HALO = 4
LANES = 128
LIMIT = 32 * 1024 * 1024


def padded_2(shard, sides, width):
    for axis, dim in sides:
        size, length = (lax.axis_size(axis), shard.shape[dim])
        up = [(i, (i + 1) % size) for i in range(size - 1)]
        down = [(j, i) for i, j in up]
        last = lax.slice_in_dim(shard, length - width, length, axis=dim)
        initial = lax.slice_in_dim(shard, 0, width, axis=dim)
        before = lax.ppermute(last, axis, up)
        after = lax.ppermute(initial, axis, down)
        shard = jnp.concatenate([before, shard, after], axis=dim)
    return shard


def shifted_2(block, axis, distance):
    devices = range(lax.axis_size(axis))
    route = [(i - distance, i) for i in devices if i - distance in devices]
    return lax.ppermute(block, axis, route)


def activate(field):
    return jax.nn.silu(field).astype(jnp.bfloat16)


def apply_stencil(padded, flat_weight, out_rows, out_cols):
    channels = padded.shape[2]
    patches = jnp.concatenate(
        [
            padded[shift_row : shift_row + out_rows, shift_col : shift_col + out_cols]
            for shift_row in range(3)
            for shift_col in range(3)
        ],
        axis=2,
    )
    summed = jnp.dot(
        patches.reshape(out_rows * out_cols, 9 * channels),
        flat_weight,
        preferred_element_type=jnp.float32,
    )
    return summed.reshape(out_rows, out_cols, channels)


def section_pass(anchor, first_weight, second_weight, step_size):
    rows_here, cols_here, channels = anchor.shape
    widened = padded_2(anchor, (("rows", 0), ("cols", 1)), 2)
    slope_wide = apply_stencil(activate(widened), first_weight, rows_here + 2, cols_here + 2)
    middle_wide = widened[1:-1, 1:-1] + step_size * slope_wide
    row_global = lax.axis_index("rows") * rows_here - 1 + jnp.arange(rows_here + 2)
    col_global = lax.axis_index("cols") * cols_here - 1 + jnp.arange(cols_here + 2)
    inside_rows = (row_global >= 0) & (row_global < rows_here * lax.axis_size("rows"))
    inside_cols = (col_global >= 0) & (col_global < cols_here * lax.axis_size("cols"))
    inside = inside_rows[:, None] & inside_cols[None, :]
    second_act = jnp.where(inside[:, :, None], activate(middle_wide), jnp.zeros((), jnp.bfloat16))
    first_slope = slope_wide[1:-1, 1:-1]
    middle = middle_wide[1:-1, 1:-1]
    second_slope = apply_stencil(second_act, second_weight, rows_here, cols_here)
    ending = middle + step_size * second_slope
    return (first_slope, middle, ending)


def chain_on_device(section_states, weights):
    rows_here, cols_here, channels = section_states.shape[1:]
    ndepth = lax.axis_size("depth")
    position = lax.axis_index("depth")
    step_size = 2.0 / (2 * ndepth)
    first_weight = weights[0].reshape(9 * channels, channels)
    second_weight = weights[1].reshape(9 * channels, channels)
    anchor = section_states[0]
    first_slope, middle, ending = section_pass(anchor, first_weight, second_weight, step_size)
    jump = ending - (anchor + 2.0 * step_size * first_slope)

    def chain_turn(step_index, current):
        padded = padded_2(activate(current), (("rows", 0), ("cols", 1)), 1)
        advanced = (
            current
            + 2.0 * step_size * apply_stencil(padded, first_weight, rows_here, cols_here)
            + jump
        )
        shifted = shifted_2(advanced, "depth", 1)
        return jnp.where(position == 0, anchor, shifted)

    corrected = lax.fori_loop(0, ndepth - 1, chain_turn, anchor)
    final_slope, final_middle, final_ending = section_pass(
        corrected, first_weight, second_weight, step_size
    )
    fine_states = jnp.stack([final_middle, final_ending])
    return (fine_states, corrected[None])


DIRECTIONS = ((-1, 0), (1, 0), (0, -1), (0, 1), (-1, -1), (-1, 1), (1, -1), (1, 1))
LEFT = 8


def silu(u):
    half = 0.5 * u
    return half + half * jnp.tanh(half)


def as_rows(block):
    return block.reshape(-1, LANES).astype(jnp.bfloat16)


def tap_dot(windows, halves, weight):
    lhs = []
    for a in range(3):
        for b in range(3):
            for c in range(halves):
                parts = [as_rows(window(c, a, b)) for window in windows]
                lhs.append(parts[0] if len(parts) == 1 else jnp.concatenate(parts, axis=0))
    return jnp.dot(jnp.concatenate(lhs, axis=1), weight[...], preferred_element_type=jnp.float32)


def lanes_of(block, c, shape):
    return block[:, c * LANES : (c + 1) * LANES].reshape(shape)


def upper_sublanes(rows):
    return lax.broadcasted_iota(jnp.int32, (rows, 8, LANES), 1) < HALO


def packed(ref, c, first_row, rows, left, right):
    near = ref[c, pl.ds(first_row, rows), left : left + 8, :]
    far = ref[c, pl.ds(first_row, rows), right : right + 8, :]
    return jnp.where(upper_sublanes(rows), near, far)


def store_packed(ref, c, first_row, left, right, value):
    whole = pl.ds(first_row, value.shape[0])
    ref[c, whole, left : left + HALO, :] = value[:, 0:HALO]
    ref[c, whole, right + HALO : right + 8, :] = value[:, HALO:8]


def largest_divisor(total, limit):
    return max(n for n in range(1, limit + 1) if total % n == 0)


def once():
    return jnp.minimum(lax.axis_index("rows"), 0) + 1


def interior(layer, act, weight, before, after, act_after, step_size, shape):
    halves, rows_here, cols_here = shape
    narrow = layer == 3 and cols_here == 16
    left, wide = (LEFT + HALO, cols_here - 2 * HALO) if narrow else (LEFT, cols_here)
    exact = layer >= 2
    first, rows = (HALO + 1 + layer, rows_here - 2 - 2 * layer) if exact else (HALO + 1, rows_here - 2)
    n = rows if exact else largest_divisor(rows, 30)

    def chunk(k, _):
        at = first + k * n

        def window(c, a, b):
            return act[c, pl.ds(at + a - 1, n), left + b - 1 : left + b - 1 + wide, :]

        acc = step_size * tap_dot([window], halves, weight)
        for c in range(halves):
            here = (c, pl.ds(at, n), slice(left, left + wide), slice(None))
            u = before[here] + lanes_of(acc, c, (n, wide, LANES))
            after[here] = u
            if act_after is not None:
                act_after[here] = silu(u)
        return 0

    lax.fori_loop(0, once() if rows == n else rows // n, chunk, 0)


def ring(layer, act, weight, before, after, act_after, step_size, shape, place):
    halves, rows_here, cols_here = shape
    nrows, ncols, row, col = place
    high = rows_here + 2 * HALO
    first, rows = 1 + layer, high - 2 - 2 * layer
    tops = (first, high - HALO - first)
    narrow = layer == 3 and cols_here == 16
    left, wide = (LEFT + HALO, cols_here - 2 * HALO) if narrow else (LEFT, cols_here)
    near, far = HALO + layer, LEFT + cols_here - 6 - layer
    above = jnp.where(row > 0, 1.0, 0.0)
    below = jnp.where(row < nrows - 1, 1.0, 0.0)
    sub = lax.broadcasted_iota(jnp.int32, (1, 8, LANES), 1)
    j = jnp.where(sub < HALO, sub + (layer - 3), sub + (cols_here - 5 - layer)) + col * cols_here
    held = jnp.where((j >= 0) & (j < ncols * cols_here), 1.0, 0.0)
    m = HALO * wide

    def whole(_, carry):
        def strip(at):
            return lambda c, a, b: act[c, pl.ds(at + a - 1, HALO), left + b - 1 : left + b - 1 + wide, :]

        def sides(c, a, b):
            return packed(act, c, first + a - 1, rows, near + b, far + b)

        acc = step_size * tap_dot([strip(at) for at in tops] + [sides], halves, weight)
        for c in range(halves):
            for k, at in enumerate(tops):
                here = (c, pl.ds(at, HALO), slice(left, left + wide), slice(None))
                u = before[here] + lanes_of(acc[k * m : (k + 1) * m], c, (HALO, wide, LANES))
                after[here] = u
                if act_after is not None:
                    value = silu(u)
                    for i in range(HALO):
                        held_row = above if at + i < HALO else below if at + i >= high - HALO else None
                        row_value = value[i] if held_row is None else value[i] * held_row
                        act_after[c, at + i, left : left + wide, :] = row_value
            u = packed(before, c, first, rows, near + 1, far + 1) + lanes_of(acc[2 * m :], c, (rows, 8, LANES))
            store_packed(after, c, first, near + 1, far + 1, u)
            if act_after is not None:
                edge = HALO - first
                for at, n, mask in (
                    (0, edge, held * above), (edge, rows - 2 * edge, held), (rows - edge, edge, held * below),
                ):
                    if n > 0:
                        value = silu(u[at : at + n]) * mask
                        store_packed(act_after, c, first + at, near + 1, far + 1, value)
        return carry

    lax.fori_loop(0, once(), whole, 0)


def gather_kernel(
    sizes, x_hbm, w_hbm,
    keep, states, mid2, fin, acts, act3, w2, w3,
    land_mid, land_end, w01, mid_side, land_side, flat, send_row, send_col, recv_row, recv_side,
    load_sem, part_sem, pass_sem, halo_sem, later,
):
    nrows, ncols, step_size = sizes
    base, mid, end = [states.at[k] for k in range(3)]
    act0, act1, act2 = [acts.at[k] for k in range(3)]
    w0, w1 = w01.at[0], w01.at[1]
    halves, high = land_mid.shape[:2]
    rows_here, cols_here = keep.shape[:2]
    depth, row, col = lax.axis_index("depth"), lax.axis_index("rows"), lax.axis_index("cols")
    shape, place = (halves, rows_here, cols_here), (nrows, ncols, row, col)
    partner = (1 - depth, row, col)
    corner = HALO * HALO
    barrier = pltpu.get_barrier_semaphore()

    def lanes(c):
        return pl.ds(c * LANES, LANES)

    def local(src, dst, k):
        return pltpu.make_async_copy(src, dst, load_sem.at[k])

    def to_partner(src, dst, k, sem=part_sem):
        return pltpu.make_async_remote_copy(
            src_ref=src, dst_ref=dst, send_sem=sem.at[k], recv_sem=sem.at[k],
            device_id=partner, device_id_type=MESH,
        )

    def exists_at(step):
        there_row, there_col = row + step[0], col + step[1]
        exists = (there_row >= 0) & (there_row < nrows) & (there_col >= 0) & (there_col < ncols)
        return exists, there_row, there_col

    odd, even = lax.rem(row, 2) == 1, lax.rem(row, 2) == 0

    def pick(step, always, sometimes, first, second):
        if step == always:
            return True, None
        if step in sometimes:
            return first, second
        return None, True

    def early(step):
        return pick(step, (0, -1), ((-1, 0), (-1, -1)), odd, even)

    def early_seen_by(step):
        return pick(step, (0, 1), ((1, 0), (1, 1)), even, odd)

    def run_if(exists, also, action):
        if also is True:
            pl.when(exists)(action)
        elif also is not None:
            pl.when(exists)(lambda: pl.when(also)(action))

    def count_of(part):
        count = jnp.int32(1)
        for step in DIRECTIONS:
            also = early(step)[part]
            if also is not None:
                there = exists_at(step)[0]
                there = there if also is True else there & also
                count = count + jnp.where(there, 1, 0)
        return count

    def own(c):
        return base.at[c, pl.ds(HALO, rows_here), pl.ds(LEFT, cols_here), :]

    x_loads = [local(x_hbm.at[0, :, :, lanes(c)], own(c), c) for c in range(halves)]
    x_parts = [to_partner(x_hbm.at[0, :, :, lanes(c)], own(c), c) for c in range(halves)]
    keep_load = local(x_hbm.at[0], keep, 1)
    w_loads = [local(w_hbm.at[0], w0, halves), local(w_hbm.at[1], w1, 0)]
    late_loads = [local(w_hbm.at[0], w2, 0), local(w_hbm.at[1], w3, 1)]
    w_parts = [to_partner(w_hbm.at[0], w0, halves), to_partner(w_hbm.at[1], w1, halves + 1)]

    def inner(ref, k):
        return ref.at[:, pl.ds(HALO + k, rows_here - 2 * k), pl.ds(LEFT, cols_here), :]

    def two_rows(ref, at):
        return ref.at[:, pl.ds(at, 2), pl.ds(LEFT, cols_here), :]

    edge_rows = (HALO + 1, HALO + rows_here - 3)
    far_side = LEFT + cols_here - 8
    mid_parts = [to_partner(mid_side, land_side, halves + 2)] + [
        to_partner(two_rows(mid, at), two_rows(land_mid, at), halves + 4 + k) for k, at in enumerate(edge_rows)
    ]
    end_part = to_partner(inner(end, 2), inner(land_end, 2), halves + 3)
    passes = [
        to_partner(ref, ref, k, pass_sem) for k, ref in enumerate((recv_row, recv_side))
    ]

    def activate_rows(source, target, first, rows, copied=None):
        for c in range(halves):
            here = (c, pl.ds(first, rows), slice(LEFT, LEFT + cols_here), slice(None))
            u = source[here]
            target[here] = silu(u)
            if copied is not None:
                copied[here] = u

    copies = []
    for k, (dr, dc) in enumerate(DIRECTIONS):
        exists, there_row, there_col = exists_at((dr, dc))
        side = (dc + 1) // 2
        mine = {-1: (0, corner), 1: ((rows_here - HALO) * HALO, corner), 0: (0, rows_here * HALO)}[dr]
        theirs = {1: (0, corner), -1: (high * HALO - corner, corner), 0: (corner, rows_here * HALO)}[dr]
        if dc == 0:
            src, dst, here = send_row.at[(dr + 1) // 2], recv_row.at[(1 - dr) // 2], recv_row.at[(dr + 1) // 2]
            empty = (recv_row, (dr + 1) // 2, slice(None))
        else:
            back = {-1: (0, corner), 1: (high * HALO - corner, corner), 0: (corner, rows_here * HALO)}[dr]
            src = send_col.at[side, pl.ds(*mine)]
            dst = recv_side.at[1 - side, pl.ds(*theirs)]
            here = recv_side.at[side, pl.ds(*back)]
            empty = (recv_side, side, slice(back[0], back[0] + back[1]))

        def remote(src, dst, slot):
            return pltpu.make_async_remote_copy(
                src_ref=src, dst_ref=dst, send_sem=halo_sem.at[k], recv_sem=halo_sem.at[slot],
                device_id=(1 - depth, there_row, there_col), device_id_type=MESH,
            )

        opposite = DIRECTIONS.index((-dr, -dc))
        copies.append((exists, remote(src, dst, opposite), remote(src, here, k), empty))
    order = (4, 5, 6, 7, 2, 3, 0, 1)

    def signal(target):
        pl.semaphore_signal(barrier, inc=1, device_id=target, device_id_type=MESH)

    def send_halos(part):
        for k in order:
            exists, copy, _, _ = copies[k]
            run_if(exists, early(DIRECTIONS[k])[part], copy.start)

    @pl.when(depth == 0)
    def _():
        for copy in x_loads + w_loads[:1]:
            copy.start()
        signal(partner)
        pl.semaphore_wait(barrier, count_of(0))
        for copy in x_parts + w_parts[:1]:
            copy.start()
        for copy in x_loads:
            copy.wait()
        w_loads[1].start()
        for side in range(2):
            top = HALO if side == 0 else rows_here
            left = LEFT if side == 0 else LEFT + cols_here - HALO
            for c in range(halves):
                send_row[side, :, lanes(c)] = as_rows(base[c, top : top + HALO, LEFT : LEFT + cols_here, :])
                for i in range(rows_here):
                    flat[side, c, i * HALO : (i + 1) * HALO, :] = base[c, HALO + i, left : left + HALO, :]
            for c in range(halves):
                send_col[side, :, lanes(c)] = flat[side, c, 0 : rows_here * HALO, :].astype(jnp.bfloat16)
        send_halos(0)
        activate_rows(base, act0, HALO, rows_here)
        w_loads[0].wait()
        first = (row == 0) & (col == 0)

        def send_rest():
            pl.semaphore_wait(later.at[0], 1)
            send_halos(1)

        def both(layer, _):
            @pl.when(layer == 1)
            def _():
                for c in range(halves):
                    mid_side[c] = packed(mid, c, HALO + 1, rows_here - 2, LEFT, far_side)
                for copy in mid_parts:
                    copy.start()
                pl.when(row + col > 0)(send_rest)
                w_loads[1].wait()

            interior(
                0, acts.at[layer], w01.at[layer], states.at[layer], states.at[layer + 1],
                acts.at[layer + 1], step_size, shape,
            )
            return 0

        lax.fori_loop(0, 2, both, 0)
        keep_load.start()
        end_part.start()
        w_parts[1].start()
        pl.when(first)(send_rest)
        for copy in mid_parts:
            copy.wait_send()
        end_part.wait_send()
        keep_load.wait()
        for exists, copy, _, _ in copies:
            pl.when(exists)(copy.wait_send)
        for copy in x_parts + w_parts:
            copy.wait_send()
        for copy in passes:
            copy.wait_recv()

    @pl.when(depth == 1)
    def _():
        for copy in late_loads:
            copy.start()
        signal(partner)
        for step in DIRECTIONS:
            exists, there_row, there_col = exists_at(step)
            for side, also in enumerate(early_seen_by(step)):
                core = 1 - depth if side == 0 else depth
                run_if(exists, also, functools.partial(signal, (core, there_row, there_col)))
        for step, (_, _, _, (ref, at, rows)) in zip(DIRECTIONS, copies):
            _, there_row, there_col = exists_at(step)
            outside = (there_row < 0) | (there_row >= nrows) | (there_col < 0) | (there_col >= ncols)

            @pl.when(outside)
            def _(ref=ref, at=at, rows=rows):
                ref[at, rows, :] = jnp.zeros_like(ref[at, rows, :])

        pl.semaphore_wait(barrier, count_of(1))
        pl.semaphore_signal(later.at[0], inc=1, device_id=partner, device_id_type=MESH)
        for copy in x_parts:
            copy.wait_recv()
        activate_rows(base, act0, HALO, rows_here)
        for copy in mid_parts:
            copy.wait_recv()
        for at in edge_rows:
            activate_rows(land_mid, act1, at, 2, mid)
        for c in range(halves):
            u = land_side[c]
            store_packed(mid, c, HALO + 1, LEFT, far_side, u)
            store_packed(act1, c, HALO + 1, LEFT, far_side, silu(u))
        end_part.wait_recv()
        activate_rows(land_end, act2, HALO + 2, rows_here - 4, end)
        def forward():
            for exists, _, arrival, _ in copies:
                pl.when(exists)(arrival.wait_recv)
            for copy in passes:
                copy.start()

        late_loads[0].wait()
        interior(2, act2, w2, end, mid2, act3, step_size, shape)
        pl.when((row == 0) & (col == 0))(forward)
        late_loads[1].wait()
        interior(3, act3, w3, mid2, fin, None, step_size, shape)
        pl.when(row + col > 0)(forward)
        w_parts[0].wait_recv()

    for side in range(2):
        for c in range(halves):
            flat[side, c, 8 : 8 + high * HALO, :] = recv_side[side, :, lanes(c)].astype(jnp.float32)
            u = recv_row[side, :, lanes(c)].astype(jnp.float32).reshape(HALO, cols_here, LANES)
            rows = slice(0, HALO) if side == 0 else slice(high - HALO, high)
            base[c, rows, LEFT : LEFT + cols_here, :] = u
            act0[c, rows, LEFT : LEFT + cols_here, :] = silu(u)
    for i in range(high):
        for c in range(halves):
            at = 8 + i * HALO
            u = jnp.where(upper_sublanes(1)[0], flat[0, c, at : at + 8, :], flat[1, c, at - HALO : at + HALO, :])
            value = silu(u)
            for ref, v in ((base, u), (act0, value)):
                ref[c, i, LEFT - HALO : LEFT, :] = v[0:HALO]
                ref[c, i, LEFT + cols_here : LEFT + cols_here + HALO, :] = v[HALO:8]
    ring(0, act0, w0, base, mid, act1, step_size, shape, place)

    @pl.when(depth == 1)
    def _():
        w_parts[1].wait_recv()

    ring(1, act1, w1, mid, end, act2, step_size, shape, place)

    @pl.when(depth == 1)
    def _():
        for copy in passes:
            copy.wait_send()


def ring_kernel(
    sizes, keep, states, acts, w2, w3, mid2_in, fin_in, act3_in,
    fine_hbm, coarse_hbm, mid2, fin, act3, store_sem,
):
    nrows, ncols, step_size = sizes
    mid, end, act2 = states.at[1], states.at[2], acts.at[2]
    halves = fin.shape[0]
    rows_here, cols_here = fine_hbm.shape[1:3]
    depth, row, col = lax.axis_index("depth"), lax.axis_index("rows"), lax.axis_index("cols")
    shape, place = (halves, rows_here, cols_here), (nrows, ncols, row, col)

    def stores(ref, target, slot):
        return [
            pltpu.make_async_copy(
                ref.at[c, pl.ds(HALO, rows_here), pl.ds(LEFT, cols_here), :],
                target.at[:, :, pl.ds(c * LANES, LANES)],
                store_sem.at[slot, c],
            )
            for c in range(halves)
        ]

    def start(copies):
        for copy in copies:
            copy.start()

    @pl.when(depth == 0)
    def _():
        kept = pltpu.make_async_copy(keep, coarse_hbm.at[0], store_sem.at[2, 0])
        both = stores(mid, fine_hbm.at[0], 0) + stores(end, fine_hbm.at[1], 1)
        start([kept] + both)
        for copy in [kept] + both:
            copy.wait()

    @pl.when(depth == 1)
    def _():
        early = stores(end, coarse_hbm.at[0], 0)
        start(early)
        ring(2, act2, w2, end, mid2, act3, step_size, shape, place)
        middle = stores(mid2, fine_hbm.at[0], 1)
        start(middle)

        ring(3, act3, w3, mid2, fin, None, step_size, shape, place)
        last = stores(fin, fine_hbm.at[1], 2)
        start(last)
        for copy in early + middle + last:
            copy.wait()


def two_sections(section_states, weights):
    _, rows_here, cols_here, channels = section_states.shape
    halves = channels // LANES
    high, wide = rows_here + 2 * HALO, cols_here + 2 * LEFT
    sizes = (lax.axis_size("rows"), lax.axis_size("cols"), 2.0 / (2 * lax.axis_size("depth")))
    f32, bf16, vmem = jnp.float32, jnp.bfloat16, pltpu.VMEM
    state = vmem((halves, high, wide, LANES), f32)
    weight = vmem((9 * channels, channels), bf16)
    flat_weights = weights.reshape(2, 9 * channels, channels)
    any_space, in_vmem = pl.BlockSpec(memory_space=pl.ANY), pl.BlockSpec(memory_space=vmem)
    dma = pltpu.SemaphoreType.DMA
    kept = vmem((rows_here, cols_here, channels), f32)
    three = vmem((3, halves, high, wide, LANES), f32)
    keep, states, mid2, fin, acts, act3, w2, w3 = pl.pallas_call(
        functools.partial(gather_kernel, sizes),
        out_shape=(kept, three, state, state, three, state, weight, weight),
        in_specs=[pl.BlockSpec(memory_space=pltpu.HBM)] * 2,
        out_specs=[in_vmem] * 8,
        scratch_shapes=[
            state, state, vmem((2, 9 * channels, channels), bf16),
            vmem((halves, rows_here - 2, 8, LANES), f32), vmem((halves, rows_here - 2, 8, LANES), f32),
            vmem((2, halves, high * HALO + 16, LANES), f32),
            vmem((2, HALO * cols_here, channels), bf16),
            vmem((2, rows_here * HALO, channels), bf16),
            vmem((2, HALO * cols_here, channels), bf16),
            vmem((2, high * HALO, channels), bf16),
            dma((halves + 1,)), dma((halves + 6,)), dma((2,)), dma((8,)),
            pltpu.SemaphoreType.REGULAR((1,)),
        ],
        compiler_params=pltpu.CompilerParams(
            collective_id=0, has_side_effects=True, vmem_limit_bytes=LIMIT
        ),
    )(
        pltpu.with_memory_space_constraint(section_states, pltpu.HBM),
        pltpu.with_memory_space_constraint(flat_weights, pltpu.HBM),
    )
    outs = pl.pallas_call(
        functools.partial(ring_kernel, sizes),
        out_shape=(
            jax.ShapeDtypeStruct((2, rows_here, cols_here, channels), f32),
            jax.ShapeDtypeStruct((1, rows_here, cols_here, channels), f32),
        ) + (state,) * 3,
        in_specs=[in_vmem] * 8,
        out_specs=[any_space] * 2 + [in_vmem] * 3,
        input_output_aliases={5: 2, 6: 3, 7: 4},
        scratch_shapes=[dma((3, halves))],
        compiler_params=pltpu.CompilerParams(vmem_limit_bytes=LIMIT),
    )(keep, states, acts, w2, w3, mid2, fin, act3)
    return outs[0], outs[1]


def on_device(section_states, weights):
    _, rows_here, cols_here, channels = section_states.shape
    tiles = rows_here % 8 == 0 and cols_here % 8 == 0 and channels % LANES == 0
    if lax.axis_size("depth") == 2 and tiles and min(rows_here, cols_here) >= 16:
        return two_sections(section_states, weights)
    return chain_on_device(section_states, weights)


def solution(mesh):
    in_specs = (P("depth", "rows", "cols", None), P("depth", None, None, None, None))
    out_specs = (P("depth", "rows", "cols", None), P("depth", "rows", "cols", None))
    return jax.shard_map(
        on_device, mesh=mesh, in_specs=in_specs, out_specs=out_specs, check_vma=False
    )
```
